128 devices in a mesh: dp: 1, x: 128 (over z, y, x, core).
Axes of the slice: x: 4, y: 4, z: 4, core: 2. Of those that a mesh axis runs over, the one named last changes fastest.
Arguments:
- c_raw: bfloat16 [512, 1024, 512], P('dp', 'x')
- k_raw: bfloat16 [512, 1024, 64], P('dp', 'x')
- norm_gain: bfloat16 [512], replicated
- rope_cos: float32 [1024, 32], P('x')
- rope_sin: float32 [1024, 32], P('x')
- seq_lens: int32 [512], P('dp')
- q_lat: bfloat16 [512, 16, 512], P(('dp', 'x'))
- q_rope: bfloat16 [512, 16, 64], P(('dp', 'x'))
Outputs:
- output 1: bfloat16 [512, 1024, 512], P(('dp', 'x'))
- output 2: bfloat16 [512, 1024, 64], P(('dp', 'x'))
- output 3: bfloat16 [512, 16, 512], P(('dp', 'x'))
All inputs are finite; a program needn't handle non-finite values.
Results may differ from the reference program's by a relative error of at most 0.00589776.
Values are sent between devices in bfloat16 or wider.
A program may use at most 1 GiB of HBM per device.

```python
import jax
import jax.numpy as jnp
from jax import lax

REQUESTS = 512
SEQ_LEN = 1024
KV_RANK = 512
ROPE_DIM = 64
NUM_HEADS = 16

NORM_EPS = 1e-6
ATTN_SCALE = (KV_RANK + ROPE_DIM) ** -0.5


def setup_inputs(seed: int = 0, part: int = 0) -> dict:
    part_key = jax.random.fold_in(jax.random.key(seed), part)
    keys = jax.random.split(part_key, 8)
    shared = jax.random.split(jax.random.key(seed + 1), 2)
    row_scale = jnp.exp(0.5 * jax.random.normal(keys[0], (REQUESTS, SEQ_LEN, 1), jnp.float32))
    c_raw = (jax.random.normal(keys[1], (REQUESTS, SEQ_LEN, KV_RANK), jnp.float32) * row_scale).astype(jnp.bfloat16)
    k_raw = jax.random.normal(keys[2], (REQUESTS, SEQ_LEN, ROPE_DIM), jnp.float32).astype(jnp.bfloat16)
    norm_gain = (1.0 + 0.3 * jax.random.normal(shared[0], (KV_RANK,), jnp.float32)).astype(jnp.bfloat16)
    half_dim = ROPE_DIM // 2
    log_base = jax.random.uniform(shared[1], (), jnp.float32, 9.0, 14.0)
    inv_freq = jnp.exp(-log_base * (2.0 * jnp.arange(half_dim, dtype=jnp.float32) / ROPE_DIM))
    angles = jnp.arange(SEQ_LEN, dtype=jnp.float32)[:, None] * inv_freq[None, :]
    seq_lens = jax.random.randint(keys[3], (REQUESTS,), SEQ_LEN // 8, SEQ_LEN + 1)
    full_index = jax.random.randint(keys[4], (), 0, REQUESTS)
    short_offset = jax.random.randint(keys[5], (), 1, REQUESTS)
    seq_lens = seq_lens.at[full_index].set(SEQ_LEN)
    seq_lens = seq_lens.at[(full_index + short_offset) % REQUESTS].set(SEQ_LEN // 8)
    q_lat = (1.3 * jax.random.normal(keys[6], (REQUESTS, NUM_HEADS, KV_RANK), jnp.float32)).astype(jnp.bfloat16)
    q_rope = (3.0 * jax.random.normal(keys[7], (REQUESTS, NUM_HEADS, ROPE_DIM), jnp.float32)).astype(jnp.bfloat16)
    return {"c_raw": c_raw, "k_raw": k_raw, "norm_gain": norm_gain, "rope_cos": jnp.cos(angles), "rope_sin": jnp.sin(angles), "seq_lens": seq_lens.astype(jnp.int32), "q_lat": q_lat, "q_rope": q_rope}


def reference(c_raw, k_raw, norm_gain, rope_cos, rope_sin, seq_lens, q_lat, q_rope):
    positions = jnp.arange(SEQ_LEN)
    half_dim = ROPE_DIM // 2
    gain = norm_gain.astype(jnp.float32)

    def one_request(operands):
        c_row, k_row, length, lat_row, rope_row = operands
        valid = positions < length
        lat_f32 = c_row.astype(jnp.float32)
        inv_rms = lax.rsqrt(jnp.mean(lat_f32 * lat_f32, axis=-1, keepdims=True) + NORM_EPS)
        c_norm = jnp.where(valid[:, None], lat_f32 * inv_rms * gain, 0.0).astype(jnp.bfloat16)
        key_f32 = k_row.astype(jnp.float32)
        key_lo = key_f32[:, :half_dim]
        key_hi = key_f32[:, half_dim:]
        rotated = jnp.concatenate([key_lo * rope_cos - key_hi * rope_sin, key_hi * rope_cos + key_lo * rope_sin], axis=-1)
        k_rope = jnp.where(valid[:, None], rotated, 0.0).astype(jnp.bfloat16)
        scores = jnp.dot(lat_row, c_norm.T, preferred_element_type=jnp.float32) + jnp.dot(rope_row, k_rope.T, preferred_element_type=jnp.float32)
        scores = jnp.where(valid[None, :], scores * ATTN_SCALE, -1e30)
        weights = jnp.exp(scores - jnp.max(scores, axis=-1, keepdims=True))
        out_row = jnp.dot(weights, c_norm.astype(jnp.float32)) / jnp.sum(weights, axis=-1, keepdims=True)
        return c_norm, k_rope, out_row.astype(jnp.bfloat16)

    c_cache, kr_cache, o_lat = lax.map(one_request, (c_raw, k_raw, seq_lens, q_lat, q_rope))
    return (c_cache, kr_cache, o_lat)
```

```python
import jax
import jax.numpy as jnp
from jax import lax
from jax.experimental import pallas as pl
from jax.experimental.pallas import tpu as pltpu
from jax.sharding import PartitionSpec as P

NORM_EPS = 1e-6
ORDERS = ((0, 1, 2), (1, 2, 0), (2, 0, 1))
FULL = (4, 4, 4, 2, 8, 768)
COPIES = 66


def exchange_kernel(c_ref, k_ref, out0, out1, out2, *scratch):
    outs = (out0, out1, out2)
    src, mid1, mid2 = scratch[0:3], scratch[3:6], scratch[6:9]
    hop1, hop2, hop3 = scratch[9:15], scratch[15:21], scratch[21:27]
    load_sem, send_sem, recv_sem = scratch[27:30]

    me = lax.axis_index("x")
    core = me % 2
    cores = (core, 1 - core)
    place = (me // 32, (me // 8) % 4, (me // 2) % 4)

    def device(dim, delta, to_core=None):
        pos = list(place)
        pos[dim] = (pos[dim] + delta + 4) % 4
        last = core if to_core is None else to_core
        return ((pos[0] * 4 + pos[1]) * 4 + pos[2]) * 2 + last

    def at(dim, delta):
        return (place[dim] + delta + 4) % 4

    def view(ref, sel):
        return ref.at[tuple(pl.ds(*sel[d]) if d in sel else slice(None) for d in range(6))]

    loads = []
    n_load = 0

    def load(a, b):
        nonlocal n_load
        copy = pltpu.make_async_copy(a, b, load_sem.at[n_load])
        n_load += 1
        copy.start()
        loads.append(copy)

    def c_view(sel, req, cols):
        return c_ref.at[tuple(pl.ds(*sel[d]) if d in sel else slice(None) for d in range(4)) + (req, slice(None), pl.ds(*cols))]

    extra = ((3, (0, 256)), (3, (256, 256)))
    for p in range(3):
        load(c_view({}, p, (0, 512)), view(src[p], {5: (0, 512)}))
        if p < 2:
            load(c_view({}, *extra[p]), view(src[p], {5: (512, 256)}))
        else:
            load(k_ref, view(src[p], {5: (512, 256)}))
    for p in range(3):
        a = ORDERS[p][0]
        own = {a: (place[a], 1)}
        load(c_view(own, p, (0, 512)), view(mid1[p], {**own, 5: (0, 512)}))
        if p < 2:
            load(c_view(own, *extra[p]), view(mid1[p], {**own, 5: (512, 256)}))
        else:
            load(view(k_ref, own), view(mid1[p], {**own, 5: (512, 256)}))

    barrier = pltpu.get_barrier_semaphore()
    for dim in range(3):
        for delta in (1, -1):
            for k in range(2):
                pl.semaphore_signal(barrier, inc=1, device_id={"x": device(dim, delta, k)}, device_id_type=pl.DeviceIdType.MESH)
    pl.semaphore_signal(barrier, inc=1, device_id={"x": me + 1 - 2 * core}, device_id_type=pl.DeviceIdType.MESH)
    pl.semaphore_wait(barrier, 13)

    copies = [{} for _ in range(3)]

    def send(p, key, a, b, to):
        n = len(copies[p])
        copy = pltpu.make_async_remote_copy(src_ref=a, dst_ref=b, send_sem=send_sem.at[p, n], recv_sem=recv_sem.at[p, n], device_id={"x": to}, device_id_type=pl.DeviceIdType.MESH)
        copies[p][key] = copy
        copy.start()

    def arrived(p, *keys):
        for key in keys:
            copies[p][key].wait_recv()

    SIGNS = (1, -1)

    def phase1(p):
        a, b, _ = ORDERS[p]
        for s, sign in enumerate(SIGNS):
            send(p, ("1far", s), view(src[p], {a: (at(a, 2), 1), b: (2 * s, 2)}), hop1[2 * p + s], device(a, sign))
        for s, sign in enumerate(SIGNS):
            send(p, ("1near", s), view(src[p], {a: (at(a, sign), 1)}), view(mid1[p], {a: (place[a], 1)}), device(a, sign))

    def forward1(p):
        a, b, _ = ORDERS[p]
        for s, sign in enumerate(SIGNS):
            arrived(p, ("1far", s))
            send(p, ("1fwd", s), hop1[2 * p + s], view(mid1[p], {a: (at(a, -sign), 1), b: (2 * s, 2)}), device(a, sign))

    def phase2(p, off):
        a, b, c = ORDERS[p]
        sa = {a: (at(a, off), 1)}
        hop_sa = {a: (off % 4, 1)}
        for s, sign in enumerate(SIGNS):
            send(p, ("2far", off, s), view(mid1[p], {**sa, b: (at(b, 2), 1), c: (2 * s, 2)}), view(hop2[2 * p + s], hop_sa), device(b, sign))
        for s, sign in enumerate(SIGNS):
            send(p, ("2near", off, s), view(mid1[p], {**sa, b: (at(b, sign), 1)}), view(mid2[p], {**sa, b: (place[b], 1)}), device(b, sign))

    def forward2(p, off):
        a, b, c = ORDERS[p]
        sa = {a: (at(a, off), 1)}
        hop_sa = {a: (off % 4, 1)}
        for s, sign in enumerate(SIGNS):
            arrived(p, ("2far", off, s))
            send(p, ("2fwd", off, s), view(hop2[2 * p + s], hop_sa), view(mid2[p], {**sa, b: (at(b, -sign), 1), c: (2 * s, 2)}), device(b, sign))

    def phase3(p, off):
        a, b, c = ORDERS[p]
        sb = {b: (at(b, off), 1)}
        hop_sb = {b: (off % 4, 1)}
        held = mid1[p] if off == 0 else mid2[p]
        mine = {**sb, c: (place[c], 1), 3: (core, 1)}
        for s, sign in enumerate(SIGNS):
            send(p, ("3far", off, s), view(held, {**sb, c: (at(c, 2), 1), 3: (cores[s], 1)}), view(hop3[2 * p + s], hop_sb), device(c, sign))
        for s, sign in enumerate(SIGNS):
            for k in range(2):
                send(p, ("3near", off, s, k), view(held, {**sb, c: (at(c, sign), 1), 3: (cores[k], 1)}), view(outs[p], mine), device(c, sign, cores[k]))
        send(p, ("3core", off), view(held, {**sb, c: (place[c], 1), 3: (cores[1], 1)}), view(outs[p], mine), me + 1 - 2 * core)
        index = tuple(pl.ds(*mine[d]) if d in mine else slice(None) for d in range(6))
        outs[p][index] = held[index]

    def forward3(p, off):
        a, b, c = ORDERS[p]
        sb = {b: (at(b, off), 1)}
        hop_sb = {b: (off % 4, 1)}
        for s, sign in enumerate(SIGNS):
            arrived(p, ("3far", off, s))
            send(p, ("3fwd", off, s), view(hop3[2 * p + s], hop_sb), view(outs[p], {**sb, c: (at(c, -sign), 1), 3: (core, 1)}), device(c, sign, cores[s]))

    for copy in loads:
        copy.wait()
    for p in range(3):
        phase1(p)
    for p in range(3):
        forward1(p)
        phase2(p, 0)
    for p in range(3):
        arrived(p, ("1near", 0), ("1near", 1))
        phase2(p, -1)
        phase2(p, 1)
    for p in range(3):
        forward2(p, 0)
    for p in range(3):
        arrived(p, ("1fwd", 0), ("1fwd", 1))
        phase2(p, 2)
    for p in range(3):
        forward2(p, -1)
        forward2(p, 1)
    for p in range(3):
        forward2(p, 2)
        phase3(p, 0)
    for p in range(3):
        for off in (0, -1, 1, 2):
            arrived(p, ("2near", off, 0), ("2near", off, 1))
        phase3(p, -1)
        phase3(p, 1)
    for p in range(3):
        forward3(p, 0)
    for p in range(3):
        for off in (0, -1, 1, 2):
            arrived(p, ("2fwd", off, 0), ("2fwd", off, 1))
        phase3(p, 2)
    for p in range(3):
        forward3(p, -1)
        forward3(p, 1)
    for p in range(3):
        forward3(p, 2)
    for p in range(3):
        for key in copies[p]:
            if key[0] in ("3near", "3core", "3fwd"):
                arrived(p, key)
    for p in range(3):
        for copy in copies[p].values():
            copy.wait_send()


def exchange(c_raw, keys):
    part = pltpu.VMEM(FULL, jnp.bfloat16)

    def shaped(sizes):
        return pltpu.VMEM(tuple(sizes.get(d, FULL[d]) for d in range(6)), jnp.bfloat16)

    hop1 = [shaped({o[0]: 1, o[1]: 2}) for o in ORDERS for _ in range(2)]
    hop2 = [shaped({o[1]: 1, o[2]: 2}) for o in ORDERS for _ in range(2)]
    hop3 = [shaped({o[2]: 1, 3: 1}) for o in ORDERS for _ in range(2)]
    return pl.pallas_call(
        exchange_kernel,
        out_shape=[jax.ShapeDtypeStruct(FULL, jnp.bfloat16)] * 3,
        in_specs=[pl.BlockSpec(memory_space=pl.ANY)] * 2,
        out_specs=[pl.BlockSpec(memory_space=pltpu.VMEM)] * 3,
        scratch_shapes=[part] * 9 + hop1 + hop2 + hop3 + [pltpu.SemaphoreType.DMA((12,)), pltpu.SemaphoreType.DMA((3, COPIES)), pltpu.SemaphoreType.DMA((3, COPIES))],
        compiler_params=pltpu.CompilerParams(collective_id=0, has_side_effects=True, vmem_limit_bytes=60 * 1024 * 1024),
        name="exchange",
    )(c_raw, keys)


def roped_keys(k_raw, rope_cos, rope_sin):
    half_dim = k_raw.shape[-1] // 2
    key_f32 = k_raw.astype(jnp.float32)
    key_lo = key_f32[..., :half_dim]
    key_hi = key_f32[..., half_dim:]
    return jnp.concatenate([key_lo * rope_cos - key_hi * rope_sin, key_hi * rope_cos + key_lo * rope_sin], axis=-1).astype(jnp.bfloat16)


def normed(c_raw, norm_gain, valid):
    lat_f32 = c_raw.astype(jnp.float32)
    inv_rms = lax.rsqrt(jnp.mean(lat_f32 * lat_f32, axis=-1, keepdims=True) + NORM_EPS)
    return jnp.where(valid[..., None], lat_f32 * inv_rms * norm_gain.astype(jnp.float32), 0.0).astype(jnp.bfloat16)


def latent_attention(q_lat, q_rope, c_cache, kr_cache, valid):
    attn_scale = (q_lat.shape[-1] + q_rope.shape[-1]) ** -0.5
    scores = jnp.einsum("rhk,rsk->rhs", q_lat, c_cache, preferred_element_type=jnp.float32)
    scores = scores + jnp.einsum("rhe,rse->rhs", q_rope, kr_cache, preferred_element_type=jnp.float32)
    scores = jnp.where(valid[:, None, :], scores * attn_scale, -1e30)
    weights = jnp.exp(scores - jnp.max(scores, axis=-1, keepdims=True))
    weight_sum = jnp.sum(weights, axis=-1)
    weighted = jnp.einsum("rhs,rsk->rhk", weights.astype(jnp.bfloat16), c_cache, preferred_element_type=jnp.float32)
    return (weighted / weight_sum[..., None]).astype(jnp.bfloat16)


def solution(mesh):
    seq_spec = P("dp", "x", None)
    req_spec = P(("dp", "x"), None, None)

    def local_step(c_raw, k_raw, norm_gain, rope_cos, rope_sin, seq_lens, q_lat, q_rope):
        dev_index = lax.axis_index("x")
        keys = roped_keys(k_raw, rope_cos, rope_sin)
        keys = keys.reshape(128, 4, 8, 64).transpose(0, 2, 1, 3).reshape(4, 4, 4, 2, 8, 256)
        got = exchange(c_raw.reshape(4, 4, 4, 2, 4, 8, 512), keys)
        got = [part.reshape(1024, 768) for part in got]
        c_own = jnp.stack([got[0][:, :512], got[1][:, :512], got[2][:, :512], jnp.concatenate([got[0][:, 512:], got[1][:, 512:]], axis=1)])
        kr_own = got[2][:, 512:].reshape(1024, 4, 64).transpose(1, 0, 2)
        own_lens = lax.dynamic_slice_in_dim(seq_lens, dev_index * 4, 4)
        valid = jnp.arange(1024)[None, :] < own_lens[:, None]
        c_cache = normed(c_own, norm_gain, valid)
        kr_cache = jnp.where(valid[..., None], kr_own, jnp.bfloat16(0))
        o_lat = latent_attention(q_lat, q_rope, c_cache, kr_cache, valid)
        return c_cache, kr_cache, o_lat

    return jax.shard_map(local_step, mesh=mesh, in_specs=(seq_spec, seq_spec, P(None), P("x", None), P("x", None), P("dp"), req_spec, req_spec), out_specs=(req_spec, req_spec, req_spec), check_vma=False)
```

```python
import jax
import jax.numpy as jnp
from jax import lax
from jax.experimental import pallas as pl
from jax.experimental.pallas import tpu as pltpu
from jax.sharding import PartitionSpec as P

NORM_EPS = 1e-6
ATTN_SCALE = (512 + 64) ** -0.5
ORDERS = ((0, 1, 2), (1, 2, 0), (2, 0, 1))
FULL = (4, 4, 4, 2, 8, 768)
STRIDES = (256, 64, 16)
POSITIONS, LATENT, ROPE, HEADS, LANES = 1024, 512, 64, 16, 128
ROWS = 64
KEY_COLS = 256
C_COLS, K_COLS, ALL_COLS = (0, LATENT), (LATENT, KEY_COLS), (0, LATENT + KEY_COLS)
CORE, COL = 3, 5
PARTS = range(3)
PAIR = range(2)
REQUESTS = range(4)
REQ = 512
COPIES = 80
LOADS = 27
SIGNS = (1, -1)
OFFSETS = (0, -1, 1, 2)
NT = (((1,), (1,)), ((), ()))
F32, BF16 = jnp.float32, jnp.bfloat16


def exchange_kernel(c_ref, k_ref, cos_ref, sin_ref, gain_ref, len_ref, qlat_ref, qrope_ref, c_out, kr_out, score_out, len_out, scratch):
    src, mid1, mid2, got, hop1, hop2, hop3, small, sems = scratch
    k_buf, cos_buf, sin_buf, gain_buf, len_buf, qlat_buf, qrope_buf, q_rows, qk_rows = small
    load_sem, send_sem, recv_sem = sems

    me = lax.axis_index("x")
    core = me % 2
    other = me + 1 - 2 * core
    cores = (core, 1 - core)
    place = (me // 32, (me // 8) % 4, (me // 2) % 4)

    def device(dim, delta, to_core=None):
        pos = list(place)
        pos[dim] = (pos[dim] + delta + 4) % 4
        last = core if to_core is None else to_core
        return ((pos[0] * 4 + pos[1]) * 4 + pos[2]) * 2 + last

    def at(dim, delta):
        return (place[dim] + delta + 4) % 4

    def index(sel, dims=len(FULL)):
        return tuple(pl.ds(*sel[d]) if d in sel else slice(None) for d in range(dims))

    def one(i):
        return (i, 1)

    def halves(s):
        return (2 * s, 2)

    def view(ref, sel):
        return ref.at[index(sel)]

    barrier = pltpu.get_barrier_semaphore()
    for dim in PARTS:
        for delta in SIGNS:
            for k in PAIR:
                pl.semaphore_signal(barrier, inc=1, device_id={"x": device(dim, delta, k)}, device_id_type=pl.DeviceIdType.MESH)
    pl.semaphore_signal(barrier, inc=1, device_id={"x": other}, device_id_type=pl.DeviceIdType.MESH)

    loads = {}

    def load(key, a, b):
        copy = pltpu.make_async_copy(a, b, load_sem.at[len(loads)])
        loads[key] = copy
        copy.start()

    def loaded(*keys):
        for key in keys:
            loads[key].wait()

    def load_slab(p, off, into, key):
        a = ORDERS[p][0]
        sel = {a: one(at(a, off))}
        rows = index(sel, COL - 1)
        load((key, 0), c_ref.at[rows + (p, slice(None), pl.ds(*C_COLS))], view(into, {**sel, COL: C_COLS}))
        if p < 2:
            load((key, 1), c_ref.at[rows + (3, slice(None), pl.ds(KEY_COLS * p, KEY_COLS))], view(into, {**sel, COL: K_COLS}))

    load("k", k_ref, k_buf)
    load("cos", cos_ref, cos_buf)
    load("sin", sin_ref, sin_buf)
    for off in (2, 1, -1):
        for p in PARTS:
            load_slab(p, off, src[p], ("src", p, off))
    for p in PARTS:
        load_slab(p, 0, mid1[p], ("own", p))
    load("gain", gain_ref, gain_buf)
    load("len", len_ref, len_buf)
    load("qlat", qlat_ref, qlat_buf)
    load("qrope", qrope_ref, qrope_buf)

    copies = [{} for _ in PARTS]

    def send(p, key, a, b, to):
        n = len(copies[p])
        copy = pltpu.make_async_remote_copy(src_ref=a, dst_ref=b, send_sem=send_sem.at[p, n], recv_sem=recv_sem.at[p, n], device_id={"x": to}, device_id_type=pl.DeviceIdType.MESH)
        copies[p][key] = copy
        copy.start()

    def arrived(p, *keys):
        for key in keys:
            copies[p][key].wait_recv()

    def phase1(p, cols=ALL_COLS):
        a, b, _ = ORDERS[p]
        wide = {COL: cols}
        for s, sign in enumerate(SIGNS):
            send(p, ("1far", cols, s), view(src[p], {a: one(at(a, 2)), b: halves(s), **wide}), view(hop1[2 * p + s], wide), device(a, sign))
        for s, sign in enumerate(SIGNS):
            send(p, ("1near", cols, s), view(src[p], {a: one(at(a, sign)), **wide}), view(mid1[p], {a: one(place[a]), **wide}), device(a, sign))

    def forward1(p, cols=ALL_COLS):
        a, b, _ = ORDERS[p]
        wide = {COL: cols}
        for s, sign in enumerate(SIGNS):
            arrived(p, ("1far", cols, s))
            send(p, ("1fwd", cols, s), view(hop1[2 * p + s], wide), view(mid1[p], {a: one(at(a, -sign)), b: halves(s), **wide}), device(a, sign))

    def arrived1(p, kind):
        for key in list(copies[p]):
            if key[0] == kind:
                arrived(p, key)

    def phase2(p, off):
        a, b, c = ORDERS[p]
        sa = {a: one(at(a, off))}
        hop_sa = {a: one(off % 4)}
        for s, sign in enumerate(SIGNS):
            send(p, ("2far", off, s), view(mid1[p], {**sa, b: one(at(b, 2)), c: halves(s)}), view(hop2[2 * p + s], hop_sa), device(b, sign))
        for s, sign in enumerate(SIGNS):
            send(p, ("2near", off, s), view(mid1[p], {**sa, b: one(at(b, sign))}), view(mid2[p], {**sa, b: one(place[b])}), device(b, sign))

    def forward2(p, off):
        a, b, c = ORDERS[p]
        sa = {a: one(at(a, off))}
        hop_sa = {a: one(off % 4)}
        for s, sign in enumerate(SIGNS):
            arrived(p, ("2far", off, s))
            send(p, ("2fwd", off, s), view(hop2[2 * p + s], hop_sa), view(mid2[p], {**sa, b: one(at(b, -sign)), c: halves(s)}), device(b, sign))

    def phase3(p, off):
        a, b, c = ORDERS[p]
        sb = {b: one(at(b, off))}
        hop_sb = {b: one(off % 4)}
        held = mid1[p] if off == 0 else mid2[p]
        mine = {**sb, c: one(place[c]), CORE: one(core)}
        for s, sign in enumerate(SIGNS):
            send(p, ("3far", off, s), view(held, {**sb, c: one(at(c, 2)), CORE: one(cores[s])}), view(hop3[2 * p + s], hop_sb), device(c, sign))
        for s, sign in enumerate(SIGNS):
            for k in PAIR:
                send(p, ("3near", off, s, k), view(held, {**sb, c: one(at(c, sign)), CORE: one(cores[k])}), view(got[p], mine), device(c, sign, cores[k]))
        send(p, ("3core", off), view(held, {**sb, c: one(place[c]), CORE: one(cores[1])}), view(got[p], mine), other)
        got[p][index(mine)] = held[index(mine)]

    def forward3(p, off):
        a, b, c = ORDERS[p]
        sb = {b: one(at(b, off))}
        hop_sb = {b: one(off % 4)}
        for s, sign in enumerate(SIGNS):
            arrived(p, ("3far", off, s))
            send(p, ("3fwd", off, s), view(hop3[2 * p + s], hop_sb), view(got[p], {**sb, c: one(at(c, -sign)), CORE: one(core)}), device(c, sign, cores[s]))

    def length(j):
        return len_buf[4 * me + j]

    def keys():
        row = lax.broadcasted_iota(jnp.int32, (32, 32), 0)
        diag = row == lax.broadcasted_iota(jnp.int32, (32, 32), 1)
        roped = []
        for pos in range(8):
            cos = jnp.sum(jnp.where(diag, cos_buf[pos : pos + 1, :], 0.0), axis=1, keepdims=True)
            sin = jnp.sum(jnp.where(diag, sin_buf[pos : pos + 1, :], 0.0), axis=1, keepdims=True)
            lo = k_buf[pos, 0:32, :].astype(F32)
            hi = k_buf[pos, 32:64, :].astype(F32)
            roped.append(jnp.concatenate([lo * cos - hi * sin, hi * cos + lo * sin], axis=0).astype(BF16))
        out_row = lax.broadcasted_iota(jnp.int32, (256, 128), 0)
        lane = lax.broadcasted_iota(jnp.int32, (256, 128), 1)
        picks = [jnp.where((out_row % 8 == pos) & (out_row // 8 == lane // 4), 1.0, 0.0).astype(BF16) for pos in range(8)]
        pick = jnp.concatenate(picks, axis=1)
        request = lax.broadcasted_iota(jnp.int32, (64, 1024), 1) % 4
        for z in REQUESTS:
            cat = jnp.concatenate([r[:, 128 * z : 128 * (z + 1)] for r in roped], axis=1)
            masked = jnp.concatenate([jnp.where(request == j, cat, jnp.zeros_like(cat)) for j in REQUESTS], axis=0)
            laid = lax.dot_general(pick, masked, NT, preferred_element_type=F32)
            laid = laid.reshape(1, 4, 4, 2, 8, 256).astype(BF16)
            src[2][z : z + 1, :, :, :, :, 512:768] = laid
        own = {2: one(place[2]), COL: K_COLS}
        mid1[2][index(own)] = src[2][index(own)]

    def queries():
        q_rows[...] = jnp.zeros_like(q_rows)
        for j in REQUESTS:
            q_rows[j, HEADS * j : HEADS * (j + 1), :] = qlat_buf[j]
        zero = jnp.zeros((HEADS, ROPE), BF16)
        qk_rows[...] = jnp.zeros_like(qk_rows)
        for j in REQUESTS:
            qk_rows[HEADS * j : HEADS * (j + 1), :] = jnp.concatenate([qrope_buf[j] if i == j else zero for i in REQUESTS], axis=1)
        score_out[...] = jnp.zeros_like(score_out)
        lane = lax.broadcasted_iota(jnp.int32, (8, LANES), 1)
        lens = jnp.zeros((8, LANES), jnp.int32)
        for j in REQUESTS:
            lens = jnp.where(lane // HEADS == j, length(j), lens)
        len_out[...] = lens

    def row_positions(a, b, c, ib, ic):
        r = lax.broadcasted_iota(jnp.int32, (ROWS, 1), 0)
        return (r // 16) * STRIDES[a] + r % 16 + ib * STRIDES[b] + ic * STRIDES[c]

    def unit_shape(a, width):
        return tuple(4 if d == a else 1 for d in range(3)) + (2, 8, width)

    def finish_rows(j, raw, gain, positions, a, where):
        square = jnp.sum(raw * raw, axis=-1, keepdims=True) * (1.0 / 512)
        inv_rms = jnp.where(positions < length(j), lax.rsqrt(square + NORM_EPS), 0.0)
        c_norm = raw * inv_rms * gain
        c_out[(j,) + where] = c_norm.reshape(unit_shape(a, LATENT)).astype(BF16)
        part = lax.dot_general(c_norm.astype(BF16), q_rows[j], NT, preferred_element_type=F32)
        score_out[where] += part.reshape(unit_shape(a, LANES))

    def gain_row():
        return gain_buf[...].astype(F32).reshape(1, LATENT)

    def unit(p, ib, ic):
        a, b, c = ORDERS[p]
        where = index({b: one(ib), c: one(ic)})[:COL]
        gain = gain_row()
        raw = got[p][where + (pl.ds(*C_COLS),)].astype(F32).reshape(ROWS, LATENT)
        finish_rows(p, raw, gain, row_positions(a, b, c, ib, ic), a, where + (slice(None),))
        if p == 2:
            held = got[2][where + (pl.ds(*K_COLS),)].astype(F32).reshape(ROWS, KEY_COLS).astype(BF16)
            part = lax.dot_general(held, qk_rows[...], NT, preferred_element_type=F32)
            score_out[where + (slice(None),)] += part.reshape(unit_shape(a, LANES))

    def near_units(p, off):
        a, b, c = ORDERS[p]
        arrived(p, ("3core", off), *[("3near", off, s, k) for s in PAIR for k in PAIR])

        @pl.loop(0, 3)
        def _(i):
            unit(p, at(b, off), (place[c] + 3 + i) % 4)

    def far_unit(p, off):
        a, b, c = ORDERS[p]
        arrived(p, ("3fwd", off, 0), ("3fwd", off, 1))
        unit(p, at(b, off), at(c, 2))
        if p == 2:
            key_columns(at(b, off))

    def key_columns(z):
        row = lax.broadcasted_iota(jnp.int32, (KEY_COLS, KEY_COLS), 0)
        col = lax.broadcasted_iota(jnp.int32, (KEY_COLS, KEY_COLS), 1)
        eye = jnp.where(row == col, 1.0, 0.0).astype(BF16)
        held = got[2][pl.ds(z, 1), :, :, :, :, pl.ds(*K_COLS)].astype(F32).reshape(KEY_COLS, KEY_COLS).astype(BF16)
        turned = lax.dot_general(eye, held, NT, preferred_element_type=F32)
        for j in REQUESTS:
            valid = col[:ROPE] + z * KEY_COLS < length(j)
            kr_out[j, :, pl.ds(pl.multiple_of(z * KEY_COLS, KEY_COLS), KEY_COLS)] = jnp.where(valid, turned[ROPE * j : ROPE * (j + 1)], 0.0).astype(BF16)

    def last_request():
        @pl.loop(0, 16)
        def _(i):
            y, x = i // 4, i % 4
            where = index({1: one(y), 2: one(x)})[:COL]
            gain = gain_row()
            raw = [got[p][where + (pl.ds(*K_COLS),)].astype(F32).reshape(ROWS, KEY_COLS) for p in PAIR]
            finish_rows(3, jnp.concatenate(raw, axis=1), gain, row_positions(0, 1, 2, y, x), 0, where + (slice(None),))

    for off in (2, 1, -1):
        for p in PARTS:
            loaded((("src", p, off), 0))
            if p < 2:
                loaded((("src", p, off), 1))
    pl.semaphore_wait(barrier, 13)
    phase1(0)
    phase1(1)
    phase1(2, C_COLS)
    loaded("k", "cos", "sin")
    keys()
    loaded("gain", "len", "qlat", "qrope")
    queries()
    phase1(2, K_COLS)
    for p in PARTS:
        loaded((("own", p), 0))
        if p < 2:
            loaded((("own", p), 1))
    forward1(0)
    forward1(1)
    forward1(2, C_COLS)
    for p in PARTS:
        phase2(p, 0)
    forward1(2, K_COLS)
    for p in PARTS:
        arrived1(p, "1near")
        phase2(p, -1)
        phase2(p, 1)
    for p in PARTS:
        forward2(p, 0)
    for p in PARTS:
        arrived1(p, "1fwd")
        phase2(p, 2)
    for p in PARTS:
        forward2(p, -1)
        forward2(p, 1)
    for p in PARTS:
        forward2(p, 2)
        phase3(p, 0)
    for p in PARTS:
        for off in OFFSETS:
            arrived(p, ("2near", off, 0), ("2near", off, 1))
        phase3(p, -1)
    for p in PARTS:
        forward3(p, 0)
        phase3(p, 1)
    for p in PARTS:
        near_units(p, 0)
    for p in PARTS:
        for off in OFFSETS:
            arrived(p, ("2fwd", off, 0), ("2fwd", off, 1))
        forward3(p, -1)
        phase3(p, 2)
    for p in PARTS:
        near_units(p, -1)
        far_unit(p, 0)
    for p in PARTS:
        forward3(p, 1)
    for p in PARTS:
        near_units(p, 1)
        far_unit(p, -1)
    for p in PARTS:
        forward3(p, 2)
    for p in PARTS:
        near_units(p, 2)
        far_unit(p, 1)
    for p in PARTS:
        far_unit(p, 2)
    last_request()
    for p in PARTS:
        for copy in copies[p].values():
            copy.wait_send()


def exchange(c_raw, k_turned, rope_cos, rope_sin, gain, seq_lens, q_lat, q_rope):
    def shaped(sizes):
        return pltpu.VMEM(tuple(sizes.get(d, FULL[d]) for d in range(6)), BF16)

    hop1 = [shaped({o[0]: 1, o[1]: 2}) for o in ORDERS for _ in PAIR]
    hop2 = [shaped({o[1]: 1, o[2]: 2}) for o in ORDERS for _ in PAIR]
    hop3 = [shaped({o[2]: 1, 3: 1}) for o in ORDERS for _ in PAIR]
    small = [
        pltpu.VMEM((8, 64, 512), BF16),
        pltpu.VMEM((8, 32), F32),
        pltpu.VMEM((8, 32), F32),
        pltpu.VMEM((LATENT,), BF16),
        pltpu.SMEM((REQ,), jnp.int32),
        pltpu.VMEM((4, 16, 512), BF16),
        pltpu.VMEM((4, 16, 64), BF16),
        pltpu.VMEM((4, 128, 512), BF16),
        pltpu.VMEM((128, 256), BF16),
    ]
    sems = [pltpu.SemaphoreType.DMA((LOADS,)), pltpu.SemaphoreType.DMA((3, COPIES)), pltpu.SemaphoreType.DMA((3, COPIES))]
    return pl.pallas_call(
        exchange_kernel,
        out_shape=[
            pltpu.VMEM((4, 4, 4, 4, 2, 8, 512), BF16),
            pltpu.VMEM((4, 64, 1024), BF16),
            pltpu.VMEM((4, 4, 4, 2, 8, 128), F32),
            pltpu.VMEM((8, LANES), jnp.int32),
        ],
        in_specs=[pl.BlockSpec(memory_space=pltpu.HBM)] * 8,
        out_specs=[pl.BlockSpec(memory_space=pltpu.VMEM)] * 4,
        scratch_shapes=[[[shaped({})] * 3] * 4 + [hop1, hop2, hop3, small, sems]],
        compiler_params=pltpu.CompilerParams(collective_id=0, has_side_effects=True, vmem_limit_bytes=40 * 1024 * 1024),
        name="exchange",
    )(c_raw, k_turned, rope_cos, rope_sin, gain, seq_lens, q_lat, q_rope)


def attend_kernel(c_ref, kr_ref, score_ref, len_ref, c_out, kr_out, o_ref, sem):
    writes = [pltpu.make_async_copy(c_ref, c_out, sem.at[0]), pltpu.make_async_copy(kr_ref, kr_out, sem.at[1])]
    for write in writes:
        write.start()
    row = lax.broadcasted_iota(jnp.int32, (POSITIONS, LANES), 0)
    scores = jnp.where(row < len_ref[0:1, :], score_ref[...] * ATTN_SCALE, -1e30)
    weights = jnp.exp(scores - jnp.max(scores, axis=0, keepdims=True)).T
    weight_sum = jnp.sum(weights[: 4 * HEADS], axis=1, keepdims=True)
    rounded = weights[: 4 * HEADS].astype(BF16)
    for j in REQUESTS:
        mine = slice(HEADS * j, HEADS * (j + 1))
        weighted = jnp.dot(rounded[mine], c_ref[j], preferred_element_type=F32)
        o_ref[j] = (weighted / weight_sum[mine]).astype(BF16)
    for write in writes:
        write.wait()


def attend(c_cache, kr_turned, scores, lens):
    whole = pl.BlockSpec(memory_space=pltpu.VMEM)
    return pl.pallas_call(
        attend_kernel,
        out_shape=[
            jax.ShapeDtypeStruct(c_cache.shape, BF16),
            jax.ShapeDtypeStruct(kr_turned.shape, BF16),
            jax.ShapeDtypeStruct((4, HEADS, LATENT), BF16),
        ],
        in_specs=[whole] * 4,
        out_specs=[pl.BlockSpec(memory_space=pltpu.HBM)] * 2 + [whole],
        scratch_shapes=[pltpu.SemaphoreType.DMA((2,))],
        compiler_params=pltpu.CompilerParams(vmem_limit_bytes=24 * 1024 * 1024),
        name="attend",
    )(c_cache, kr_turned, scores, lens)


def solution(mesh):
    seq_spec = P("dp", "x", None)
    req_spec = P(("dp", "x"), None, None)

    def local_step(c_raw, k_raw, norm_gain, rope_cos, rope_sin, seq_lens, q_lat, q_rope):
        args = (c_raw.reshape(FULL[:4] + (4, 8, LATENT)), k_raw.transpose(1, 2, 0), rope_cos, rope_sin, norm_gain, seq_lens, q_lat, q_rope)
        c_cache, kr_turned, scores, lens = exchange(*[pltpu.with_memory_space_constraint(arg, pltpu.HBM) for arg in args])
        c_cache, kr_turned, o_lat = attend(c_cache.reshape(4, POSITIONS, LATENT), kr_turned, scores.reshape(POSITIONS, LANES), lens)
        return c_cache, kr_turned.transpose(0, 2, 1), o_lat

    return jax.shard_map(local_step, mesh=mesh, in_specs=(seq_spec, seq_spec, P(None), P("x", None), P("x", None), P("dp"), req_spec, req_spec), out_specs=(req_spec, req_spec, req_spec), check_vma=False)
```

```python
import jax
import jax.numpy as jnp
from jax import lax
from jax.experimental import pallas as pl
from jax.experimental.pallas import tpu as pltpu
from jax.sharding import PartitionSpec as P

NORM_EPS = 1e-6
ATTN_SCALE = (512 + 64) ** -0.5
ORDERS = ((0, 1, 2), (1, 2, 0), (2, 0, 1))
FULL = (4, 4, 4, 2, 8, 768)
STRIDES = (256, 64, 16)
POSITIONS, LATENT, ROPE, HEADS, LANES = 1024, 512, 64, 16, 128
ROWS = 64
KEY_COLS = 256
C_COLS, K_COLS, ALL_COLS = (0, LATENT), (LATENT, KEY_COLS), (0, LATENT + KEY_COLS)
CORE, COL = 3, 5
PARTS = range(3)
PAIR = range(2)
REQUESTS = range(4)
REQ = 512
GROUPS = 28
LOADS = 16
SCORE_PARTS = 5
SIGNS = (1, -1)
OFFSETS = (0, -1, 1, 2)
NT = (((1,), (1,)), ((), ()))
F32, BF16 = jnp.float32, jnp.bfloat16


def exchange_kernel(c_ref, k_ref, cos_ref, sin_ref, gain_ref, len_ref, qlat_ref, qrope_ref, c_out, kr_out, score_out, len_out, scratch):
    src, mid1, mid2, got, hop1, hop2, hop3, small, sems = scratch
    k_buf, cos_buf, sin_buf, gain_buf, len_buf, qlat_buf, qrope_buf, q_rows, qk_rows = small
    load_sem, send_sem, recv_sem = sems

    me = lax.axis_index("x")
    core = me % 2
    other = me + 1 - 2 * core
    cores = (core, 1 - core)
    place = (me // 32, (me // 8) % 4, (me // 2) % 4)

    def device(dim, delta, to_core=None):
        pos = list(place)
        pos[dim] = (pos[dim] + delta + 4) % 4
        last = core if to_core is None else to_core
        return ((pos[0] * 4 + pos[1]) * 4 + pos[2]) * 2 + last

    def at(dim, delta):
        return (place[dim] + delta + 4) % 4

    def index(sel, dims=len(FULL)):
        return tuple(pl.ds(*sel[d]) if d in sel else slice(None) for d in range(dims))

    def one(i):
        return (i, 1)

    def halves(s):
        return (2 * s, 2)

    def view(ref, sel):
        return ref.at[index(sel)]

    barrier = pltpu.get_barrier_semaphore()
    for dim in PARTS:
        for delta in SIGNS:
            for k in PAIR:
                pl.semaphore_signal(barrier, inc=1, device_id={"x": device(dim, delta, k)}, device_id_type=pl.DeviceIdType.MESH)
    pl.semaphore_signal(barrier, inc=1, device_id={"x": other}, device_id_type=pl.DeviceIdType.MESH)

    load_slots = {}

    def load(key, a, b):
        slot = load_slots.setdefault(key, len(load_slots))
        copy = pltpu.make_async_copy(a, b, load_sem.at[slot])
        copy.start()
        return copy

    def load_slab(p, off, into, key):
        a = ORDERS[p][0]
        sel = {a: one(at(a, off))}
        rows = index(sel, COL - 1)
        load(key, c_ref.at[rows + (p, slice(None), pl.ds(*C_COLS))], view(into, {**sel, COL: C_COLS}))
        if p < 2:
            load(key, c_ref.at[rows + (3, slice(None), pl.ds(KEY_COLS * p, KEY_COLS))], view(into, {**sel, COL: K_COLS}))

    def taken(sem, shape):
        pltpu.make_async_copy(view(got[0], shape), view(got[0], shape), sem).wait()

    def slabs(p, n):
        return {ORDERS[p][0]: (0, n), COL: ALL_COLS if p < 2 else C_COLS}

    def loaded(key, p, n):
        taken(load_sem.at[load_slots[key, p]], slabs(p, n))

    key_loads = [load("k", k_ref, k_buf), load("cos", cos_ref, cos_buf), load("sin", sin_ref, sin_buf)]
    for p in PARTS:
        load_slab(p, 2, src[p], ("far", p))
    for p in PARTS:
        for sign in SIGNS:
            load_slab(p, sign, src[p], ("near", p))
    for p in PARTS:
        load_slab(p, 0, mid1[p], ("own", p))
    other_loads = [load("gain", gain_ref, gain_buf), load("len", len_ref, len_buf), load("qlat", qlat_ref, qlat_buf), load("qrope", qrope_ref, qrope_buf)]

    slots = [{} for _ in PARTS]

    def send(p, group, a, b, to, sent):
        slot = slots[p].setdefault(group, len(slots[p]))
        pltpu.make_async_remote_copy(src_ref=a, dst_ref=b, send_sem=send_sem.at[p, sent], recv_sem=recv_sem.at[p, slot], device_id={"x": to}, device_id_type=pl.DeviceIdType.MESH).start()

    def arrived(p, group, shape):
        taken(recv_sem.at[p, slots[p][group]], shape)

    def far1(p, cols=ALL_COLS):
        a, b, _ = ORDERS[p]
        wide = {COL: cols}
        for s, sign in enumerate(SIGNS):
            send(p, ("1far", cols), view(src[p], {a: one(at(a, 2)), b: halves(s), **wide}), view(hop1[2 * p + s], wide), device(a, sign), 0)

    def near1(p, cols=ALL_COLS):
        a, b, _ = ORDERS[p]
        wide = {COL: cols}
        for s, sign in enumerate(SIGNS):
            send(p, ("1near", cols), view(src[p], {a: one(at(a, sign)), **wide}), view(mid1[p], {a: one(place[a]), **wide}), device(a, sign), 0)

    def forward1(p, cols=ALL_COLS):
        a, b, _ = ORDERS[p]
        wide = {COL: cols}
        arrived(p, ("1far", cols), {a: one(0), **wide})
        for s, sign in enumerate(SIGNS):
            send(p, ("1fwd", cols), view(hop1[2 * p + s], wide), view(mid1[p], {a: one(at(a, -sign)), b: halves(s), **wide}), device(a, sign), 0)

    def arrived1(p, kind, n):
        for cols in (ALL_COLS,) if p < 2 else (C_COLS, K_COLS):
            arrived(p, (kind, cols), {ORDERS[p][0]: (0, n), COL: cols})

    def phase2(p, off):
        a, b, c = ORDERS[p]
        sa = {a: one(at(a, off))}
        hop_sa = {a: one(off % 4)}
        for s, sign in enumerate(SIGNS):
            send(p, ("2far", off), view(mid1[p], {**sa, b: one(at(b, 2)), c: halves(s)}), view(hop2[2 * p + s], hop_sa), device(b, sign), 1)
        for s, sign in enumerate(SIGNS):
            send(p, "2near", view(mid1[p], {**sa, b: one(at(b, sign))}), view(mid2[p], {**sa, b: one(place[b])}), device(b, sign), 1)

    def forward2(p, off):
        a, b, c = ORDERS[p]
        sa = {a: one(at(a, off))}
        hop_sa = {a: one(off % 4)}
        arrived(p, ("2far", off), {a: one(0), b: one(0)})
        for s, sign in enumerate(SIGNS):
            send(p, "2fwd", view(hop2[2 * p + s], hop_sa), view(mid2[p], {**sa, b: one(at(b, -sign)), c: halves(s)}), device(b, sign), 1)

    def phase3(p, off):
        a, b, c = ORDERS[p]
        sb = {b: one(at(b, off))}
        hop_sb = {b: one(off % 4)}
        held = mid1[p] if off == 0 else mid2[p]
        mine = {**sb, c: one(place[c]), CORE: one(core)}
        for s, sign in enumerate(SIGNS):
            send(p, ("3far", off), view(held, {**sb, c: one(at(c, 2)), CORE: one(cores[s])}), view(hop3[2 * p + s], hop_sb), device(c, sign), 2)
        for s, sign in enumerate(SIGNS):
            for k in PAIR:
                send(p, ("3near", off), view(held, {**sb, c: one(at(c, sign)), CORE: one(cores[k])}), view(got[p], mine), device(c, sign, cores[k]), 2)
        send(p, ("3core", off), view(held, {**sb, c: one(place[c]), CORE: one(cores[1])}), view(got[p], mine), other, 3)
        got[p][index(mine)] = held[index(mine)]

    def forward3(p, off):
        a, b, c = ORDERS[p]
        sb = {b: one(at(b, off))}
        hop_sb = {b: one(off % 4)}
        arrived(p, ("3far", off), {b: one(0), c: one(0)})
        for s, sign in enumerate(SIGNS):
            send(p, ("3fwd", off), view(hop3[2 * p + s], hop_sb), view(got[p], {**sb, c: one(at(c, -sign)), CORE: one(core)}), device(c, sign, cores[s]), 2)

    def length(j):
        return len_buf[4 * me + j]

    def keys():
        row = lax.broadcasted_iota(jnp.int32, (32, 32), 0)
        diag = row == lax.broadcasted_iota(jnp.int32, (32, 32), 1)
        roped = []
        for pos in range(8):
            cos = jnp.sum(jnp.where(diag, cos_buf[pos : pos + 1, :], 0.0), axis=1, keepdims=True)
            sin = jnp.sum(jnp.where(diag, sin_buf[pos : pos + 1, :], 0.0), axis=1, keepdims=True)
            lo = k_buf[pos, 0:32, :].astype(F32)
            hi = k_buf[pos, 32:64, :].astype(F32)
            roped.append(jnp.concatenate([lo * cos - hi * sin, hi * cos + lo * sin], axis=0).astype(BF16))
        out_row = lax.broadcasted_iota(jnp.int32, (256, 128), 0)
        lane = lax.broadcasted_iota(jnp.int32, (256, 128), 1)
        picks = [jnp.where((out_row % 8 == pos) & (out_row // 8 == lane // 4), 1.0, 0.0).astype(BF16) for pos in range(8)]
        pick = jnp.concatenate(picks, axis=1)
        request = lax.broadcasted_iota(jnp.int32, (64, 1024), 1) % 4
        for z in REQUESTS:
            cat = jnp.concatenate([r[:, 128 * z : 128 * (z + 1)] for r in roped], axis=1)
            masked = jnp.concatenate([jnp.where(request == j, cat, jnp.zeros_like(cat)) for j in REQUESTS], axis=0)
            laid = lax.dot_general(pick, masked, NT, preferred_element_type=F32)
            laid = laid.reshape(1, 4, 4, 2, 8, 256).astype(BF16)
            src[2][z : z + 1, :, :, :, :, 512:768] = laid
        own = {2: one(place[2]), COL: K_COLS}
        mid1[2][index(own)] = src[2][index(own)]

    def queries():
        q_rows[...] = jnp.zeros_like(q_rows)
        for j in REQUESTS:
            q_rows[j, HEADS * j : HEADS * (j + 1), :] = qlat_buf[j]
        zero = jnp.zeros((HEADS, ROPE), BF16)
        qk_rows[...] = jnp.zeros_like(qk_rows)
        for j in REQUESTS:
            qk_rows[HEADS * j : HEADS * (j + 1), :] = jnp.concatenate([qrope_buf[j] if i == j else zero for i in REQUESTS], axis=1)
        lane = lax.broadcasted_iota(jnp.int32, (8, LANES), 1)
        lens = jnp.zeros((8, LANES), jnp.int32)
        for j in REQUESTS:
            lens = jnp.where(lane // HEADS == j, length(j), lens)
        len_out[...] = lens

    def row_positions(a, b, c, ib, ic):
        r = lax.broadcasted_iota(jnp.int32, (ROWS, 1), 0)
        return (r // 16) * STRIDES[a] + r % 16 + ib * STRIDES[b] + ic * STRIDES[c]

    def unit_shape(a, width):
        return tuple(4 if d == a else 1 for d in range(3)) + (2, 8, width)

    def finish_rows(j, raw, gain, positions, a, where):
        square = jnp.sum(raw * raw, axis=-1, keepdims=True) * (1.0 / 512)
        inv_rms = jnp.where(positions < length(j), lax.rsqrt(square + NORM_EPS), 0.0)
        c_norm = raw * inv_rms * gain
        c_out[(j,) + where] = c_norm.reshape(unit_shape(a, LATENT)).astype(BF16)
        part = lax.dot_general(c_norm.astype(BF16), q_rows[j], NT, preferred_element_type=F32)
        score_out[(j,) + where] = part.reshape(unit_shape(a, LANES))

    def gain_row():
        return gain_buf[...].astype(F32).reshape(1, LATENT)

    def unit(p, ib, ic):
        a, b, c = ORDERS[p]
        where = index({b: one(ib), c: one(ic)})[:COL]
        gain = gain_row()
        raw = got[p][where + (pl.ds(*C_COLS),)].astype(F32).reshape(ROWS, LATENT)
        finish_rows(p, raw, gain, row_positions(a, b, c, ib, ic), a, where + (slice(None),))
        if p == 2:
            held = got[2][where + (pl.ds(*K_COLS),)].astype(F32).reshape(ROWS, KEY_COLS).astype(BF16)
            part = lax.dot_general(held, qk_rows[...], NT, preferred_element_type=F32)
            score_out[(4,) + where + (slice(None),)] = part.reshape(unit_shape(a, LANES))

    def near_units(p, off):
        a, b, c = ORDERS[p]
        arrived(p, ("3near", off), {b: one(0), c: (0, 2)})
        arrived(p, ("3core", off), {b: one(0), c: one(0), CORE: one(0)})
        for step in OFFSETS[:3]:
            unit(p, at(b, off), at(c, step))

    def far_unit(p, off):
        a, b, c = ORDERS[p]
        arrived(p, ("3fwd", off), {b: one(0), c: one(0)})
        unit(p, at(b, off), at(c, 2))
        if p == 2:
            key_columns(at(b, off))

    def key_columns(z):
        row = lax.broadcasted_iota(jnp.int32, (KEY_COLS, KEY_COLS), 0)
        col = lax.broadcasted_iota(jnp.int32, (KEY_COLS, KEY_COLS), 1)
        eye = jnp.where(row == col, 1.0, 0.0).astype(BF16)
        held = got[2][pl.ds(z, 1), :, :, :, :, pl.ds(*K_COLS)].astype(F32).reshape(KEY_COLS, KEY_COLS).astype(BF16)
        turned = lax.dot_general(eye, held, NT, preferred_element_type=F32)
        for j in REQUESTS:
            valid = col[:ROPE] + z * KEY_COLS < length(j)
            kr_out[j, :, pl.ds(pl.multiple_of(z * KEY_COLS, KEY_COLS), KEY_COLS)] = jnp.where(valid, turned[ROPE * j : ROPE * (j + 1)], 0.0).astype(BF16)

    def last_request(blocks):
        for off_y, off_x in blocks:
            y, x = at(1, off_y), at(2, off_x)
            where = index({1: one(y), 2: one(x)})[:COL]
            gain = gain_row()
            raw = [got[p][where + (pl.ds(*K_COLS),)].astype(F32).reshape(ROWS, KEY_COLS) for p in PAIR]
            finish_rows(3, jnp.concatenate(raw, axis=1), gain, row_positions(0, 1, 2, y, x), 0, where + (slice(None),))

    def blocks(n):
        inner = OFFSETS[: n - 1]
        return [(y, x) for y in OFFSETS[:n] for x in OFFSETS[:n] if y not in inner or x not in inner]

    for p in PARTS:
        loaded("far", p, 1)
    pl.semaphore_wait(barrier, 13)
    far1(0)
    far1(1)
    far1(2, C_COLS)
    for p in PARTS:
        loaded("near", p, 2)
        near1(p, ALL_COLS if p < 2 else C_COLS)
    for copy in key_loads:
        copy.wait()
    keys()
    for copy in other_loads:
        copy.wait()
    queries()
    far1(2, K_COLS)
    near1(2, K_COLS)
    for p in PARTS:
        loaded("own", p, 1)
    forward1(0)
    forward1(1)
    forward1(2, C_COLS)
    for p in PARTS:
        phase2(p, 0)
    forward1(2, K_COLS)
    for p in PARTS:
        arrived1(p, "1near", 2)
        phase2(p, -1)
        phase2(p, 1)
    for p in PARTS:
        forward2(p, 0)
    for p in PARTS:
        arrived1(p, "1fwd", 1)
        phase2(p, 2)
    for p in PARTS:
        forward2(p, -1)
        forward2(p, 1)
    for p in PARTS:
        forward2(p, 2)
        phase3(p, 0)
    for p in PARTS:
        arrived(p, "2near", {ORDERS[p][1]: (0, 2)})
        phase3(p, -1)
    for p in PARTS:
        forward3(p, 0)
        phase3(p, 1)
    for p in PARTS:
        near_units(p, 0)
    for p in PARTS:
        arrived(p, "2fwd", {ORDERS[p][1]: one(0)})
        forward3(p, -1)
        phase3(p, 2)
    for p in PARTS:
        near_units(p, -1)
        far_unit(p, 0)
    for p in PARTS:
        forward3(p, 1)
    for p in PARTS:
        near_units(p, 1)
        far_unit(p, -1)
    last_request(blocks(1) + blocks(2))
    for p in PARTS:
        forward3(p, 2)
    for p in PARTS:
        near_units(p, 2)
        far_unit(p, 1)
    last_request(blocks(3))
    for p in PARTS:
        far_unit(p, 2)
    last_request(blocks(4))
    for p in PARTS:
        c = ORDERS[p][2]
        for phase in PARTS:
            taken(send_sem.at[p, phase], {})
        taken(send_sem.at[p, 3], {c: one(0), CORE: one(0)})


def exchange(c_raw, k_turned, rope_cos, rope_sin, gain, seq_lens, q_lat, q_rope):
    def shaped(sizes):
        return pltpu.VMEM(tuple(sizes.get(d, FULL[d]) for d in range(6)), BF16)

    hop1 = [shaped({o[0]: 1, o[1]: 2}) for o in ORDERS for _ in PAIR]
    hop2 = [shaped({o[1]: 1, o[2]: 2}) for o in ORDERS for _ in PAIR]
    hop3 = [shaped({o[2]: 1, 3: 1}) for o in ORDERS for _ in PAIR]
    small = [
        pltpu.VMEM((8, 64, 512), BF16),
        pltpu.VMEM((8, 32), F32),
        pltpu.VMEM((8, 32), F32),
        pltpu.VMEM((LATENT,), BF16),
        pltpu.SMEM((REQ,), jnp.int32),
        pltpu.VMEM((4, 16, 512), BF16),
        pltpu.VMEM((4, 16, 64), BF16),
        pltpu.VMEM((4, 128, 512), BF16),
        pltpu.VMEM((128, 256), BF16),
    ]
    sems = [pltpu.SemaphoreType.DMA((LOADS,)), pltpu.SemaphoreType.DMA((3, 4)), pltpu.SemaphoreType.DMA((3, GROUPS))]
    return pl.pallas_call(
        exchange_kernel,
        out_shape=[
            pltpu.VMEM((4, 4, 4, 4, 2, 8, 512), BF16),
            pltpu.VMEM((4, 64, 1024), BF16),
            pltpu.VMEM((SCORE_PARTS,) + FULL[:COL] + (LANES,), F32),
            pltpu.VMEM((8, LANES), jnp.int32),
        ],
        in_specs=[pl.BlockSpec(memory_space=pltpu.HBM)] * 8,
        out_specs=[pl.BlockSpec(memory_space=pltpu.VMEM)] * 4,
        scratch_shapes=[[[shaped({})] * 3] * 4 + [hop1, hop2, hop3, small, sems]],
        compiler_params=pltpu.CompilerParams(collective_id=0, has_side_effects=True, vmem_limit_bytes=40 * 1024 * 1024),
        name="exchange",
    )(c_raw, k_turned, rope_cos, rope_sin, gain, seq_lens, q_lat, q_rope)


def attend_kernel(c_ref, kr_ref, score_ref, len_ref, c_out, kr_out, o_ref, sem):
    writes = [pltpu.make_async_copy(c_ref, c_out, sem.at[0]), pltpu.make_async_copy(kr_ref, kr_out, sem.at[1])]
    for write in writes:
        write.start()
    row = lax.broadcasted_iota(jnp.int32, (POSITIONS, LANES), 0)
    scores = jnp.where(row < len_ref[0:1, :], jnp.sum(score_ref[...], axis=0) * ATTN_SCALE, -1e30)
    weights = jnp.exp(scores - jnp.max(scores, axis=0, keepdims=True)).T
    weight_sum = jnp.sum(weights[: 4 * HEADS], axis=1, keepdims=True)
    rounded = weights[: 4 * HEADS].astype(BF16)
    for j in REQUESTS:
        mine = slice(HEADS * j, HEADS * (j + 1))
        weighted = jnp.dot(rounded[mine], c_ref[j], preferred_element_type=F32)
        o_ref[j] = (weighted / weight_sum[mine]).astype(BF16)
    for write in writes:
        write.wait()


def attend(c_cache, kr_turned, scores, lens):
    whole = pl.BlockSpec(memory_space=pltpu.VMEM)
    return pl.pallas_call(
        attend_kernel,
        out_shape=[
            jax.ShapeDtypeStruct(c_cache.shape, BF16),
            jax.ShapeDtypeStruct(kr_turned.shape, BF16),
            jax.ShapeDtypeStruct((4, HEADS, LATENT), BF16),
        ],
        in_specs=[whole] * 4,
        out_specs=[pl.BlockSpec(memory_space=pltpu.HBM)] * 2 + [whole],
        scratch_shapes=[pltpu.SemaphoreType.DMA((2,))],
        compiler_params=pltpu.CompilerParams(vmem_limit_bytes=24 * 1024 * 1024),
        name="attend",
    )(c_cache, kr_turned, scores, lens)


def solution(mesh):
    seq_spec = P("dp", "x", None)
    req_spec = P(("dp", "x"), None, None)

    def local_step(c_raw, k_raw, norm_gain, rope_cos, rope_sin, seq_lens, q_lat, q_rope):
        args = (c_raw.reshape(FULL[:4] + (4, 8, LATENT)), k_raw.transpose(1, 2, 0), rope_cos, rope_sin, norm_gain, seq_lens, q_lat, q_rope)
        c_cache, kr_turned, scores, lens = exchange(*[pltpu.with_memory_space_constraint(arg, pltpu.HBM) for arg in args])
        c_cache, kr_turned, o_lat = attend(c_cache.reshape(4, POSITIONS, LATENT), kr_turned, scores.reshape(SCORE_PARTS, POSITIONS, LANES), lens)
        return c_cache, kr_turned.transpose(0, 2, 1), o_lat

    return jax.shard_map(local_step, mesh=mesh, in_specs=(seq_spec, seq_spec, P(None), P("x", None), P("x", None), P("dp"), req_spec, req_spec), out_specs=(req_spec, req_spec, req_spec), check_vma=False)
```

```python
import jax
import jax.numpy as jnp
from jax import lax
from jax.experimental import pallas as pl
from jax.experimental.pallas import tpu as pltpu
from jax.sharding import PartitionSpec as P

NORM_EPS = 1e-6
ATTN_SCALE = (512 + 64) ** -0.5
ORDERS = ((0, 1, 2), (1, 2, 0), (2, 0, 1))
FULL = (4, 4, 4, 2, 8, 768)
STRIDES = (256, 64, 16)
POSITIONS, LATENT, ROPE, HEADS, LANES = 1024, 512, 64, 16, 128
ROWS = 64
KEY_COLS = 256
C_COLS, K_COLS, ALL_COLS = (0, LATENT), (LATENT, KEY_COLS), (0, LATENT + KEY_COLS)
CORE, COL = 3, 5
PARTS = range(3)
PAIR = range(2)
REQUESTS = range(4)
REQ = 512
GROUPS = 23
LOADS = 9
SCORE_PARTS = 5
SIGNS = (1, -1)
OFFSETS = (0, -1, 1, 2)
NT = (((1,), (1,)), ((), ()))
F32, BF16 = jnp.float32, jnp.bfloat16


def exchange_kernel(c_ref, k_ref, cos_ref, sin_ref, gain_ref, len_ref, qlat_ref, qrope_ref, c_out, kr_out, score_out, len_out, scratch):
    parts, k_laid, hop1, hop2, hop3, small, sems = scratch
    mid1, mid2, got = [[parts.at[3 * stage + p] for p in PARTS] for stage in PARTS]
    k_buf, cos_buf, sin_buf, gain_buf, len_buf, qlat_buf, qrope_buf, q_rows, qk_rows = small
    load_sem, send_sem, recv_sem = sems

    me = lax.axis_index("x")
    core = me % 2
    other = me + 1 - 2 * core
    cores = (core, 1 - core)
    place = (me // 32, (me // 8) % 4, (me // 2) % 4)

    def device(dim, delta, to_core=None):
        pos = list(place)
        pos[dim] = (pos[dim] + delta + 4) % 4
        last = core if to_core is None else to_core
        return ((pos[0] * 4 + pos[1]) * 4 + pos[2]) * 2 + last

    def at(dim, delta):
        return (place[dim] + delta + 4) % 4

    def index(sel, dims=len(FULL)):
        return tuple(pl.ds(*sel[d]) if d in sel else slice(None) for d in range(dims))

    def one(i):
        return (i, 1)

    def halves(s):
        return (2 * s, 2)

    def view(ref, sel):
        return ref.at[index(sel)]

    barrier = pltpu.get_barrier_semaphore()
    for dim in PARTS:
        for delta in SIGNS:
            for k in PAIR:
                pl.semaphore_signal(barrier, inc=1, device_id={"x": device(dim, delta, k)}, device_id_type=pl.DeviceIdType.MESH)
    pl.semaphore_signal(barrier, inc=1, device_id={"x": other}, device_id_type=pl.DeviceIdType.MESH)

    def taken(sem, n, shape):
        block = parts.at[(pl.ds(0, n),) + index(shape)]
        pltpu.make_async_copy(block, block, sem).wait()

    def taken_from(p, sel, extra):
        where = index(sel, COL - 1)
        if extra:
            return c_ref.at[where + (3, slice(None), pl.ds(KEY_COLS * p, KEY_COLS))]
        return c_ref.at[where + (p, slice(None), pl.ds(*C_COLS))]

    def load(slot, a, b):
        copy = pltpu.make_async_copy(a, b, load_sem.at[slot])
        copy.start()
        return copy

    key_loads = [load(i, a, b) for i, (a, b) in enumerate(((k_ref, k_buf), (cos_ref, cos_buf), (sin_ref, sin_buf)))]
    other_loads = [load(3 + i, a, b) for i, (a, b) in enumerate(((gain_ref, gain_buf), (len_ref, len_buf), (qlat_ref, qlat_buf), (qrope_ref, qrope_buf)))]
    for p in PARTS:
        own = {ORDERS[p][0]: one(place[ORDERS[p][0]])}
        load(LOADS - 1 if p == 2 else LOADS - 2, taken_from(p, own, False), view(mid1[p], {**own, COL: C_COLS}))
        if p < 2:
            load(LOADS - 2, taken_from(p, own, True), view(mid1[p], {**own, COL: K_COLS}))

    slots = {}

    def send(group, a, b, to, sent=0):
        slot = slots.setdefault(group, len(slots))
        pltpu.make_async_remote_copy(src_ref=a, dst_ref=b, send_sem=send_sem.at[sent], recv_sem=recv_sem.at[slot], device_id={"x": to}, device_id_type=pl.DeviceIdType.MESH).start()

    def arrived(group, n, shape):
        taken(recv_sem.at[slots[group]], n, shape)

    def held(p, sel, cols):
        if cols == C_COLS:
            return taken_from(p, sel, False)
        return taken_from(p, sel, True) if p < 2 else view(k_laid, sel)

    def first_group(p, cols):
        return ("1far", cols if p == 2 else None)

    def far1(p, cols):
        a, b, _ = ORDERS[p]
        wide = {COL: cols}
        for s, sign in enumerate(SIGNS):
            send(first_group(p, cols), held(p, {a: one(at(a, 2)), b: halves(s)}, cols), view(hop1[2 * p + s], wide), device(a, sign))

    def near1(p, cols):
        a, b, _ = ORDERS[p]
        wide = {COL: cols}
        for s, sign in enumerate(SIGNS):
            send("1near", held(p, {a: one(at(a, sign))}, cols), view(mid1[p], {a: one(place[a]), **wide}), device(a, sign))

    def forward1(p, cols=ALL_COLS):
        a, b, _ = ORDERS[p]
        wide = {COL: cols}
        for s, sign in enumerate(SIGNS):
            send("1fwd", view(hop1[2 * p + s], wide), view(mid1[p], {a: one(at(a, -sign)), b: halves(s), **wide}), device(a, sign))

    def phase2(p, off):
        a, b, c = ORDERS[p]
        sa = {a: one(at(a, off))}
        hop_sa = {a: one(off % 4)}
        for s, sign in enumerate(SIGNS):
            send(("2far", off), view(mid1[p], {**sa, b: one(at(b, 2)), c: halves(s)}), view(hop2[2 * p + s], hop_sa), device(b, sign))
        for s, sign in enumerate(SIGNS):
            send("2near", view(mid1[p], {**sa, b: one(at(b, sign))}), view(mid2[p], {**sa, b: one(place[b])}), device(b, sign))

    def forward2(p, off):
        a, b, c = ORDERS[p]
        sa = {a: one(at(a, off))}
        hop_sa = {a: one(off % 4)}
        for s, sign in enumerate(SIGNS):
            send("2fwd", view(hop2[2 * p + s], hop_sa), view(mid2[p], {**sa, b: one(at(b, -sign)), c: halves(s)}), device(b, sign))

    def phase3(p, off):
        a, b, c = ORDERS[p]
        sb = {b: one(at(b, off))}
        hop_sb = {b: one(off % 4)}
        got_b = mid1[p] if off == 0 else mid2[p]
        mine = {**sb, c: one(place[c]), CORE: one(core)}
        for s, sign in enumerate(SIGNS):
            send(("3far", off), view(got_b, {**sb, c: one(at(c, 2)), CORE: one(cores[s])}), view(hop3[2 * p + s], hop_sb), device(c, sign))
        for s, sign in enumerate(SIGNS):
            for k in PAIR:
                send(("3near", off), view(got_b, {**sb, c: one(at(c, sign)), CORE: one(cores[k])}), view(got[p], mine), device(c, sign, cores[k]))
        send(("3near", off), view(got_b, {**sb, c: one(place[c]), CORE: one(cores[1])}), view(got[p], mine), other, 1)
        got[p][index(mine)] = got_b[index(mine)]

    def forward3(p, off):
        a, b, c = ORDERS[p]
        sb = {b: one(at(b, off))}
        hop_sb = {b: one(off % 4)}
        for s, sign in enumerate(SIGNS):
            send(("3fwd", off), view(hop3[2 * p + s], hop_sb), view(got[p], {**sb, c: one(at(c, -sign)), CORE: one(core)}), device(c, sign, cores[s]))

    def length(j):
        return len_buf[4 * me + j]

    def keys():
        row = lax.broadcasted_iota(jnp.int32, (32, 32), 0)
        diag = row == lax.broadcasted_iota(jnp.int32, (32, 32), 1)
        roped = []
        for pos in range(8):
            cos = jnp.sum(jnp.where(diag, cos_buf[pos : pos + 1, :], 0.0), axis=1, keepdims=True)
            sin = jnp.sum(jnp.where(diag, sin_buf[pos : pos + 1, :], 0.0), axis=1, keepdims=True)
            lo = k_buf[pos, 0:32, :].astype(F32)
            hi = k_buf[pos, 32:64, :].astype(F32)
            roped.append(jnp.concatenate([lo * cos - hi * sin, hi * cos + lo * sin], axis=0).astype(BF16))
        out_row = lax.broadcasted_iota(jnp.int32, (256, 128), 0)
        lane = lax.broadcasted_iota(jnp.int32, (256, 128), 1)
        picks = [jnp.where((out_row % 8 == pos) & (out_row // 8 == lane // 4), 1.0, 0.0).astype(BF16) for pos in range(8)]
        pick = jnp.concatenate(picks, axis=1)
        request = lax.broadcasted_iota(jnp.int32, (64, 1024), 1) % 4
        for z in REQUESTS:
            cat = jnp.concatenate([r[:, 128 * z : 128 * (z + 1)] for r in roped], axis=1)
            masked = jnp.concatenate([jnp.where(request == j, cat, jnp.zeros_like(cat)) for j in REQUESTS], axis=0)
            laid = lax.dot_general(pick, masked, NT, preferred_element_type=F32)
            laid = laid.reshape(1, 4, 4, 2, 8, 256).astype(BF16)
            k_laid[z : z + 1] = laid
        own = {2: one(place[2])}
        mid1[2][index({**own, COL: K_COLS})] = k_laid[index(own)]

    def queries():
        q_rows[...] = jnp.zeros_like(q_rows)
        for j in REQUESTS:
            q_rows[j, HEADS * j : HEADS * (j + 1), :] = qlat_buf[j]
        zero = jnp.zeros((HEADS, ROPE), BF16)
        qk_rows[...] = jnp.zeros_like(qk_rows)
        for j in REQUESTS:
            qk_rows[HEADS * j : HEADS * (j + 1), :] = jnp.concatenate([qrope_buf[j] if i == j else zero for i in REQUESTS], axis=1)
        lane = lax.broadcasted_iota(jnp.int32, (8, LANES), 1)
        lens = jnp.zeros((8, LANES), jnp.int32)
        for j in REQUESTS:
            lens = jnp.where(lane // HEADS == j, length(j), lens)
        len_out[...] = lens

    def row_positions(a, b, c, ib, ic):
        r = lax.broadcasted_iota(jnp.int32, (ROWS, 1), 0)
        return (r // 16) * STRIDES[a] + r % 16 + ib * STRIDES[b] + ic * STRIDES[c]

    def unit_shape(a, width):
        return tuple(4 if d == a else 1 for d in range(3)) + (2, 8, width)

    def finish_rows(j, raw, gain, positions, a, where):
        square = jnp.sum(raw * raw, axis=-1, keepdims=True) * (1.0 / 512)
        inv_rms = jnp.where(positions < length(j), lax.rsqrt(square + NORM_EPS), 0.0)
        c_norm = raw * inv_rms * gain
        c_out[(j,) + where] = c_norm.reshape(unit_shape(a, LATENT)).astype(BF16)
        part = lax.dot_general(c_norm.astype(BF16), q_rows[j], NT, preferred_element_type=F32)
        score_out[(j,) + where] = part.reshape(unit_shape(a, LANES))

    def gain_row():
        return gain_buf[...].astype(F32).reshape(1, LATENT)

    def unit(p, ib, ic):
        a, b, c = ORDERS[p]
        where = index({b: one(ib), c: one(ic)})[:COL]
        gain = gain_row()
        raw = got[p][where + (pl.ds(*C_COLS),)].astype(F32).reshape(ROWS, LATENT)
        finish_rows(p, raw, gain, row_positions(a, b, c, ib, ic), a, where + (slice(None),))
        if p == 2:
            tile = got[2][where + (pl.ds(*K_COLS),)].astype(F32).reshape(ROWS, KEY_COLS).astype(BF16)
            part = lax.dot_general(tile, qk_rows[...], NT, preferred_element_type=F32)
            score_out[(4,) + where + (slice(None),)] = part.reshape(unit_shape(a, LANES))

    def near_units(off):
        arrived(("3near", off), 5, {0: (0, 3), 1: one(0), CORE: one(0)})
        for p in PARTS:
            _, b, c = ORDERS[p]
            for step in OFFSETS[:3]:
                unit(p, at(b, off), at(c, step))

    def far_units(off):
        arrived(("3fwd", off), 3, {0: one(0), 1: one(0)})
        for p in PARTS:
            _, b, c = ORDERS[p]
            unit(p, at(b, off), at(c, 2))
        key_columns(at(ORDERS[2][1], off))

    def key_columns(z):
        row = lax.broadcasted_iota(jnp.int32, (KEY_COLS, KEY_COLS), 0)
        col = lax.broadcasted_iota(jnp.int32, (KEY_COLS, KEY_COLS), 1)
        eye = jnp.where(row == col, 1.0, 0.0).astype(BF16)
        tile = got[2][pl.ds(z, 1), :, :, :, :, pl.ds(*K_COLS)].astype(F32).reshape(KEY_COLS, KEY_COLS).astype(BF16)
        turned = lax.dot_general(eye, tile, NT, preferred_element_type=F32)
        for j in REQUESTS:
            valid = col[:ROPE] + z * KEY_COLS < length(j)
            kr_out[j, :, pl.ds(pl.multiple_of(z * KEY_COLS, KEY_COLS), KEY_COLS)] = jnp.where(valid, turned[ROPE * j : ROPE * (j + 1)], 0.0).astype(BF16)

    def last_request(blocks):
        for off_y, off_x in blocks:
            y, x = at(1, off_y), at(2, off_x)
            where = index({1: one(y), 2: one(x)})[:COL]
            gain = gain_row()
            raw = [got[p][where + (pl.ds(*K_COLS),)].astype(F32).reshape(ROWS, KEY_COLS) for p in PAIR]
            finish_rows(3, jnp.concatenate(raw, axis=1), gain, row_positions(0, 1, 2, y, x), 0, where + (slice(None),))

    def blocks(n):
        inner = OFFSETS[: n - 1]
        return [(y, x) for y in OFFSETS[:n] for x in OFFSETS[:n] if y not in inner or x not in inner]

    def all_parts(step, *args):
        for p in PARTS:
            step(p, *args)

    EIGHTH, SIXTEENTH = {0: one(0), 1: (0, 2)}, {0: one(0), 1: one(0)}
    pl.semaphore_wait(barrier, 13)
    for first in (far1, near1):
        all_parts(first, C_COLS)
        first(0, K_COLS)
        first(1, K_COLS)
    for copy in key_loads:
        copy.wait()
    keys()
    for copy in other_loads:
        copy.wait()
    queries()
    far1(2, K_COLS)
    near1(2, K_COLS)
    taken(load_sem.at[LOADS - 2], 2, {0: one(0)})
    taken(load_sem.at[LOADS - 1], 1, {0: one(0), COL: C_COLS})
    arrived(first_group(0, None), 2, {0: one(0)})
    forward1(0)
    forward1(1)
    arrived(first_group(2, C_COLS), 1, {0: one(0), COL: C_COLS})
    forward1(2, C_COLS)
    all_parts(phase2, 0)
    arrived(first_group(2, K_COLS), 1, {0: one(0), COL: K_COLS})
    forward1(2, K_COLS)
    arrived("1near", 3, {0: (0, 2)})
    all_parts(phase2, -1)
    all_parts(phase2, 1)
    arrived(("2far", 0), 3, SIXTEENTH)
    all_parts(forward2, 0)
    arrived("1fwd", 3, {0: one(0)})
    all_parts(phase2, 2)
    for off in (-1, 1):
        arrived(("2far", off), 3, SIXTEENTH)
        all_parts(forward2, off)
    arrived(("2far", 2), 3, SIXTEENTH)
    all_parts(forward2, 2)
    all_parts(phase3, 0)
    arrived("2near", 3, {0: (0, 2)})
    all_parts(phase3, -1)
    arrived(("3far", 0), 3, SIXTEENTH)
    all_parts(forward3, 0)
    all_parts(phase3, 1)
    near_units(0)
    arrived("2fwd", 3, {0: one(0)})
    arrived(("3far", -1), 3, SIXTEENTH)
    all_parts(forward3, -1)
    all_parts(phase3, 2)
    near_units(-1)
    far_units(0)
    arrived(("3far", 1), 3, SIXTEENTH)
    all_parts(forward3, 1)
    near_units(1)
    far_units(-1)
    last_request(blocks(1) + blocks(2))
    arrived(("3far", 2), 3, SIXTEENTH)
    all_parts(forward3, 2)
    near_units(2)
    far_units(1)
    last_request(blocks(3))
    far_units(2)
    last_request(blocks(4))
    taken(send_sem.at[0], 9, {})
    taken(send_sem.at[1], 3, EIGHTH)


def exchange(c_raw, k_turned, rope_cos, rope_sin, gain, seq_lens, q_lat, q_rope):
    def shaped(sizes):
        return pltpu.VMEM(tuple(sizes.get(d, FULL[d]) for d in range(6)), BF16)

    hop1 = [shaped({o[0]: 1, o[1]: 2}) for o in ORDERS for _ in PAIR]
    hop2 = [shaped({o[1]: 1, o[2]: 2}) for o in ORDERS for _ in PAIR]
    hop3 = [shaped({o[2]: 1, 3: 1}) for o in ORDERS for _ in PAIR]
    small = [
        pltpu.VMEM((8, 64, 512), BF16),
        pltpu.VMEM((8, 32), F32),
        pltpu.VMEM((8, 32), F32),
        pltpu.VMEM((LATENT,), BF16),
        pltpu.SMEM((REQ,), jnp.int32),
        pltpu.VMEM((4, 16, 512), BF16),
        pltpu.VMEM((4, 16, 64), BF16),
        pltpu.VMEM((4, 128, 512), BF16),
        pltpu.VMEM((128, 256), BF16),
    ]
    sems = [pltpu.SemaphoreType.DMA((n,)) for n in (LOADS, 2, GROUPS)]
    return pl.pallas_call(
        exchange_kernel,
        out_shape=[
            pltpu.VMEM((4, 4, 4, 4, 2, 8, 512), BF16),
            pltpu.VMEM((4, 64, 1024), BF16),
            pltpu.VMEM((SCORE_PARTS,) + FULL[:COL] + (LANES,), F32),
            pltpu.VMEM((8, LANES), jnp.int32),
        ],
        in_specs=[pl.BlockSpec(memory_space=pltpu.HBM)] * 8,
        out_specs=[pl.BlockSpec(memory_space=pltpu.VMEM)] * 4,
        scratch_shapes=[[pltpu.VMEM((9,) + FULL, BF16), shaped({COL: KEY_COLS}), hop1, hop2, hop3, small, sems]],
        compiler_params=pltpu.CompilerParams(collective_id=0, has_side_effects=True, vmem_limit_bytes=40 * 1024 * 1024),
        name="exchange",
    )(c_raw, k_turned, rope_cos, rope_sin, gain, seq_lens, q_lat, q_rope)


def attend_kernel(c_ref, kr_ref, score_ref, len_ref, c_out, kr_out, o_out, o_buf, sem):
    writes = [pltpu.make_async_copy(c_ref, c_out, sem.at[0]), pltpu.make_async_copy(kr_ref, kr_out, sem.at[1])]
    for write in writes:
        write.start()
    row = lax.broadcasted_iota(jnp.int32, (POSITIONS, LANES), 0)
    scores = jnp.where(row < len_ref[0:1, :], jnp.sum(score_ref[...], axis=0) * ATTN_SCALE, -1e30)
    weights = jnp.exp(scores - jnp.max(scores, axis=0, keepdims=True)).T
    weight_sum = jnp.sum(weights[: 4 * HEADS], axis=1, keepdims=True)
    rounded = weights[: 4 * HEADS].astype(BF16)
    for j in REQUESTS:
        mine = slice(HEADS * j, HEADS * (j + 1))
        weighted = jnp.dot(rounded[mine], c_ref[j], preferred_element_type=F32)
        o_buf[j] = (weighted / weight_sum[mine]).astype(BF16)
        writes.append(pltpu.make_async_copy(o_buf.at[j], o_out.at[j], sem.at[2 + j]))
        writes[-1].start()
    for write in writes:
        write.wait()


def attend(c_cache, kr_turned, scores, lens):
    whole = pl.BlockSpec(memory_space=pltpu.VMEM)
    return pl.pallas_call(
        attend_kernel,
        out_shape=[
            jax.ShapeDtypeStruct(c_cache.shape, BF16),
            jax.ShapeDtypeStruct(kr_turned.shape, BF16),
            jax.ShapeDtypeStruct((4, HEADS, LATENT), BF16),
        ],
        in_specs=[whole] * 4,
        out_specs=[pl.BlockSpec(memory_space=pltpu.HBM)] * 3,
        scratch_shapes=[pltpu.VMEM((4, HEADS, LATENT), BF16), pltpu.SemaphoreType.DMA((6,))],
        compiler_params=pltpu.CompilerParams(vmem_limit_bytes=24 * 1024 * 1024),
        name="attend",
    )(c_cache, kr_turned, scores, lens)


def solution(mesh):
    seq_spec = P("dp", "x", None)
    req_spec = P(("dp", "x"), None, None)

    def local_step(c_raw, k_raw, norm_gain, rope_cos, rope_sin, seq_lens, q_lat, q_rope):
        args = (c_raw.reshape(FULL[:4] + (4, 8, LATENT)), k_raw.transpose(1, 2, 0), rope_cos, rope_sin, norm_gain, seq_lens, q_lat, q_rope)
        c_cache, kr_turned, scores, lens = exchange(*[pltpu.with_memory_space_constraint(arg, pltpu.HBM) for arg in args])
        c_cache, kr_turned, o_lat = attend(c_cache.reshape(4, POSITIONS, LATENT), kr_turned, scores.reshape(SCORE_PARTS, POSITIONS, LANES), lens)
        return c_cache, kr_turned.transpose(0, 2, 1), o_lat

    return jax.shard_map(local_step, mesh=mesh, in_specs=(seq_spec, seq_spec, P(None), P("x", None), P("x", None), P("dp"), req_spec, req_spec), out_specs=(req_spec, req_spec, req_spec), check_vma=False)
```

```python
import jax
import jax.numpy as jnp
from jax import lax
from jax.experimental import pallas as pl
from jax.experimental.pallas import tpu as pltpu
from jax.sharding import PartitionSpec as P

NORM_EPS = 1e-6
ATTN_SCALE = (512 + 64) ** -0.5
ORDERS = ((0, 1, 2), (1, 2, 0), (2, 0, 1))
FULL = (4, 4, 4, 2, 8, 768)
STRIDES = (256, 64, 16)
POSITIONS, LATENT, ROPE, HEADS, LANES = 1024, 512, 64, 16, 128
ROWS = 64
KEY_COLS = 256
C_COLS, K_COLS, ALL_COLS = (0, LATENT), (LATENT, KEY_COLS), (0, LATENT + KEY_COLS)
CORE, COL = 3, 5
PARTS = range(3)
PAIR = range(2)
REQUESTS = range(4)
REQ = 512
GROUPS = 23
LOADS = 9
SIGNS = (1, -1)
OFFSETS = (0, -1, 1, 2)
NT = (((1,), (1,)), ((), ()))
F32, BF16 = jnp.float32, jnp.bfloat16


def exchange_kernel(c_ref, k_ref, cos_ref, sin_ref, gain_ref, len_ref, qlat_ref, qrope_ref, c_out, kr_out, score_out, len_out, scratch):
    parts, k_laid, hop1, hop2, hop3, small, sems = scratch
    mid1, mid2, got = [[parts.at[3 * stage + p] for p in PARTS] for stage in PARTS]
    k_buf, cos_buf, sin_buf, gain_buf, len_buf, qlat_buf, qrope_buf, q_cols, qk_cols = small
    load_sem, send_sem, recv_sem = sems

    me = lax.axis_index("x")
    core = me % 2
    other = me + 1 - 2 * core
    cores = (core, 1 - core)
    place = (me // 32, (me // 8) % 4, (me // 2) % 4)

    def device(dim, delta, to_core=None):
        pos = list(place)
        pos[dim] = (pos[dim] + delta + 4) % 4
        last = core if to_core is None else to_core
        return ((pos[0] * 4 + pos[1]) * 4 + pos[2]) * 2 + last

    def at(dim, delta):
        return (place[dim] + delta + 4) % 4

    def index(sel, dims=len(FULL)):
        return tuple(pl.ds(*sel[d]) if d in sel else slice(None) for d in range(dims))

    def one(i):
        return (i, 1)

    def halves(s):
        return (2 * s, 2)

    def view(ref, sel):
        return ref.at[index(sel)]

    barrier = pltpu.get_barrier_semaphore()
    for dim in PARTS:
        for delta in SIGNS:
            for k in PAIR:
                pl.semaphore_signal(barrier, inc=1, device_id={"x": device(dim, delta, k)}, device_id_type=pl.DeviceIdType.MESH)
    pl.semaphore_signal(barrier, inc=1, device_id={"x": other}, device_id_type=pl.DeviceIdType.MESH)

    def taken(sem, n, shape):
        block = parts.at[(pl.ds(0, n),) + index(shape)]
        pltpu.make_async_copy(block, block, sem).wait()

    def taken_from(p, sel, extra):
        where = index(sel, COL - 1)
        if extra:
            return c_ref.at[where + (3, slice(None), pl.ds(KEY_COLS * p, KEY_COLS))]
        return c_ref.at[where + (p, slice(None), pl.ds(*C_COLS))]

    def load(slot, a, b):
        copy = pltpu.make_async_copy(a, b, load_sem.at[slot])
        copy.start()
        return copy

    key_loads = [load(i, a, b) for i, (a, b) in enumerate(((k_ref, k_buf), (cos_ref, cos_buf), (sin_ref, sin_buf)))]
    other_loads = [load(3 + i, a, b) for i, (a, b) in enumerate(((gain_ref, gain_buf), (len_ref, len_buf), (qlat_ref, qlat_buf), (qrope_ref, qrope_buf)))]
    for p in PARTS:
        own = {ORDERS[p][0]: one(place[ORDERS[p][0]])}
        load(LOADS - 1 if p == 2 else LOADS - 2, taken_from(p, own, False), view(mid1[p], {**own, COL: C_COLS}))
        if p < 2:
            load(LOADS - 2, taken_from(p, own, True), view(mid1[p], {**own, COL: K_COLS}))

    slots = {}

    def send(group, a, b, to, sent=0):
        slot = slots.setdefault(group, len(slots))
        pltpu.make_async_remote_copy(src_ref=a, dst_ref=b, send_sem=send_sem.at[sent], recv_sem=recv_sem.at[slot], device_id={"x": to}, device_id_type=pl.DeviceIdType.MESH).start()

    def arrived(group, n, shape):
        taken(recv_sem.at[slots[group]], n, shape)

    def held(p, sel, cols):
        if cols == C_COLS:
            return taken_from(p, sel, False)
        return taken_from(p, sel, True) if p < 2 else view(k_laid, sel)

    def first_group(p, cols):
        return ("1far", cols if p == 2 else None)

    def far1(p, cols):
        a, b, _ = ORDERS[p]
        wide = {COL: cols}
        for s, sign in enumerate(SIGNS):
            send(first_group(p, cols), held(p, {a: one(at(a, 2)), b: halves(s)}, cols), view(hop1[2 * p + s], wide), device(a, sign))

    def near1(p, cols):
        a, b, _ = ORDERS[p]
        wide = {COL: cols}
        for s, sign in enumerate(SIGNS):
            send("1near", held(p, {a: one(at(a, sign))}, cols), view(mid1[p], {a: one(place[a]), **wide}), device(a, sign))

    def forward1(p, cols=ALL_COLS):
        a, b, _ = ORDERS[p]
        wide = {COL: cols}
        for s, sign in enumerate(SIGNS):
            send("1fwd", view(hop1[2 * p + s], wide), view(mid1[p], {a: one(at(a, -sign)), b: halves(s), **wide}), device(a, sign))

    def phase2(p, off):
        a, b, c = ORDERS[p]
        sa = {a: one(at(a, off))}
        hop_sa = {a: one(off % 4)}
        for s, sign in enumerate(SIGNS):
            send(("2far", off), view(mid1[p], {**sa, b: one(at(b, 2)), c: halves(s)}), view(hop2[2 * p + s], hop_sa), device(b, sign))
        for s, sign in enumerate(SIGNS):
            send("2near", view(mid1[p], {**sa, b: one(at(b, sign))}), view(mid2[p], {**sa, b: one(place[b])}), device(b, sign))

    def forward2(p, off):
        a, b, c = ORDERS[p]
        sa = {a: one(at(a, off))}
        hop_sa = {a: one(off % 4)}
        for s, sign in enumerate(SIGNS):
            send("2fwd", view(hop2[2 * p + s], hop_sa), view(mid2[p], {**sa, b: one(at(b, -sign)), c: halves(s)}), device(b, sign))

    def phase3(p, off):
        a, b, c = ORDERS[p]
        sb = {b: one(at(b, off))}
        hop_sb = {b: one(off % 4)}
        got_b = mid1[p] if off == 0 else mid2[p]
        mine = {**sb, c: one(place[c]), CORE: one(core)}
        for s, sign in enumerate(SIGNS):
            send(("3far", off), view(got_b, {**sb, c: one(at(c, 2)), CORE: one(cores[s])}), view(hop3[2 * p + s], hop_sb), device(c, sign))
        for s, sign in enumerate(SIGNS):
            for k in PAIR:
                send(("3near", off), view(got_b, {**sb, c: one(at(c, sign)), CORE: one(cores[k])}), view(got[p], mine), device(c, sign, cores[k]))
        send(("3near", off), view(got_b, {**sb, c: one(place[c]), CORE: one(cores[1])}), view(got[p], mine), other, 1)
        got[p][index(mine)] = got_b[index(mine)]

    def forward3(p, off):
        a, b, c = ORDERS[p]
        sb = {b: one(at(b, off))}
        hop_sb = {b: one(off % 4)}
        for s, sign in enumerate(SIGNS):
            send(("3fwd", off), view(hop3[2 * p + s], hop_sb), view(got[p], {**sb, c: one(at(c, -sign)), CORE: one(core)}), device(c, sign, cores[s]))

    def length(j):
        return len_buf[4 * me + j]

    def keys():
        row = lax.broadcasted_iota(jnp.int32, (32, 32), 0)
        diag = row == lax.broadcasted_iota(jnp.int32, (32, 32), 1)
        roped = []
        for pos in range(8):
            cos = jnp.sum(jnp.where(diag, cos_buf[pos : pos + 1, :], 0.0), axis=1, keepdims=True)
            sin = jnp.sum(jnp.where(diag, sin_buf[pos : pos + 1, :], 0.0), axis=1, keepdims=True)
            lo = k_buf[pos, 0:32, :].astype(F32)
            hi = k_buf[pos, 32:64, :].astype(F32)
            roped.append(jnp.concatenate([lo * cos - hi * sin, hi * cos + lo * sin], axis=0).astype(BF16))
        out_row = lax.broadcasted_iota(jnp.int32, (256, 128), 0)
        lane = lax.broadcasted_iota(jnp.int32, (256, 128), 1)
        picks = [jnp.where((out_row % 8 == pos) & (out_row // 8 == lane // 4), 1.0, 0.0).astype(BF16) for pos in range(8)]
        pick = jnp.concatenate(picks, axis=1)
        request = lax.broadcasted_iota(jnp.int32, (64, 1024), 1) % 4
        for z in REQUESTS:
            cat = jnp.concatenate([r[:, 128 * z : 128 * (z + 1)] for r in roped], axis=1)
            masked = jnp.concatenate([jnp.where(request == j, cat, jnp.zeros_like(cat)) for j in REQUESTS], axis=0)
            laid = lax.dot_general(pick, masked, NT, preferred_element_type=F32)
            laid = laid.reshape(1, 4, 4, 2, 8, 256).astype(BF16)
            k_laid[z : z + 1] = laid
        own = {2: one(place[2])}
        mid1[2][index({**own, COL: K_COLS})] = k_laid[index(own)]

    def queries():
        for j in REQUESTS:
            rows = [qlat_buf[j].astype(F32) if i == j else jnp.zeros((HEADS, LATENT), F32) for i in REQUESTS]
            q_cols[j] = jnp.concatenate(rows + [jnp.zeros((LANES - 4 * HEADS, LATENT), F32)], axis=0).T.astype(BF16)
        zero = jnp.zeros((HEADS, ROPE), F32)
        rows = [jnp.concatenate([qrope_buf[j].astype(F32) if i == j else zero for i in REQUESTS], axis=1) for j in REQUESTS]
        qk_cols[...] = jnp.concatenate(rows + [jnp.zeros((LANES - 4 * HEADS, KEY_COLS), F32)], axis=0).T.astype(BF16)
        score_out[...] = jnp.zeros_like(score_out)
        lane = lax.broadcasted_iota(jnp.int32, (8, LANES), 1)
        lens = jnp.zeros((8, LANES), jnp.int32)
        for j in REQUESTS:
            lens = jnp.where(lane // HEADS == j, length(j), lens)
        len_out[...] = lens

    def row_positions(a, b, c, ib, ic):
        r = lax.broadcasted_iota(jnp.int32, (ROWS, 1), 0)
        return (r // 16) * STRIDES[a] + r % 16 + ib * STRIDES[b] + ic * STRIDES[c]

    def unit_shape(a, width):
        return tuple(4 if d == a else 1 for d in range(3)) + (2, 8, width)

    def add_scores(a, wheres, rows, columns):
        part = jnp.dot(jnp.concatenate(rows, axis=0), columns, preferred_element_type=F32)
        for i, where in enumerate(wheres):
            score_out[where] += part[ROWS * i : ROWS * (i + 1)].reshape(unit_shape(a, LANES))

    def finish(j, a, wheres, raws, positions):
        gain = gain_row()
        rows = []
        for where, raw, pos in zip(wheres, raws, positions):
            square = jnp.sum(raw * raw, axis=-1, keepdims=True) * (1.0 / LATENT)
            inv_rms = jnp.where(pos < length(j), lax.rsqrt(square + NORM_EPS), 0.0)
            c_norm = raw * inv_rms * gain
            c_out[(j,) + where] = c_norm.reshape(unit_shape(a, LATENT)).astype(BF16)
            rows.append(c_norm.astype(BF16))
        add_scores(a, wheres, rows, q_cols[j])

    def gain_row():
        return gain_buf[...].astype(F32).reshape(1, LATENT)

    def units(p, off, steps):
        a, b, c = ORDERS[p]
        ib, ics = at(b, off), [at(c, step) for step in steps]
        wheres = [index({b: one(ib), c: one(ic)})[:COL] for ic in ics]
        full = [where + (slice(None),) for where in wheres]
        raws = [got[p][where + (pl.ds(*C_COLS),)].astype(F32).reshape(ROWS, LATENT) for where in wheres]
        finish(p, a, full, raws, [row_positions(a, b, c, ib, ic) for ic in ics])
        if p == 2:
            tiles = [got[2][where + (pl.ds(*K_COLS),)].astype(F32).reshape(ROWS, KEY_COLS).astype(BF16) for where in wheres]
            add_scores(a, full, tiles, qk_cols[...])

    def near_units(off):
        arrived(("3near", off), 5, {0: (0, 3), 1: one(0), CORE: one(0)})
        all_parts(units, off, OFFSETS[:3])

    def far_units(off):
        arrived(("3fwd", off), 3, {0: one(0), 1: one(0)})
        all_parts(units, off, OFFSETS[3:])
        key_columns(at(ORDERS[2][1], off))

    def key_columns(z):
        row = lax.broadcasted_iota(jnp.int32, (KEY_COLS, KEY_COLS), 0)
        col = lax.broadcasted_iota(jnp.int32, (KEY_COLS, KEY_COLS), 1)
        eye = jnp.where(row == col, 1.0, 0.0).astype(BF16)
        tile = got[2][pl.ds(z, 1), :, :, :, :, pl.ds(*K_COLS)].astype(F32).reshape(KEY_COLS, KEY_COLS).astype(BF16)
        turned = lax.dot_general(eye, tile, NT, preferred_element_type=F32)
        for j in REQUESTS:
            valid = col[:ROPE] + z * KEY_COLS < length(j)
            kr_out[j, :, pl.ds(pl.multiple_of(z * KEY_COLS, KEY_COLS), KEY_COLS)] = jnp.where(valid, turned[ROPE * j : ROPE * (j + 1)], 0.0).astype(BF16)

    def last_request(steps):
        places = [(at(1, y), at(2, x)) for y, x in steps]
        wheres = [index({1: one(y), 2: one(x)})[:COL] for y, x in places]
        raws = [jnp.concatenate([got[p][where + (pl.ds(*K_COLS),)].astype(F32).reshape(ROWS, KEY_COLS) for p in PAIR], axis=1) for where in wheres]
        finish(3, 0, [where + (slice(None),) for where in wheres], raws, [row_positions(0, 1, 2, y, x) for y, x in places])

    def all_parts(step, *args):
        for p in PARTS:
            step(p, *args)

    EIGHTH, SIXTEENTH = {0: one(0), 1: (0, 2)}, {0: one(0), 1: one(0)}
    pl.semaphore_wait(barrier, 13)
    for first in (far1, near1):
        all_parts(first, C_COLS)
        first(0, K_COLS)
        first(1, K_COLS)
    for copy in key_loads:
        copy.wait()
    keys()
    for copy in other_loads:
        copy.wait()
    queries()
    far1(2, K_COLS)
    near1(2, K_COLS)
    taken(load_sem.at[LOADS - 2], 2, {0: one(0)})
    taken(load_sem.at[LOADS - 1], 1, {0: one(0), COL: C_COLS})
    arrived(first_group(0, None), 2, {0: one(0)})
    forward1(0)
    forward1(1)
    arrived(first_group(2, C_COLS), 1, {0: one(0), COL: C_COLS})
    forward1(2, C_COLS)
    all_parts(phase2, 0)
    arrived(first_group(2, K_COLS), 1, {0: one(0), COL: K_COLS})
    forward1(2, K_COLS)
    arrived("1near", 3, {0: (0, 2)})
    all_parts(phase2, -1)
    all_parts(phase2, 1)
    arrived(("2far", 0), 3, SIXTEENTH)
    all_parts(forward2, 0)
    arrived("1fwd", 3, {0: one(0)})
    all_parts(phase2, 2)
    for off in (-1, 1):
        arrived(("2far", off), 3, SIXTEENTH)
        all_parts(forward2, off)
    arrived(("2far", 2), 3, SIXTEENTH)
    all_parts(forward2, 2)
    all_parts(phase3, 0)
    arrived("2near", 3, {0: (0, 2)})
    all_parts(phase3, -1)
    arrived(("3far", 0), 3, SIXTEENTH)
    all_parts(forward3, 0)
    all_parts(phase3, 1)
    near_units(0)
    arrived("2fwd", 3, {0: one(0)})
    arrived(("3far", -1), 3, SIXTEENTH)
    all_parts(forward3, -1)
    all_parts(phase3, 2)
    near_units(-1)
    far_units(0)
    arrived(("3far", 1), 3, SIXTEENTH)
    all_parts(forward3, 1)
    near_units(1)
    far_units(-1)
    last_request([(y, x) for y in OFFSETS[:2] for x in OFFSETS[:2]])
    arrived(("3far", 2), 3, SIXTEENTH)
    all_parts(forward3, 2)
    near_units(2)
    far_units(1)
    last_request([(y, x) for y in OFFSETS for x in OFFSETS[:3] if y > 0 or x > 0])
    far_units(2)
    last_request([(y, 2) for y in OFFSETS])
    taken(send_sem.at[0], 9, {})
    taken(send_sem.at[1], 3, EIGHTH)


def exchange(c_raw, k_turned, rope_cos, rope_sin, gain, seq_lens, q_lat, q_rope):
    def shaped(sizes):
        return pltpu.VMEM(tuple(sizes.get(d, FULL[d]) for d in range(6)), BF16)

    hop1 = [shaped({o[0]: 1, o[1]: 2}) for o in ORDERS for _ in PAIR]
    hop2 = [shaped({o[1]: 1, o[2]: 2}) for o in ORDERS for _ in PAIR]
    hop3 = [shaped({o[2]: 1, 3: 1}) for o in ORDERS for _ in PAIR]
    small = [
        pltpu.VMEM((8, 64, 512), BF16),
        pltpu.VMEM((8, 32), F32),
        pltpu.VMEM((8, 32), F32),
        pltpu.VMEM((LATENT,), BF16),
        pltpu.SMEM((REQ,), jnp.int32),
        pltpu.VMEM((4, 16, 512), BF16),
        pltpu.VMEM((4, 16, 64), BF16),
        pltpu.VMEM((4, LATENT, LANES), BF16),
        pltpu.VMEM((KEY_COLS, LANES), BF16),
    ]
    sems = [pltpu.SemaphoreType.DMA((n,)) for n in (LOADS, 2, GROUPS)]
    return pl.pallas_call(
        exchange_kernel,
        out_shape=[
            pltpu.VMEM((4, 4, 4, 4, 2, 8, 512), BF16),
            pltpu.VMEM((4, 64, 1024), BF16),
            pltpu.VMEM(FULL[:COL] + (LANES,), F32),
            pltpu.VMEM((8, LANES), jnp.int32),
        ],
        in_specs=[pl.BlockSpec(memory_space=pltpu.HBM)] * 8,
        out_specs=[pl.BlockSpec(memory_space=pltpu.VMEM)] * 4,
        scratch_shapes=[[pltpu.VMEM((9,) + FULL, BF16), shaped({COL: KEY_COLS}), hop1, hop2, hop3, small, sems]],
        compiler_params=pltpu.CompilerParams(collective_id=0, has_side_effects=True, vmem_limit_bytes=40 * 1024 * 1024),
        name="exchange",
    )(c_raw, k_turned, rope_cos, rope_sin, gain, seq_lens, q_lat, q_rope)


def attend_kernel(c_ref, kr_ref, score_ref, len_ref, c_out, kr_out, o_out, o_buf, sem):
    writes = []

    def write(a, b):
        writes.append(pltpu.make_async_copy(a, b, sem.at[len(writes)]))
        writes[-1].start()

    for j in REQUESTS:
        for half in PAIR:
            rows = pl.ds(half * (POSITIONS // 2), POSITIONS // 2)
            write(c_ref.at[j, rows], c_out.at[j, rows])
    write(kr_ref, kr_out)
    row = lax.broadcasted_iota(jnp.int32, (POSITIONS, LANES), 0)
    scores = jnp.where(row < len_ref[0:1, :], score_ref[...] * ATTN_SCALE, -1e30)
    weights = jnp.exp(scores - jnp.max(scores, axis=0, keepdims=True)).T
    weight_sum = jnp.sum(weights[: 4 * HEADS], axis=1, keepdims=True)
    rounded = weights[: 4 * HEADS].astype(BF16)
    for j in REQUESTS:
        mine = slice(HEADS * j, HEADS * (j + 1))
        weighted = jnp.dot(rounded[mine], c_ref[j], preferred_element_type=F32)
        o_buf[j] = (weighted / weight_sum[mine]).astype(BF16)
        write(o_buf.at[j], o_out.at[j])
    for copy in writes:
        copy.wait()


def attend(c_cache, kr_turned, scores, lens):
    whole = pl.BlockSpec(memory_space=pltpu.VMEM)
    return pl.pallas_call(
        attend_kernel,
        out_shape=[
            jax.ShapeDtypeStruct(c_cache.shape, BF16),
            jax.ShapeDtypeStruct(kr_turned.shape, BF16),
            jax.ShapeDtypeStruct((4, HEADS, LATENT), BF16),
        ],
        in_specs=[whole] * 4,
        out_specs=[pl.BlockSpec(memory_space=pltpu.HBM)] * 3,
        scratch_shapes=[pltpu.VMEM((4, HEADS, LATENT), BF16), pltpu.SemaphoreType.DMA((13,))],
        compiler_params=pltpu.CompilerParams(vmem_limit_bytes=24 * 1024 * 1024),
        name="attend",
    )(c_cache, kr_turned, scores, lens)


def solution(mesh):
    seq_spec = P("dp", "x", None)
    req_spec = P(("dp", "x"), None, None)

    def local_step(c_raw, k_raw, norm_gain, rope_cos, rope_sin, seq_lens, q_lat, q_rope):
        args = (c_raw.reshape(FULL[:4] + (4, 8, LATENT)), k_raw.transpose(1, 2, 0), rope_cos, rope_sin, norm_gain, seq_lens, q_lat, q_rope)
        c_cache, kr_turned, scores, lens = exchange(*[pltpu.with_memory_space_constraint(arg, pltpu.HBM) for arg in args])
        c_cache, kr_turned, o_lat = attend(c_cache.reshape(4, POSITIONS, LATENT), kr_turned, scores.reshape(POSITIONS, LANES), lens)
        return c_cache, kr_turned.transpose(0, 2, 1), o_lat

    return jax.shard_map(local_step, mesh=mesh, in_specs=(seq_spec, seq_spec, P(None), P("x", None), P("x", None), P("dp"), req_spec, req_spec), out_specs=(req_spec, req_spec, req_spec), check_vma=False)
```

```python
import jax
import jax.numpy as jnp
from jax import lax
from jax.experimental import pallas as pl
from jax.experimental.pallas import tpu as pltpu
from jax.sharding import PartitionSpec as P

NORM_EPS = 1e-6
ATTN_SCALE = (512 + 64) ** -0.5
ORDERS = ((0, 1, 2), (1, 2, 0), (2, 0, 1))
FULL = (4, 4, 4, 2, 8, 768)
STRIDES = (256, 64, 16)
POSITIONS, LATENT, ROPE, HEADS, LANES = 1024, 512, 64, 16, 128
ROWS = 64
KEY_COLS = 256
C_COLS, K_COLS, ALL_COLS = (0, LATENT), (LATENT, KEY_COLS), (0, LATENT + KEY_COLS)
CORE, COL = 3, 5
PARTS = range(3)
PAIR = range(2)
REQUESTS = range(4)
REQ = 512
GROUPS = 23
LOADS = 11
SIGNS = (1, -1)
OFFSETS = (0, -1, 1, 2)
NT = (((1,), (1,)), ((), ()))
F32, BF16 = jnp.float32, jnp.bfloat16


def exchange_kernel(c_ref, k_ref, cos_ref, sin_ref, gain_ref, len_ref, qlat_ref, qrope_ref, c_out, kr_out, score_out, len_out, scratch):
    parts, k_laid, staged, hop1, hop2, hop3, small, sems = scratch
    mid1, mid2, got = [[parts.at[3 * stage + p] for p in PARTS] for stage in PARTS]
    k_buf, cos_buf, sin_buf, gain_buf, len_buf, qlat_buf, qrope_buf, q_cols, qk_cols = small
    load_sem, send_sem, recv_sem = sems

    me = lax.axis_index("x")
    core = me % 2
    other = me + 1 - 2 * core
    cores = (core, 1 - core)
    place = (me // 32, (me // 8) % 4, (me // 2) % 4)

    def device(dim, delta, to_core=None):
        pos = list(place)
        pos[dim] = (pos[dim] + delta + 4) % 4
        last = core if to_core is None else to_core
        return ((pos[0] * 4 + pos[1]) * 4 + pos[2]) * 2 + last

    def at(dim, delta):
        return (place[dim] + delta + 4) % 4

    def index(sel, dims=len(FULL)):
        return tuple(pl.ds(*sel[d]) if d in sel else slice(None) for d in range(dims))

    def one(i):
        return (i, 1)

    def halves(s):
        return (2 * s, 2)

    def view(ref, sel):
        return ref.at[index(sel)]

    barrier = pltpu.get_barrier_semaphore()
    for dim in PARTS:
        for delta in SIGNS:
            for k in PAIR:
                pl.semaphore_signal(barrier, inc=1, device_id={"x": device(dim, delta, k)}, device_id_type=pl.DeviceIdType.MESH)
    pl.semaphore_signal(barrier, inc=1, device_id={"x": other}, device_id_type=pl.DeviceIdType.MESH)

    def taken(sem, n, shape):
        block = parts.at[(pl.ds(0, n),) + index(shape)]
        pltpu.make_async_copy(block, block, sem).wait()

    def taken_from(p, sel, extra):
        where = index(sel, COL - 1)
        if extra:
            return c_ref.at[where + (3, slice(None), pl.ds(KEY_COLS * p, KEY_COLS))]
        return c_ref.at[where + (p, slice(None), pl.ds(*C_COLS))]

    def load(slot, a, b):
        copy = pltpu.make_async_copy(a, b, load_sem.at[slot])
        copy.start()
        return copy

    for extra in (False, True):
        for p in PARTS[: 2 if extra else 3]:
            a, b, _ = ORDERS[p]
            for s in PAIR:
                far = {a: one(at(a, 2)), b: halves(s)}
                load(8 if p == 2 else 7, taken_from(p, far, extra), view(staged[2 * p + s], {COL: K_COLS if extra else C_COLS}))
    key_loads = [load(i, a, b) for i, (a, b) in enumerate(((k_ref, k_buf), (cos_ref, cos_buf), (sin_ref, sin_buf)))]
    other_loads = [load(3 + i, a, b) for i, (a, b) in enumerate(((gain_ref, gain_buf), (len_ref, len_buf), (qlat_ref, qlat_buf), (qrope_ref, qrope_buf)))]
    for p in PARTS:
        own = {ORDERS[p][0]: one(place[ORDERS[p][0]])}
        load(LOADS - 1 if p == 2 else LOADS - 2, taken_from(p, own, False), view(mid1[p], {**own, COL: C_COLS}))
        if p < 2:
            load(LOADS - 2, taken_from(p, own, True), view(mid1[p], {**own, COL: K_COLS}))

    slots = {}

    def send(group, a, b, to, sent=0):
        slot = slots.setdefault(group, len(slots))
        pltpu.make_async_remote_copy(src_ref=a, dst_ref=b, send_sem=send_sem.at[sent], recv_sem=recv_sem.at[slot], device_id={"x": to}, device_id_type=pl.DeviceIdType.MESH).start()

    def arrived(group, n, shape):
        taken(recv_sem.at[slots[group]], n, shape)

    def held(p, sel, cols):
        if cols == C_COLS:
            return taken_from(p, sel, False)
        return taken_from(p, sel, True) if p < 2 else view(k_laid, sel)

    def first_group(p, cols):
        return ("1far", cols if p == 2 else None)

    def far1(p, cols):
        a, b, _ = ORDERS[p]
        wide = {COL: cols}
        for s, sign in enumerate(SIGNS):
            source = view(k_laid, {a: one(at(a, 2)), b: halves(s)}) if cols == K_COLS else view(staged[2 * p + s], wide)
            send(first_group(p, cols), source, view(hop1[2 * p + s], wide), device(a, sign))

    def near1(p, cols):
        a, b, _ = ORDERS[p]
        wide = {COL: cols}
        for s, sign in enumerate(SIGNS):
            send("1near", held(p, {a: one(at(a, sign))}, cols), view(mid1[p], {a: one(place[a]), **wide}), device(a, sign))

    def forward1(p, cols=ALL_COLS):
        a, b, _ = ORDERS[p]
        wide = {COL: cols}
        for s, sign in enumerate(SIGNS):
            send("1fwd", view(hop1[2 * p + s], wide), view(mid1[p], {a: one(at(a, -sign)), b: halves(s), **wide}), device(a, sign))

    def phase2(p, off):
        a, b, c = ORDERS[p]
        sa = {a: one(at(a, off))}
        hop_sa = {a: one(off % 4)}
        for s, sign in enumerate(SIGNS):
            send(("2far", off), view(mid1[p], {**sa, b: one(at(b, 2)), c: halves(s)}), view(hop2[2 * p + s], hop_sa), device(b, sign))
        for s, sign in enumerate(SIGNS):
            send("2near", view(mid1[p], {**sa, b: one(at(b, sign))}), view(mid2[p], {**sa, b: one(place[b])}), device(b, sign))

    def forward2(p, off):
        a, b, c = ORDERS[p]
        sa = {a: one(at(a, off))}
        hop_sa = {a: one(off % 4)}
        for s, sign in enumerate(SIGNS):
            send("2fwd", view(hop2[2 * p + s], hop_sa), view(mid2[p], {**sa, b: one(at(b, -sign)), c: halves(s)}), device(b, sign))

    def phase3(p, off):
        a, b, c = ORDERS[p]
        sb = {b: one(at(b, off))}
        hop_sb = {b: one(off % 4)}
        got_b = mid1[p] if off == 0 else mid2[p]
        mine = {**sb, c: one(place[c]), CORE: one(core)}
        for s, sign in enumerate(SIGNS):
            send(("3far", off), view(got_b, {**sb, c: one(at(c, 2)), CORE: one(cores[s])}), view(hop3[2 * p + s], hop_sb), device(c, sign))
        for s, sign in enumerate(SIGNS):
            for k in PAIR:
                send(("3near", off), view(got_b, {**sb, c: one(at(c, sign)), CORE: one(cores[k])}), view(got[p], mine), device(c, sign, cores[k]))
        send(("3near", off), view(got_b, {**sb, c: one(place[c]), CORE: one(cores[1])}), view(got[p], mine), other, 1)
        got[p][index(mine)] = got_b[index(mine)]

    def forward3(p, off):
        a, b, c = ORDERS[p]
        sb = {b: one(at(b, off))}
        hop_sb = {b: one(off % 4)}
        for s, sign in enumerate(SIGNS):
            send(("3fwd", off), view(hop3[2 * p + s], hop_sb), view(got[p], {**sb, c: one(at(c, -sign)), CORE: one(core)}), device(c, sign, cores[s]))

    def length(j):
        return len_buf[4 * me + j]

    def keys():
        row = lax.broadcasted_iota(jnp.int32, (32, 32), 0)
        diag = row == lax.broadcasted_iota(jnp.int32, (32, 32), 1)
        roped = []
        for pos in range(8):
            cos = jnp.sum(jnp.where(diag, cos_buf[pos : pos + 1, :], 0.0), axis=1, keepdims=True)
            sin = jnp.sum(jnp.where(diag, sin_buf[pos : pos + 1, :], 0.0), axis=1, keepdims=True)
            lo = k_buf[pos, 0:32, :].astype(F32)
            hi = k_buf[pos, 32:64, :].astype(F32)
            roped.append(jnp.concatenate([lo * cos - hi * sin, hi * cos + lo * sin], axis=0).astype(BF16))
        out_row = lax.broadcasted_iota(jnp.int32, (256, 128), 0)
        lane = lax.broadcasted_iota(jnp.int32, (256, 128), 1)
        picks = [jnp.where((out_row % 8 == pos) & (out_row // 8 == lane // 4), 1.0, 0.0).astype(BF16) for pos in range(8)]
        pick = jnp.concatenate(picks, axis=1)
        request = lax.broadcasted_iota(jnp.int32, (64, 1024), 1) % 4
        for z in REQUESTS:
            cat = jnp.concatenate([r[:, 128 * z : 128 * (z + 1)] for r in roped], axis=1)
            masked = jnp.concatenate([jnp.where(request == j, cat, jnp.zeros_like(cat)) for j in REQUESTS], axis=0)
            laid = lax.dot_general(pick, masked, NT, preferred_element_type=F32)
            laid = laid.reshape(1, 4, 4, 2, 8, 256).astype(BF16)
            k_laid[z : z + 1] = laid
        own = {2: one(place[2])}
        mid1[2][index({**own, COL: K_COLS})] = k_laid[index(own)]

    def queries():
        for j in REQUESTS:
            rows = [qlat_buf[j].astype(F32) if i == j else jnp.zeros((HEADS, LATENT), F32) for i in REQUESTS]
            q_cols[j] = jnp.concatenate(rows + [jnp.zeros((LANES - 4 * HEADS, LATENT), F32)], axis=0).T.astype(BF16)
        zero = jnp.zeros((HEADS, ROPE), F32)
        rows = [jnp.concatenate([qrope_buf[j].astype(F32) if i == j else zero for i in REQUESTS], axis=1) for j in REQUESTS]
        qk_cols[...] = jnp.concatenate(rows + [jnp.zeros((LANES - 4 * HEADS, KEY_COLS), F32)], axis=0).T.astype(BF16)
        score_out[...] = jnp.zeros_like(score_out)
        lane = lax.broadcasted_iota(jnp.int32, (8, LANES), 1)
        lens = jnp.zeros((8, LANES), jnp.int32)
        for j in REQUESTS:
            lens = jnp.where(lane // HEADS == j, length(j), lens)
        len_out[...] = lens

    def row_positions(a, b, c, ib, ic):
        r = lax.broadcasted_iota(jnp.int32, (ROWS, 1), 0)
        return (r // 16) * STRIDES[a] + r % 16 + ib * STRIDES[b] + ic * STRIDES[c]

    def unit_shape(a, width):
        return tuple(4 if d == a else 1 for d in range(3)) + (2, 8, width)

    def add_scores(a, wheres, rows, columns):
        part = jnp.dot(jnp.concatenate(rows, axis=0), columns, preferred_element_type=F32)
        for i, where in enumerate(wheres):
            score_out[where] += part[ROWS * i : ROWS * (i + 1)].reshape(unit_shape(a, LANES))

    def finish(j, a, wheres, raws, positions):
        gain = gain_row()
        rows = []
        for where, raw, pos in zip(wheres, raws, positions):
            square = jnp.sum(raw * raw, axis=-1, keepdims=True) * (1.0 / LATENT)
            inv_rms = jnp.where(pos < length(j), lax.rsqrt(square + NORM_EPS), 0.0)
            c_norm = raw * inv_rms * gain
            c_out[(j,) + where] = c_norm.reshape(unit_shape(a, LATENT)).astype(BF16)
            rows.append(c_norm.astype(BF16))
        add_scores(a, wheres, rows, q_cols[j])

    def gain_row():
        return gain_buf[...].astype(F32).reshape(1, LATENT)

    def units(p, off, steps):
        a, b, c = ORDERS[p]
        ib, ics = at(b, off), [at(c, step) for step in steps]
        wheres = [index({b: one(ib), c: one(ic)})[:COL] for ic in ics]
        full = [where + (slice(None),) for where in wheres]
        raws = [got[p][where + (pl.ds(*C_COLS),)].astype(F32).reshape(ROWS, LATENT) for where in wheres]
        finish(p, a, full, raws, [row_positions(a, b, c, ib, ic) for ic in ics])
        if p == 2:
            tiles = [got[2][where + (pl.ds(*K_COLS),)].astype(F32).reshape(ROWS, KEY_COLS).astype(BF16) for where in wheres]
            add_scores(a, full, tiles, qk_cols[...])

    def near_units(off):
        arrived(("3near", off), 5, {0: (0, 3), 1: one(0), CORE: one(0)})
        all_parts(units, off, OFFSETS[:3])

    def far_units(off):
        arrived(("3fwd", off), 3, {0: one(0), 1: one(0)})
        all_parts(units, off, OFFSETS[3:])
        key_columns(at(ORDERS[2][1], off))

    def key_columns(z):
        row = lax.broadcasted_iota(jnp.int32, (KEY_COLS, KEY_COLS), 0)
        col = lax.broadcasted_iota(jnp.int32, (KEY_COLS, KEY_COLS), 1)
        eye = jnp.where(row == col, 1.0, 0.0).astype(BF16)
        tile = got[2][pl.ds(z, 1), :, :, :, :, pl.ds(*K_COLS)].astype(F32).reshape(KEY_COLS, KEY_COLS).astype(BF16)
        turned = lax.dot_general(eye, tile, NT, preferred_element_type=F32)
        for j in REQUESTS:
            valid = col[:ROPE] + z * KEY_COLS < length(j)
            kr_out[j, :, pl.ds(pl.multiple_of(z * KEY_COLS, KEY_COLS), KEY_COLS)] = jnp.where(valid, turned[ROPE * j : ROPE * (j + 1)], 0.0).astype(BF16)

    def last_request(steps):
        places = [(at(1, y), at(2, x)) for y, x in steps]
        wheres = [index({1: one(y), 2: one(x)})[:COL] for y, x in places]
        raws = [jnp.concatenate([got[p][where + (pl.ds(*K_COLS),)].astype(F32).reshape(ROWS, KEY_COLS) for p in PAIR], axis=1) for where in wheres]
        finish(3, 0, [where + (slice(None),) for where in wheres], raws, [row_positions(0, 1, 2, y, x) for y, x in places])

    def all_parts(step, *args):
        for p in PARTS:
            step(p, *args)

    EIGHTH, SIXTEENTH = {0: one(0), 1: (0, 2)}, {0: one(0), 1: one(0)}
    pl.semaphore_wait(barrier, 13)
    taken(load_sem.at[7], 2, {0: one(0)})
    far1(0, ALL_COLS)
    far1(1, ALL_COLS)
    taken(load_sem.at[8], 1, {0: one(0), COL: C_COLS})
    far1(2, C_COLS)
    all_parts(near1, C_COLS)
    near1(0, K_COLS)
    near1(1, K_COLS)
    for copy in key_loads:
        copy.wait()
    keys()
    for copy in other_loads:
        copy.wait()
    queries()
    far1(2, K_COLS)
    near1(2, K_COLS)
    taken(load_sem.at[LOADS - 2], 2, {0: one(0)})
    taken(load_sem.at[LOADS - 1], 1, {0: one(0), COL: C_COLS})
    arrived(first_group(0, None), 2, {0: one(0)})
    forward1(0)
    forward1(1)
    arrived(first_group(2, C_COLS), 1, {0: one(0), COL: C_COLS})
    forward1(2, C_COLS)
    all_parts(phase2, 0)
    arrived(first_group(2, K_COLS), 1, {0: one(0), COL: K_COLS})
    forward1(2, K_COLS)
    arrived("1near", 3, {0: (0, 2)})
    all_parts(phase2, -1)
    all_parts(phase2, 1)
    arrived(("2far", 0), 3, SIXTEENTH)
    all_parts(forward2, 0)
    arrived("1fwd", 3, {0: one(0)})
    all_parts(phase2, 2)
    for off in (-1, 1):
        arrived(("2far", off), 3, SIXTEENTH)
        all_parts(forward2, off)
    arrived(("2far", 2), 3, SIXTEENTH)
    all_parts(forward2, 2)
    all_parts(phase3, 0)
    arrived("2near", 3, {0: (0, 2)})
    all_parts(phase3, -1)
    arrived(("3far", 0), 3, SIXTEENTH)
    all_parts(forward3, 0)
    all_parts(phase3, 1)
    near_units(0)
    arrived("2fwd", 3, {0: one(0)})
    arrived(("3far", -1), 3, SIXTEENTH)
    all_parts(forward3, -1)
    all_parts(phase3, 2)
    near_units(-1)
    far_units(0)
    arrived(("3far", 1), 3, SIXTEENTH)
    all_parts(forward3, 1)
    near_units(1)
    far_units(-1)
    last_request([(y, x) for y in OFFSETS[:2] for x in OFFSETS[:2]])
    arrived(("3far", 2), 3, SIXTEENTH)
    all_parts(forward3, 2)
    near_units(2)
    far_units(1)
    last_request([(y, x) for y in OFFSETS for x in OFFSETS[:3] if y > 0 or x > 0])
    far_units(2)
    last_request([(y, 2) for y in OFFSETS])
    taken(send_sem.at[0], 9, {})
    taken(send_sem.at[1], 3, EIGHTH)


def exchange(c_raw, k_turned, rope_cos, rope_sin, gain, seq_lens, q_lat, q_rope):
    def shaped(sizes):
        return pltpu.VMEM(tuple(sizes.get(d, FULL[d]) for d in range(6)), BF16)

    hop1 = [shaped({o[0]: 1, o[1]: 2}) for o in ORDERS for _ in PAIR]
    hop2 = [shaped({o[1]: 1, o[2]: 2}) for o in ORDERS for _ in PAIR]
    hop3 = [shaped({o[2]: 1, 3: 1}) for o in ORDERS for _ in PAIR]
    small = [
        pltpu.VMEM((8, 64, 512), BF16),
        pltpu.VMEM((8, 32), F32),
        pltpu.VMEM((8, 32), F32),
        pltpu.VMEM((LATENT,), BF16),
        pltpu.SMEM((REQ,), jnp.int32),
        pltpu.VMEM((4, 16, 512), BF16),
        pltpu.VMEM((4, 16, 64), BF16),
        pltpu.VMEM((4, LATENT, LANES), BF16),
        pltpu.VMEM((KEY_COLS, LANES), BF16),
    ]
    sems = [pltpu.SemaphoreType.DMA((n,)) for n in (LOADS, 2, GROUPS)]
    return pl.pallas_call(
        exchange_kernel,
        out_shape=[
            pltpu.VMEM((4, 4, 4, 4, 2, 8, 512), BF16),
            pltpu.VMEM((4, 64, 1024), BF16),
            pltpu.VMEM(FULL[:COL] + (LANES,), F32),
            pltpu.VMEM((8, LANES), jnp.int32),
        ],
        in_specs=[pl.BlockSpec(memory_space=pltpu.HBM)] * 8,
        out_specs=[pl.BlockSpec(memory_space=pltpu.VMEM)] * 4,
        scratch_shapes=[[pltpu.VMEM((9,) + FULL, BF16), shaped({COL: KEY_COLS}), hop1, hop1, hop2, hop3, small, sems]],
        compiler_params=pltpu.CompilerParams(collective_id=0, has_side_effects=True, vmem_limit_bytes=40 * 1024 * 1024),
        name="exchange",
    )(c_raw, k_turned, rope_cos, rope_sin, gain, seq_lens, q_lat, q_rope)


def attend_kernel(c_ref, kr_ref, score_ref, len_ref, c_out, kr_out, o_out, o_buf, sem):
    writes = []

    def write(a, b):
        writes.append(pltpu.make_async_copy(a, b, sem.at[len(writes)]))
        writes[-1].start()

    for j in REQUESTS:
        for half in PAIR:
            rows = pl.ds(half * (POSITIONS // 2), POSITIONS // 2)
            write(c_ref.at[j, rows], c_out.at[j, rows])
    write(kr_ref, kr_out)
    row = lax.broadcasted_iota(jnp.int32, (POSITIONS, LANES), 0)
    scores = jnp.where(row < len_ref[0:1, :], score_ref[...] * ATTN_SCALE, -1e30)
    weights = jnp.exp(scores - jnp.max(scores, axis=0, keepdims=True)).T
    weight_sum = jnp.sum(weights[: 4 * HEADS], axis=1, keepdims=True)
    rounded = weights[: 4 * HEADS].astype(BF16)
    for j in REQUESTS:
        mine = slice(HEADS * j, HEADS * (j + 1))
        weighted = jnp.dot(rounded[mine], c_ref[j], preferred_element_type=F32)
        o_buf[j] = (weighted / weight_sum[mine]).astype(BF16)
        write(o_buf.at[j], o_out.at[j])
    for copy in writes:
        copy.wait()


def attend(c_cache, kr_turned, scores, lens):
    whole = pl.BlockSpec(memory_space=pltpu.VMEM)
    return pl.pallas_call(
        attend_kernel,
        out_shape=[
            jax.ShapeDtypeStruct(c_cache.shape, BF16),
            jax.ShapeDtypeStruct(kr_turned.shape, BF16),
            jax.ShapeDtypeStruct((4, HEADS, LATENT), BF16),
        ],
        in_specs=[whole] * 4,
        out_specs=[pl.BlockSpec(memory_space=pltpu.HBM)] * 3,
        scratch_shapes=[pltpu.VMEM((4, HEADS, LATENT), BF16), pltpu.SemaphoreType.DMA((13,))],
        compiler_params=pltpu.CompilerParams(vmem_limit_bytes=24 * 1024 * 1024),
        name="attend",
    )(c_cache, kr_turned, scores, lens)


def solution(mesh):
    seq_spec = P("dp", "x", None)
    req_spec = P(("dp", "x"), None, None)

    def local_step(c_raw, k_raw, norm_gain, rope_cos, rope_sin, seq_lens, q_lat, q_rope):
        args = (c_raw.reshape(FULL[:4] + (4, 8, LATENT)), k_raw.transpose(1, 2, 0), rope_cos, rope_sin, norm_gain, seq_lens, q_lat, q_rope)
        c_cache, kr_turned, scores, lens = exchange(*[pltpu.with_memory_space_constraint(arg, pltpu.HBM) for arg in args])
        c_cache, kr_turned, o_lat = attend(c_cache.reshape(4, POSITIONS, LATENT), kr_turned, scores.reshape(POSITIONS, LANES), lens)
        return c_cache, kr_turned.transpose(0, 2, 1), o_lat

    return jax.shard_map(local_step, mesh=mesh, in_specs=(seq_spec, seq_spec, P(None), P("x", None), P("x", None), P("dp"), req_spec, req_spec), out_specs=(req_spec, req_spec, req_spec), check_vma=False)
```

```python
import jax
import jax.numpy as jnp
from jax import lax
from jax.experimental import pallas as pl
from jax.experimental.pallas import tpu as pltpu
from jax.sharding import PartitionSpec as P

NORM_EPS = 1e-6
ATTN_SCALE = (512 + 64) ** -0.5
ORDERS = ((0, 1, 2), (1, 2, 0), (2, 0, 1))
FULL = (4, 4, 4, 2, 8, 768)
STRIDES = (256, 64, 16)
POSITIONS, LATENT, ROPE, HEADS, LANES = 1024, 512, 64, 16, 128
ROWS = 64
KEY_COLS = 256
C_COLS, K_COLS, ALL_COLS = (0, LATENT), (LATENT, KEY_COLS), (0, LATENT + KEY_COLS)
CORE, COL = 3, 5
PARTS = range(3)
PAIR = range(2)
REQUESTS = range(4)
REQ = 512
GROUPS = 23
LOADS = 9
SIGNS = (1, -1)
OFFSETS = (0, -1, 1, 2)
NT = (((1,), (1,)), ((), ()))
F32, BF16 = jnp.float32, jnp.bfloat16


def all_parts(step, *args):
    for p in PARTS:
        step(p, *args)


def index(sel, dims=len(FULL)):
    return tuple(pl.ds(*sel[d]) if d in sel else slice(None) for d in range(dims))


def one(i):
    return (i, 1)


def place_of(me):
    return (me // 32, (me // 8) % 4, (me // 2) % 4)


def stepper(place):
    return lambda dim, delta: (place[dim] + delta + 4) % 4


def row_work(at, length, got, gain_row, q_cols, qk_cols, c_out, kr_out, score_out):
    def row_positions(a, b, c, ib, ic):
        r = lax.broadcasted_iota(jnp.int32, (ROWS, 1), 0)
        return (r // 16) * STRIDES[a] + r % 16 + ib * STRIDES[b] + ic * STRIDES[c]

    def unit_shape(a, width):
        return tuple(4 if d == a else 1 for d in range(3)) + (2, 8, width)

    def add_scores(a, wheres, rows, columns):
        part = jnp.dot(jnp.concatenate(rows, axis=0), columns, preferred_element_type=F32)
        for i, where in enumerate(wheres):
            score_out[where] += part[ROWS * i : ROWS * (i + 1)].reshape(unit_shape(a, LANES))

    def finish(j, a, wheres, raws, positions):
        gain = gain_row()
        rows = []
        for where, raw, pos in zip(wheres, raws, positions):
            square = jnp.sum(raw * raw, axis=-1, keepdims=True) * (1.0 / LATENT)
            inv_rms = jnp.where(pos < length(j), lax.rsqrt(square + NORM_EPS), 0.0)
            c_norm = raw * inv_rms * gain
            c_out[(j,) + where] = c_norm.reshape(unit_shape(a, LATENT)).astype(BF16)
            rows.append(c_norm.astype(BF16))
        add_scores(a, wheres, rows, q_cols[j])

    def units(p, off, steps):
        a, b, c = ORDERS[p]
        ib, ics = at(b, off), [at(c, step) for step in steps]
        wheres = [index({b: one(ib), c: one(ic)})[:COL] for ic in ics]
        full = [where + (slice(None),) for where in wheres]
        raws = [got[p][where + (pl.ds(*C_COLS),)].astype(F32).reshape(ROWS, LATENT) for where in wheres]
        finish(p, a, full, raws, [row_positions(a, b, c, ib, ic) for ic in ics])
        if p == 2:
            tiles = [got[2][where + (pl.ds(*K_COLS),)].astype(F32).reshape(ROWS, KEY_COLS).astype(BF16) for where in wheres]
            add_scores(a, full, tiles, qk_cols[...])

    def key_columns(z):
        row = lax.broadcasted_iota(jnp.int32, (KEY_COLS, KEY_COLS), 0)
        col = lax.broadcasted_iota(jnp.int32, (KEY_COLS, KEY_COLS), 1)
        eye = jnp.where(row == col, 1.0, 0.0).astype(BF16)
        tile = got[2][pl.ds(z, 1), :, :, :, :, pl.ds(*K_COLS)].astype(F32).reshape(KEY_COLS, KEY_COLS).astype(BF16)
        turned = lax.dot_general(eye, tile, NT, preferred_element_type=F32)
        for j in REQUESTS:
            valid = col[:ROPE] + z * KEY_COLS < length(j)
            kr_out[j, :, pl.ds(pl.multiple_of(z * KEY_COLS, KEY_COLS), KEY_COLS)] = jnp.where(valid, turned[ROPE * j : ROPE * (j + 1)], 0.0).astype(BF16)

    def last_request(steps):
        places = [(at(1, y), at(2, x)) for y, x in steps]
        wheres = [index({1: one(y), 2: one(x)})[:COL] for y, x in places]
        raws = [jnp.concatenate([got[p][where + (pl.ds(*K_COLS),)].astype(F32).reshape(ROWS, KEY_COLS) for p in PAIR], axis=1) for where in wheres]
        finish(3, 0, [where + (slice(None),) for where in wheres], raws, [row_positions(0, 1, 2, y, x) for y, x in places])

    return units, last_request, key_columns


def exchange_kernel(c_ref, k_ref, cos_ref, sin_ref, gain_ref, len_ref, qlat_ref, qrope_ref, c_out, kr_out, score_out, len_out, got, q_cols, qk_cols, gain_out, scratch):
    parts, k_laid, hop1, hop2, hop3, small, sems = scratch
    mid1, mid2 = [[parts.at[3 * stage + p] for p in PARTS] for stage in PAIR]
    got = [got.at[p] for p in PARTS]
    k_buf, cos_buf, sin_buf, gain_buf, len_buf, qlat_buf, qrope_buf = small
    load_sem, send_sem, recv_sem = sems

    me = lax.axis_index("x")
    core = me % 2
    other = me + 1 - 2 * core
    cores = (core, 1 - core)
    place = place_of(me)
    at = stepper(place)

    def device(dim, delta, to_core=None):
        pos = list(place)
        pos[dim] = (pos[dim] + delta + 4) % 4
        last = core if to_core is None else to_core
        return ((pos[0] * 4 + pos[1]) * 4 + pos[2]) * 2 + last

    def halves(s):
        return (2 * s, 2)

    def view(ref, sel):
        return ref.at[index(sel)]

    barrier = pltpu.get_barrier_semaphore()
    for dim in PARTS:
        for delta in SIGNS:
            for k in PAIR:
                pl.semaphore_signal(barrier, inc=1, device_id={"x": device(dim, delta, k)}, device_id_type=pl.DeviceIdType.MESH)
    pl.semaphore_signal(barrier, inc=1, device_id={"x": other}, device_id_type=pl.DeviceIdType.MESH)

    def taken(sem, n, shape):
        block = parts.at[(pl.ds(0, n),) + index(shape)]
        pltpu.make_async_copy(block, block, sem).wait()

    def taken_from(p, sel, extra):
        where = index(sel, COL - 1)
        if extra:
            return c_ref.at[where + (3, slice(None), pl.ds(KEY_COLS * p, KEY_COLS))]
        return c_ref.at[where + (p, slice(None), pl.ds(*C_COLS))]

    def load(slot, a, b):
        copy = pltpu.make_async_copy(a, b, load_sem.at[slot])
        copy.start()
        return copy

    key_loads = [load(i, a, b) for i, (a, b) in enumerate(((k_ref, k_buf), (cos_ref, cos_buf), (sin_ref, sin_buf)))]
    other_loads = [load(3 + i, a, b) for i, (a, b) in enumerate(((gain_ref, gain_buf), (len_ref, len_buf), (qlat_ref, qlat_buf), (qrope_ref, qrope_buf)))]
    for p in PARTS:
        own = {ORDERS[p][0]: one(place[ORDERS[p][0]])}
        load(LOADS - 1 if p == 2 else LOADS - 2, taken_from(p, own, False), view(mid1[p], {**own, COL: C_COLS}))
        if p < 2:
            load(LOADS - 2, taken_from(p, own, True), view(mid1[p], {**own, COL: K_COLS}))

    slots = {}

    def send(group, a, b, to, sent=0):
        slot = slots.setdefault(group, len(slots))
        pltpu.make_async_remote_copy(src_ref=a, dst_ref=b, send_sem=send_sem.at[sent], recv_sem=recv_sem.at[slot], device_id={"x": to}, device_id_type=pl.DeviceIdType.MESH).start()

    def arrived(group, n, shape):
        taken(recv_sem.at[slots[group]], n, shape)

    def held(p, sel, cols):
        if cols == C_COLS:
            return taken_from(p, sel, False)
        return taken_from(p, sel, True) if p < 2 else view(k_laid, sel)

    def first_group(p, cols):
        return ("1far", cols if p == 2 else None)

    def far1(p, cols):
        a, b, _ = ORDERS[p]
        wide = {COL: cols}
        for s, sign in enumerate(SIGNS):
            send(first_group(p, cols), held(p, {a: one(at(a, 2)), b: halves(s)}, cols), view(hop1[2 * p + s], wide), device(a, sign))

    def near1(p, cols):
        a, b, _ = ORDERS[p]
        wide = {COL: cols}
        for s, sign in enumerate(SIGNS):
            send("1near", held(p, {a: one(at(a, sign))}, cols), view(mid1[p], {a: one(place[a]), **wide}), device(a, sign))

    def forward1(p, cols=ALL_COLS):
        a, b, _ = ORDERS[p]
        wide = {COL: cols}
        for s, sign in enumerate(SIGNS):
            send("1fwd", view(hop1[2 * p + s], wide), view(mid1[p], {a: one(at(a, -sign)), b: halves(s), **wide}), device(a, sign))

    def phase2(p, off):
        a, b, c = ORDERS[p]
        sa = {a: one(at(a, off))}
        hop_sa = {a: one(off % 4)}
        for s, sign in enumerate(SIGNS):
            send(("2far", off), view(mid1[p], {**sa, b: one(at(b, 2)), c: halves(s)}), view(hop2[2 * p + s], hop_sa), device(b, sign))
        for s, sign in enumerate(SIGNS):
            send("2near", view(mid1[p], {**sa, b: one(at(b, sign))}), view(mid2[p], {**sa, b: one(place[b])}), device(b, sign))

    def forward2(p, off):
        a, b, c = ORDERS[p]
        sa = {a: one(at(a, off))}
        hop_sa = {a: one(off % 4)}
        for s, sign in enumerate(SIGNS):
            send("2fwd", view(hop2[2 * p + s], hop_sa), view(mid2[p], {**sa, b: one(at(b, -sign)), c: halves(s)}), device(b, sign))

    def phase3(p, off):
        a, b, c = ORDERS[p]
        sb = {b: one(at(b, off))}
        hop_sb = {b: one(off % 4)}
        got_b = mid1[p] if off == 0 else mid2[p]
        mine = {**sb, c: one(place[c]), CORE: one(core)}
        for s, sign in enumerate(SIGNS):
            send(("3far", off), view(got_b, {**sb, c: one(at(c, 2)), CORE: one(cores[s])}), view(hop3[2 * p + s], hop_sb), device(c, sign))
        for s, sign in enumerate(SIGNS):
            for k in PAIR:
                send(("3near", off), view(got_b, {**sb, c: one(at(c, sign)), CORE: one(cores[k])}), view(got[p], mine), device(c, sign, cores[k]))
        send(("3near", off), view(got_b, {**sb, c: one(place[c]), CORE: one(cores[1])}), view(got[p], mine), other, 1)
        got[p][index(mine)] = got_b[index(mine)]

    def forward3(p, off):
        a, b, c = ORDERS[p]
        sb = {b: one(at(b, off))}
        hop_sb = {b: one(off % 4)}
        for s, sign in enumerate(SIGNS):
            send(("3fwd", off), view(hop3[2 * p + s], hop_sb), view(got[p], {**sb, c: one(at(c, -sign)), CORE: one(core)}), device(c, sign, cores[s]))

    def length(j):
        return len_buf[4 * me + j]

    def keys():
        row = lax.broadcasted_iota(jnp.int32, (32, 32), 0)
        diag = row == lax.broadcasted_iota(jnp.int32, (32, 32), 1)
        roped = []
        for pos in range(8):
            cos = jnp.sum(jnp.where(diag, cos_buf[pos : pos + 1, :], 0.0), axis=1, keepdims=True)
            sin = jnp.sum(jnp.where(diag, sin_buf[pos : pos + 1, :], 0.0), axis=1, keepdims=True)
            lo = k_buf[pos, 0:32, :].astype(F32)
            hi = k_buf[pos, 32:64, :].astype(F32)
            roped.append(jnp.concatenate([lo * cos - hi * sin, hi * cos + lo * sin], axis=0).astype(BF16))
        out_row = lax.broadcasted_iota(jnp.int32, (256, 128), 0)
        lane = lax.broadcasted_iota(jnp.int32, (256, 128), 1)
        picks = [jnp.where((out_row % 8 == pos) & (out_row // 8 == lane // 4), 1.0, 0.0).astype(BF16) for pos in range(8)]
        pick = jnp.concatenate(picks, axis=1)
        request = lax.broadcasted_iota(jnp.int32, (64, 1024), 1) % 4
        for z in REQUESTS:
            cat = jnp.concatenate([r[:, 128 * z : 128 * (z + 1)] for r in roped], axis=1)
            masked = jnp.concatenate([jnp.where(request == j, cat, jnp.zeros_like(cat)) for j in REQUESTS], axis=0)
            laid = lax.dot_general(pick, masked, NT, preferred_element_type=F32)
            laid = laid.reshape(1, 4, 4, 2, 8, 256).astype(BF16)
            k_laid[z : z + 1] = laid
        own = {2: one(place[2])}
        mid1[2][index({**own, COL: K_COLS})] = k_laid[index(own)]

    def queries():
        for j in REQUESTS:
            rows = [qlat_buf[j].astype(F32) if i == j else jnp.zeros((HEADS, LATENT), F32) for i in REQUESTS]
            q_cols[j] = jnp.concatenate(rows + [jnp.zeros((LANES - 4 * HEADS, LATENT), F32)], axis=0).T.astype(BF16)
        zero = jnp.zeros((HEADS, ROPE), F32)
        rows = [jnp.concatenate([qrope_buf[j].astype(F32) if i == j else zero for i in REQUESTS], axis=1) for j in REQUESTS]
        qk_cols[...] = jnp.concatenate(rows + [jnp.zeros((LANES - 4 * HEADS, KEY_COLS), F32)], axis=0).T.astype(BF16)
        score_out[...] = jnp.zeros_like(score_out)
        lane = lax.broadcasted_iota(jnp.int32, (8, LANES), 1)
        lens = jnp.zeros((8, LANES), jnp.int32)
        for j in REQUESTS:
            lens = jnp.where(lane // HEADS == j, length(j), lens)
            len_out[j] = jnp.zeros((8, LANES), jnp.int32) + length(j)
        len_out[4] = lens
        gain_out[...] = jnp.broadcast_to(gain_buf[...].astype(F32).reshape(1, LATENT), gain_out.shape)

    units, last_request, key_columns = row_work(at, length, got, lambda: gain_out[0:1, :], q_cols, qk_cols, c_out, kr_out, score_out)

    def near_units(off):
        arrived(("3near", off), 5, {0: (0, 3), 1: one(0), CORE: one(0)})
        all_parts(units, off, OFFSETS[:3])

    def far_units(off):
        arrived(("3fwd", off), 3, {0: one(0), 1: one(0)})
        all_parts(units, off, OFFSETS[3:])
        key_columns(at(ORDERS[2][1], off))

    EIGHTH, SIXTEENTH = {0: one(0), 1: (0, 2)}, {0: one(0), 1: one(0)}
    pl.semaphore_wait(barrier, 13)
    for first in (far1, near1):
        all_parts(first, C_COLS)
        first(0, K_COLS)
        first(1, K_COLS)
    for copy in key_loads:
        copy.wait()
    keys()
    for copy in other_loads:
        copy.wait()
    queries()
    far1(2, K_COLS)
    near1(2, K_COLS)
    taken(load_sem.at[LOADS - 2], 2, {0: one(0)})
    taken(load_sem.at[LOADS - 1], 1, {0: one(0), COL: C_COLS})
    arrived(first_group(0, None), 2, {0: one(0)})
    forward1(0)
    forward1(1)
    arrived(first_group(2, C_COLS), 1, {0: one(0), COL: C_COLS})
    forward1(2, C_COLS)
    all_parts(phase2, 0)
    arrived(first_group(2, K_COLS), 1, {0: one(0), COL: K_COLS})
    forward1(2, K_COLS)
    arrived("1near", 3, {0: (0, 2)})
    all_parts(phase2, -1)
    all_parts(phase2, 1)
    arrived(("2far", 0), 3, SIXTEENTH)
    all_parts(forward2, 0)
    arrived("1fwd", 3, {0: one(0)})
    all_parts(phase2, 2)
    for off in (-1, 1):
        arrived(("2far", off), 3, SIXTEENTH)
        all_parts(forward2, off)
    arrived(("2far", 2), 3, SIXTEENTH)
    all_parts(forward2, 2)
    all_parts(phase3, 0)
    arrived("2near", 3, {0: (0, 2)})
    all_parts(phase3, -1)
    arrived(("3far", 0), 3, SIXTEENTH)
    all_parts(forward3, 0)
    all_parts(phase3, 1)
    near_units(0)
    arrived("2fwd", 3, {0: one(0)})
    arrived(("3far", -1), 3, SIXTEENTH)
    all_parts(forward3, -1)
    all_parts(phase3, 2)
    near_units(-1)
    far_units(0)
    arrived(("3far", 1), 3, SIXTEENTH)
    all_parts(forward3, 1)
    near_units(1)
    far_units(-1)
    last_request([(y, x) for y in OFFSETS[:2] for x in OFFSETS[:2]])
    arrived(("3far", 2), 3, SIXTEENTH)
    all_parts(forward3, 2)
    near_units(2)
    far_units(1)
    last_request([(y, x) for y in OFFSETS for x in OFFSETS[:3] if y > 0 or x > 0])
    arrived(("3fwd", 2), 3, SIXTEENTH)
    taken(send_sem.at[0], 9, {})
    taken(send_sem.at[1], 3, EIGHTH)


def exchange(c_raw, k_turned, rope_cos, rope_sin, gain, seq_lens, q_lat, q_rope):
    def shaped(sizes):
        return pltpu.VMEM(tuple(sizes.get(d, FULL[d]) for d in range(6)), BF16)

    hop1 = [shaped({o[0]: 1, o[1]: 2}) for o in ORDERS for _ in PAIR]
    hop2 = [shaped({o[1]: 1, o[2]: 2}) for o in ORDERS for _ in PAIR]
    hop3 = [shaped({o[2]: 1, 3: 1}) for o in ORDERS for _ in PAIR]
    small = [
        pltpu.VMEM((8, 64, 512), BF16),
        pltpu.VMEM((8, 32), F32),
        pltpu.VMEM((8, 32), F32),
        pltpu.VMEM((LATENT,), BF16),
        pltpu.SMEM((REQ,), jnp.int32),
        pltpu.VMEM((4, 16, 512), BF16),
        pltpu.VMEM((4, 16, 64), BF16),
    ]
    sems = [pltpu.SemaphoreType.DMA((n,)) for n in (LOADS, 2, GROUPS)]
    return pl.pallas_call(
        exchange_kernel,
        out_shape=[
            pltpu.VMEM((4, 4, 4, 4, 2, 8, 512), BF16),
            pltpu.VMEM((4, 64, 1024), BF16),
            pltpu.VMEM(FULL[:COL] + (LANES,), F32),
            pltpu.VMEM((5, 8, LANES), jnp.int32),
            pltpu.VMEM((3,) + FULL, BF16),
            pltpu.VMEM((4, LATENT, LANES), BF16),
            pltpu.VMEM((KEY_COLS, LANES), BF16),
            pltpu.VMEM((8, LATENT), F32),
        ],
        in_specs=[pl.BlockSpec(memory_space=pltpu.HBM)] * 8,
        out_specs=[pl.BlockSpec(memory_space=pltpu.VMEM)] * 8,
        scratch_shapes=[[pltpu.VMEM((9,) + FULL, BF16), shaped({COL: KEY_COLS}), hop1, hop2, hop3, small, sems]],
        compiler_params=pltpu.CompilerParams(collective_id=0, has_side_effects=True, vmem_limit_bytes=40 * 1024 * 1024),
        name="exchange",
    )(c_raw, k_turned, rope_cos, rope_sin, gain, seq_lens, q_lat, q_rope)


def attend_kernel(c_in, kr_in, score_in, len_ref, got_ref, q_cols, qk_cols, gain_ref, c_hbm, kr_hbm, o_hbm, c_buf, kr_buf, scores, o_buf, sem):
    at = stepper(place_of(lax.axis_index("x")))
    writes = []

    def write(a, b):
        writes.append(pltpu.make_async_copy(a, b, sem))
        writes[-1].start()

    def write_rows(j, sel):
        where = (j,) + index(sel)
        write(c_buf.at[where], c_hbm.at[where])

    def write_keys(z):
        where = (slice(None), slice(None), pl.ds(pl.multiple_of(z * KEY_COLS, KEY_COLS), KEY_COLS))
        write(kr_buf.at[where], kr_hbm.at[where])

    near, far = OFFSETS[:3], OFFSETS[3]
    for p, (_, b, c) in enumerate(ORDERS):
        for off in near:
            write_rows(p, {b: one(at(b, off))})
        for off in near:
            write_rows(p, {b: one(at(b, far)), c: one(at(c, off))})
    for off in near:
        write_rows(3, {2: one(at(2, off))})
        write_keys(at(ORDERS[2][1], off))

    got = [got_ref.at[p] for p in PARTS]
    units, last_request, key_columns = row_work(at, lambda j: len_ref[j, 0:1, 0:1], got, lambda: gain_ref[0:1, :], q_cols, qk_cols, c_buf, kr_buf, scores)
    all_parts(units, far, OFFSETS[3:])
    last_request([(y, far) for y in OFFSETS])
    for p, (_, b, c) in enumerate(ORDERS):
        write_rows(p, {b: one(at(b, far)), c: one(at(c, far))})
    write_rows(3, {2: one(at(2, far))})
    key_columns(at(ORDERS[2][1], far))
    write_keys(at(ORDERS[2][1], far))

    row = lax.broadcasted_iota(jnp.int32, (POSITIONS, LANES), 0)
    masked = jnp.where(row < len_ref[4, 0:1, :], scores[...].reshape(POSITIONS, LANES) * ATTN_SCALE, -1e30)
    weights = jnp.exp(masked - jnp.max(masked, axis=0, keepdims=True)).T
    weight_sum = jnp.sum(weights[: 4 * HEADS], axis=1, keepdims=True)
    rounded = weights[: 4 * HEADS].astype(BF16)
    for j in REQUESTS:
        mine = slice(HEADS * j, HEADS * (j + 1))
        weighted = jnp.dot(rounded[mine], c_buf[j].reshape(POSITIONS, LATENT), preferred_element_type=F32)
        o_buf[j] = (weighted / weight_sum[mine]).astype(BF16)
        write(o_buf.at[j], o_hbm.at[j])
    for copy in writes:
        copy.wait()


def attend(*handed):
    c_cache, kr_turned, scores = handed[:3]
    in_hbm, in_vmem = pl.BlockSpec(memory_space=pltpu.HBM), pl.BlockSpec(memory_space=pltpu.VMEM)
    return pl.pallas_call(
        attend_kernel,
        out_shape=[
            jax.ShapeDtypeStruct(c_cache.shape, BF16),
            jax.ShapeDtypeStruct(kr_turned.shape, BF16),
            jax.ShapeDtypeStruct((4, HEADS, LATENT), BF16),
            pltpu.VMEM(c_cache.shape, BF16),
            pltpu.VMEM(kr_turned.shape, BF16),
            pltpu.VMEM(scores.shape, F32),
        ],
        in_specs=[in_vmem] * len(handed),
        out_specs=[in_hbm] * 3 + [in_vmem] * 3,
        input_output_aliases={0: 3, 1: 4, 2: 5},
        scratch_shapes=[pltpu.VMEM((4, HEADS, LATENT), BF16), pltpu.SemaphoreType.DMA],
        compiler_params=pltpu.CompilerParams(vmem_limit_bytes=16 * 1024 * 1024),
        name="attend",
    )(*handed)[:3]


def solution(mesh):
    seq_spec = P("dp", "x", None)
    req_spec = P(("dp", "x"), None, None)

    def local_step(c_raw, k_raw, norm_gain, rope_cos, rope_sin, seq_lens, q_lat, q_rope):
        args = (c_raw.reshape(FULL[:4] + (4, 8, LATENT)), k_raw.transpose(1, 2, 0), rope_cos, rope_sin, norm_gain, seq_lens, q_lat, q_rope)
        handed = exchange(*[pltpu.with_memory_space_constraint(arg, pltpu.HBM) for arg in args])
        c_cache, kr_turned, o_lat = attend(*handed)
        c_cache = c_cache.reshape(4, POSITIONS, LATENT)
        return c_cache, kr_turned.transpose(0, 2, 1), o_lat

    return jax.shard_map(local_step, mesh=mesh, in_specs=(seq_spec, seq_spec, P(None), P("x", None), P("x", None), P("dp"), req_spec, req_spec), out_specs=(req_spec, req_spec, req_spec), check_vma=False)
```

```python
import jax
import jax.numpy as jnp
from jax import lax
from jax.experimental import pallas as pl
from jax.experimental.pallas import tpu as pltpu
from jax.sharding import PartitionSpec as P

NORM_EPS = 1e-6
ATTN_SCALE = (512 + 64) ** -0.5
ORDERS = ((0, 1, 2), (1, 2, 0), (2, 0, 1))
FULL = (4, 4, 4, 2, 8, 768)
STRIDES = (256, 64, 16)
POSITIONS, LATENT, ROPE, HEADS, LANES = 1024, 512, 64, 16, 128
ROWS = 64
KEY_COLS = 256
C_COLS, K_COLS, ALL_COLS = (0, LATENT), (LATENT, KEY_COLS), (0, LATENT + KEY_COLS)
CORE, COL = 3, 5
PARTS = range(3)
PAIR = range(2)
REQUESTS = range(4)
REQ = 512
GROUPS = 23
LOADS = 9
SIGNS = (1, -1)
OFFSETS = (0, -1, 1, 2)
NT = (((1,), (1,)), ((), ()))
F32, BF16 = jnp.float32, jnp.bfloat16


def all_parts(step, *args):
    for p in PARTS:
        step(p, *args)


def index(sel, dims=len(FULL)):
    return tuple(pl.ds(*sel[d]) if d in sel else slice(None) for d in range(dims))


def one(i):
    return (i, 1)


def place_of(me):
    return (me // 32, (me // 8) % 4, (me // 2) % 4)


def stepper(place):
    return lambda dim, delta: (place[dim] + delta + 4) % 4


def row_work(at, length, got, gain_row, q_cols, qk_cols, c_out, kr_out, score_out):
    def row_positions(a, b, c, ib, ic):
        r = lax.broadcasted_iota(jnp.int32, (ROWS, 1), 0)
        return (r // 16) * STRIDES[a] + r % 16 + ib * STRIDES[b] + ic * STRIDES[c]

    def unit_shape(a, width):
        return tuple(4 if d == a else 1 for d in range(3)) + (2, 8, width)

    def add_scores(a, wheres, rows, columns):
        part = jnp.dot(jnp.concatenate(rows, axis=0), columns, preferred_element_type=F32)
        for i, where in enumerate(wheres):
            score_out[where] += part[ROWS * i : ROWS * (i + 1)].reshape(unit_shape(a, LANES))

    def finish(j, a, wheres, raws, positions):
        gain = gain_row()
        rows = []
        for where, raw, pos in zip(wheres, raws, positions):
            square = jnp.sum(raw * raw, axis=-1, keepdims=True) * (1.0 / LATENT)
            inv_rms = jnp.where(pos < length(j), lax.rsqrt(square + NORM_EPS), 0.0)
            c_norm = raw * inv_rms * gain
            c_out[(j,) + where] = c_norm.reshape(unit_shape(a, LATENT)).astype(BF16)
            rows.append(c_norm.astype(BF16))
        add_scores(a, wheres, rows, q_cols[j])

    def units(p, off, steps):
        a, b, c = ORDERS[p]
        ib, ics = at(b, off), [at(c, step) for step in steps]
        wheres = [index({b: one(ib), c: one(ic)})[:COL] for ic in ics]
        full = [where + (slice(None),) for where in wheres]
        raws = [got[p][where + (pl.ds(*C_COLS),)].astype(F32).reshape(ROWS, LATENT) for where in wheres]
        finish(p, a, full, raws, [row_positions(a, b, c, ib, ic) for ic in ics])
        if p == 2:
            tiles = [got[2][where + (pl.ds(*K_COLS),)].astype(F32).reshape(ROWS, KEY_COLS).astype(BF16) for where in wheres]
            add_scores(a, full, tiles, qk_cols[...])

    def key_columns(z):
        row = lax.broadcasted_iota(jnp.int32, (KEY_COLS, KEY_COLS), 0)
        col = lax.broadcasted_iota(jnp.int32, (KEY_COLS, KEY_COLS), 1)
        eye = jnp.where(row == col, 1.0, 0.0).astype(BF16)
        tile = got[2][pl.ds(z, 1), :, :, :, :, pl.ds(*K_COLS)].astype(F32).reshape(KEY_COLS, KEY_COLS).astype(BF16)
        turned = lax.dot_general(eye, tile, NT, preferred_element_type=F32)
        for j in REQUESTS:
            valid = col[:ROPE] + z * KEY_COLS < length(j)
            kr_out[j, :, pl.ds(pl.multiple_of(z * KEY_COLS, KEY_COLS), KEY_COLS)] = jnp.where(valid, turned[ROPE * j : ROPE * (j + 1)], 0.0).astype(BF16)

    def last_request(steps):
        places = [(at(1, y), at(2, x)) for y, x in steps]
        wheres = [index({1: one(y), 2: one(x)})[:COL] for y, x in places]
        raws = [jnp.concatenate([got[p][where + (pl.ds(*K_COLS),)].astype(F32).reshape(ROWS, KEY_COLS) for p in PAIR], axis=1) for where in wheres]
        finish(3, 0, [where + (slice(None),) for where in wheres], raws, [row_positions(0, 1, 2, y, x) for y, x in places])

    return units, last_request, key_columns


def exchange_kernel(c_ref, k_ref, cos_ref, sin_ref, gain_ref, len_ref, qlat_ref, qrope_ref, c_out, kr_out, score_out, len_out, got, q_cols, qk_cols, gain_out, scratch):
    parts, k_laid, hop1, hop2, hop3, hop4, small, sems = scratch
    mid1, mid2 = [[parts.at[3 * stage + p] for p in PARTS] for stage in PAIR]
    got = [got.at[p] for p in PARTS]
    k_buf, cos_buf, sin_buf, gain_buf, len_buf, qlat_buf, qrope_buf = small
    load_sem, send_sem, recv_sem = sems

    me = lax.axis_index("x")
    core = me % 2
    other = me + 1 - 2 * core
    cores = (core, 1 - core)
    place = place_of(me)
    at = stepper(place)

    def device(dim, delta, to_core=None):
        pos = list(place)
        pos[dim] = (pos[dim] + delta + 4) % 4
        last = core if to_core is None else to_core
        return ((pos[0] * 4 + pos[1]) * 4 + pos[2]) * 2 + last

    def halves(s):
        return (2 * s, 2)

    def view(ref, sel):
        return ref.at[index(sel)]

    barrier = pltpu.get_barrier_semaphore()
    for dim in PARTS:
        for delta in SIGNS:
            for k in PAIR:
                pl.semaphore_signal(barrier, inc=1, device_id={"x": device(dim, delta, k)}, device_id_type=pl.DeviceIdType.MESH)
    pl.semaphore_signal(barrier, inc=1, device_id={"x": other}, device_id_type=pl.DeviceIdType.MESH)

    def taken(sem, n, shape):
        block = parts.at[(pl.ds(0, n),) + index(shape)]
        pltpu.make_async_copy(block, block, sem).wait()

    def taken_from(p, sel, extra):
        where = index(sel, COL - 1)
        if extra:
            return c_ref.at[where + (3, slice(None), pl.ds(KEY_COLS * p, KEY_COLS))]
        return c_ref.at[where + (p, slice(None), pl.ds(*C_COLS))]

    def load(slot, a, b):
        copy = pltpu.make_async_copy(a, b, load_sem.at[slot])
        copy.start()
        return copy

    key_loads = [load(i, a, b) for i, (a, b) in enumerate(((k_ref, k_buf), (cos_ref, cos_buf), (sin_ref, sin_buf)))]
    other_loads = [load(3 + i, a, b) for i, (a, b) in enumerate(((gain_ref, gain_buf), (len_ref, len_buf), (qlat_ref, qlat_buf), (qrope_ref, qrope_buf)))]
    for p in PARTS:
        own = {ORDERS[p][0]: one(place[ORDERS[p][0]])}
        load(LOADS - 1 if p == 2 else LOADS - 2, taken_from(p, own, False), view(mid1[p], {**own, COL: C_COLS}))
        if p < 2:
            load(LOADS - 2, taken_from(p, own, True), view(mid1[p], {**own, COL: K_COLS}))

    slots = {}

    def send(group, a, b, to, sent=0):
        slot = slots.setdefault(group, len(slots))
        pltpu.make_async_remote_copy(src_ref=a, dst_ref=b, send_sem=send_sem.at[sent], recv_sem=recv_sem.at[slot], device_id={"x": to}, device_id_type=pl.DeviceIdType.MESH).start()

    def arrived(group, n, shape):
        taken(recv_sem.at[slots[group]], n, shape)

    def held(p, sel, cols):
        if cols == C_COLS:
            return taken_from(p, sel, False)
        return taken_from(p, sel, True) if p < 2 else view(k_laid, sel)

    def first_group(p, cols):
        return ("1far", cols if p == 2 else None)

    def far1(p, cols):
        a, b, _ = ORDERS[p]
        wide = {COL: cols}
        for s, sign in enumerate(SIGNS):
            send(first_group(p, cols), held(p, {a: one(at(a, 2)), b: halves(s)}, cols), view(hop1[2 * p + s], wide), device(a, sign))

    def near1(p, cols):
        a, b, _ = ORDERS[p]
        wide = {COL: cols}
        for s, sign in enumerate(SIGNS):
            send("1near", held(p, {a: one(at(a, sign))}, cols), view(mid1[p], {a: one(place[a]), **wide}), device(a, sign))

    def forward1(p, cols=ALL_COLS):
        a, b, _ = ORDERS[p]
        wide = {COL: cols}
        for s, sign in enumerate(SIGNS):
            send("1fwd", view(hop1[2 * p + s], wide), view(mid1[p], {a: one(at(a, -sign)), b: halves(s), **wide}), device(a, sign))

    def phase2(p, off):
        a, b, c = ORDERS[p]
        sa = {a: one(at(a, off))}
        hop_sa = {a: one(off % 4)}
        for s, sign in enumerate(SIGNS):
            send(("2far", off), view(mid1[p], {**sa, b: one(at(b, 2)), c: halves(s)}), view(hop2[2 * p + s], hop_sa), device(b, sign))
        for s, sign in enumerate(SIGNS):
            send("2near", view(mid1[p], {**sa, b: one(at(b, sign))}), view(mid2[p], {**sa, b: one(place[b])}), device(b, sign))

    def forward2(p, off):
        a, b, c = ORDERS[p]
        sa = {a: one(at(a, off))}
        hop_sa = {a: one(off % 4)}
        for s, sign in enumerate(SIGNS):
            send("2fwd", view(hop2[2 * p + s], hop_sa), view(mid2[p], {**sa, b: one(at(b, -sign)), c: halves(s)}), device(b, sign))

    def phase3(p, off):
        a, b, c = ORDERS[p]
        sb = {b: one(at(b, off))}
        got_b = mid1[p] if off == 0 else mid2[p]
        mine = {**sb, c: one(place[c]), CORE: one(core)}
        for s, sign in enumerate(SIGNS):
            far = view(got_b, {**sb, c: one(at(c, 2)), CORE: one(cores[s])})
            if off == 2:
                send(("3far", off), far, view(hop4[2 * p + s], {CORE: one(core)}), device(c, sign, 1), 2)
            else:
                send(("3far", off), far, view(hop3[2 * p + s], {b: one(off % 4)}), device(c, sign), 2)
        for s, sign in enumerate(SIGNS):
            for k in PAIR:
                send(("3near", off), view(got_b, {**sb, c: one(at(c, sign)), CORE: one(cores[k])}), view(got[p], mine), device(c, sign, cores[k]), 2)
        send(("3near", off), view(got_b, {**sb, c: one(place[c]), CORE: one(cores[1])}), view(got[p], mine), other, 1)
        got[p][index(mine)] = got_b[index(mine)]

    def forward3(p, off):
        a, b, c = ORDERS[p]
        sb = {b: one(at(b, off))}
        for s, sign in enumerate(SIGNS):
            send(("3fwd", off), view(hop3[2 * p + s], {b: one(off % 4)}), view(got[p], {**sb, c: one(at(c, -sign)), CORE: one(core)}), device(c, sign, cores[s]), 2)

    def last_forward(p, to):
        a, b, c = ORDERS[p]
        for s, sign in enumerate(SIGNS):
            origin = one(1 - to if s else to)
            send(("3fwd", 2), view(hop4[2 * p + s], {CORE: origin}), view(got[p], {b: one(at(b, 2)), c: one(at(c, -sign)), CORE: origin}), device(c, sign, to), 3)

    def length(j):
        return len_buf[4 * me + j]

    def keys():
        row = lax.broadcasted_iota(jnp.int32, (32, 32), 0)
        diag = row == lax.broadcasted_iota(jnp.int32, (32, 32), 1)
        roped = []
        for pos in range(8):
            cos = jnp.sum(jnp.where(diag, cos_buf[pos : pos + 1, :], 0.0), axis=1, keepdims=True)
            sin = jnp.sum(jnp.where(diag, sin_buf[pos : pos + 1, :], 0.0), axis=1, keepdims=True)
            lo = k_buf[pos, 0:32, :].astype(F32)
            hi = k_buf[pos, 32:64, :].astype(F32)
            roped.append(jnp.concatenate([lo * cos - hi * sin, hi * cos + lo * sin], axis=0).astype(BF16))
        out_row = lax.broadcasted_iota(jnp.int32, (256, 128), 0)
        lane = lax.broadcasted_iota(jnp.int32, (256, 128), 1)
        picks = [jnp.where((out_row % 8 == pos) & (out_row // 8 == lane // 4), 1.0, 0.0).astype(BF16) for pos in range(8)]
        pick = jnp.concatenate(picks, axis=1)
        request = lax.broadcasted_iota(jnp.int32, (64, 1024), 1) % 4
        for z in REQUESTS:
            cat = jnp.concatenate([r[:, 128 * z : 128 * (z + 1)] for r in roped], axis=1)
            masked = jnp.concatenate([jnp.where(request == j, cat, jnp.zeros_like(cat)) for j in REQUESTS], axis=0)
            laid = lax.dot_general(pick, masked, NT, preferred_element_type=F32)
            laid = laid.reshape(1, 4, 4, 2, 8, 256).astype(BF16)
            k_laid[z : z + 1] = laid
        own = {2: one(place[2])}
        mid1[2][index({**own, COL: K_COLS})] = k_laid[index(own)]

    def queries():
        for j in REQUESTS:
            rows = [qlat_buf[j].astype(F32) if i == j else jnp.zeros((HEADS, LATENT), F32) for i in REQUESTS]
            q_cols[j] = jnp.concatenate(rows + [jnp.zeros((LANES - 4 * HEADS, LATENT), F32)], axis=0).T.astype(BF16)
        zero = jnp.zeros((HEADS, ROPE), F32)
        rows = [jnp.concatenate([qrope_buf[j].astype(F32) if i == j else zero for i in REQUESTS], axis=1) for j in REQUESTS]
        qk_cols[...] = jnp.concatenate(rows + [jnp.zeros((LANES - 4 * HEADS, KEY_COLS), F32)], axis=0).T.astype(BF16)
        score_out[...] = jnp.zeros_like(score_out)
        lane = lax.broadcasted_iota(jnp.int32, (8, LANES), 1)
        lens = jnp.zeros((8, LANES), jnp.int32)
        for j in REQUESTS:
            lens = jnp.where(lane // HEADS == j, length(j), lens)
            len_out[j] = jnp.zeros((8, LANES), jnp.int32) + length(j)
        len_out[4] = lens
        gain_out[...] = jnp.broadcast_to(gain_buf[...].astype(F32).reshape(1, LATENT), gain_out.shape)

    units, last_request, key_columns = row_work(at, length, got, lambda: gain_out[0:1, :], q_cols, qk_cols, c_out, kr_out, score_out)

    def near_units(off):
        arrived(("3near", off), 5, {0: (0, 3), 1: one(0), CORE: one(0)})
        all_parts(units, off, OFFSETS[:3])

    def far_units(off):
        arrived(("3fwd", off), 3, {0: one(0), 1: one(0)})
        all_parts(units, off, OFFSETS[3:])
        key_columns(at(ORDERS[2][1], off))

    EIGHTH, SIXTEENTH = {0: one(0), 1: (0, 2)}, {0: one(0), 1: one(0)}
    pl.semaphore_wait(barrier, 13)
    for first in (far1, near1):
        all_parts(first, C_COLS)
        first(0, K_COLS)
        first(1, K_COLS)
    for copy in key_loads:
        copy.wait()
    keys()
    for copy in other_loads:
        copy.wait()
    queries()
    far1(2, K_COLS)
    near1(2, K_COLS)
    taken(load_sem.at[LOADS - 2], 2, {0: one(0)})
    taken(load_sem.at[LOADS - 1], 1, {0: one(0), COL: C_COLS})
    arrived(first_group(0, None), 2, {0: one(0)})
    forward1(0)
    forward1(1)
    arrived(first_group(2, C_COLS), 1, {0: one(0), COL: C_COLS})
    forward1(2, C_COLS)
    all_parts(phase2, 0)
    arrived(first_group(2, K_COLS), 1, {0: one(0), COL: K_COLS})
    forward1(2, K_COLS)
    arrived("1near", 3, {0: (0, 2)})
    all_parts(phase2, -1)
    all_parts(phase2, 1)
    arrived(("2far", 0), 3, SIXTEENTH)
    all_parts(forward2, 0)
    arrived("1fwd", 3, {0: one(0)})
    all_parts(phase2, 2)
    for off in (-1, 1):
        arrived(("2far", off), 3, SIXTEENTH)
        all_parts(forward2, off)
    arrived(("2far", 2), 3, SIXTEENTH)
    all_parts(forward2, 2)
    all_parts(phase3, 0)
    arrived("2near", 3, {0: (0, 2)})
    all_parts(phase3, -1)
    arrived(("3far", 0), 3, SIXTEENTH)
    all_parts(forward3, 0)
    all_parts(phase3, 1)
    near_units(0)
    arrived("2fwd", 3, {0: one(0)})
    arrived(("3far", -1), 3, SIXTEENTH)
    all_parts(forward3, -1)
    all_parts(phase3, 2)
    near_units(-1)
    far_units(0)
    arrived(("3far", 1), 3, SIXTEENTH)
    all_parts(forward3, 1)
    near_units(1)
    far_units(-1)
    last_request([(y, x) for y in OFFSETS[:2] for x in OFFSETS[:2]])
    @pl.when(core == 1)
    def _():
        arrived(("3far", 2), 3, EIGHTH)
        all_parts(last_forward, 0)
        all_parts(last_forward, 1)

    near_units(2)
    far_units(1)
    last_request([(y, x) for y in OFFSETS for x in OFFSETS[:3] if y > 0 or x > 0])
    arrived(("3fwd", 2), 3, SIXTEENTH)
    taken(send_sem.at[0], 6, {})
    taken(send_sem.at[1], 3, EIGHTH)
    taken(send_sem.at[2], 5, {0: (0, 3), 1: (0, 3)})

    @pl.when(core == 1)
    def _():
        taken(send_sem.at[3], 3, EIGHTH)


def exchange(c_raw, k_turned, rope_cos, rope_sin, gain, seq_lens, q_lat, q_rope):
    def shaped(sizes):
        return pltpu.VMEM(tuple(sizes.get(d, FULL[d]) for d in range(6)), BF16)

    hop1 = [shaped({o[0]: 1, o[1]: 2}) for o in ORDERS for _ in PAIR]
    hop2 = [shaped({o[1]: 1, o[2]: 2}) for o in ORDERS for _ in PAIR]
    hop3 = [shaped({o[2]: 1, CORE: 1}) for o in ORDERS for _ in PAIR]
    hop4 = [shaped({o[1]: 1, o[2]: 1}) for o in ORDERS for _ in PAIR]
    small = [
        pltpu.VMEM((8, 64, 512), BF16),
        pltpu.VMEM((8, 32), F32),
        pltpu.VMEM((8, 32), F32),
        pltpu.VMEM((LATENT,), BF16),
        pltpu.SMEM((REQ,), jnp.int32),
        pltpu.VMEM((4, 16, 512), BF16),
        pltpu.VMEM((4, 16, 64), BF16),
    ]
    sems = [pltpu.SemaphoreType.DMA((n,)) for n in (LOADS, 4, GROUPS)]
    return pl.pallas_call(
        exchange_kernel,
        out_shape=[
            pltpu.VMEM((4, 4, 4, 4, 2, 8, 512), BF16),
            pltpu.VMEM((4, 64, 1024), BF16),
            pltpu.VMEM(FULL[:COL] + (LANES,), F32),
            pltpu.VMEM((5, 8, LANES), jnp.int32),
            pltpu.VMEM((3,) + FULL, BF16),
            pltpu.VMEM((4, LATENT, LANES), BF16),
            pltpu.VMEM((KEY_COLS, LANES), BF16),
            pltpu.VMEM((8, LATENT), F32),
        ],
        in_specs=[pl.BlockSpec(memory_space=pltpu.HBM)] * 8,
        out_specs=[pl.BlockSpec(memory_space=pltpu.VMEM)] * 8,
        scratch_shapes=[[pltpu.VMEM((9,) + FULL, BF16), shaped({COL: KEY_COLS}), hop1, hop2, hop3, hop4, small, sems]],
        compiler_params=pltpu.CompilerParams(collective_id=0, has_side_effects=True, vmem_limit_bytes=40 * 1024 * 1024),
        name="exchange",
    )(c_raw, k_turned, rope_cos, rope_sin, gain, seq_lens, q_lat, q_rope)


def attend_kernel(c_in, kr_in, score_in, len_ref, got_ref, q_cols, qk_cols, gain_ref, c_hbm, kr_hbm, o_hbm, c_buf, kr_buf, scores, o_buf, sem):
    at = stepper(place_of(lax.axis_index("x")))
    writes = []

    def write(a, b):
        writes.append(pltpu.make_async_copy(a, b, sem))
        writes[-1].start()

    def write_rows(j, sel):
        where = (j,) + index(sel)
        write(c_buf.at[where], c_hbm.at[where])

    def write_keys(z):
        where = (slice(None), slice(None), pl.ds(pl.multiple_of(z * KEY_COLS, KEY_COLS), KEY_COLS))
        write(kr_buf.at[where], kr_hbm.at[where])

    near, far = OFFSETS[:3], OFFSETS[3]
    for p, (_, b, c) in enumerate(ORDERS):
        for off in near:
            write_rows(p, {b: one(at(b, off))})
        for off in near:
            write_rows(p, {b: one(at(b, far)), c: one(at(c, off))})
    for off in near:
        write_rows(3, {2: one(at(2, off))})
        write_keys(at(ORDERS[2][1], off))

    got = [got_ref.at[p] for p in PARTS]
    units, last_request, key_columns = row_work(at, lambda j: len_ref[j, 0:1, 0:1], got, lambda: gain_ref[0:1, :], q_cols, qk_cols, c_buf, kr_buf, scores)
    all_parts(units, far, OFFSETS[3:])
    last_request([(y, far) for y in OFFSETS])
    for p, (_, b, c) in enumerate(ORDERS):
        write_rows(p, {b: one(at(b, far)), c: one(at(c, far))})
    write_rows(3, {2: one(at(2, far))})
    key_columns(at(ORDERS[2][1], far))
    write_keys(at(ORDERS[2][1], far))

    row = lax.broadcasted_iota(jnp.int32, (POSITIONS, LANES), 0)
    masked = jnp.where(row < len_ref[4, 0:1, :], scores[...].reshape(POSITIONS, LANES) * ATTN_SCALE, -1e30)
    weights = jnp.exp(masked - jnp.max(masked, axis=0, keepdims=True)).T
    weight_sum = jnp.sum(weights[: 4 * HEADS], axis=1, keepdims=True)
    rounded = weights[: 4 * HEADS].astype(BF16)
    for j in REQUESTS:
        mine = slice(HEADS * j, HEADS * (j + 1))
        weighted = jnp.dot(rounded[mine], c_buf[j].reshape(POSITIONS, LATENT), preferred_element_type=F32)
        o_buf[j] = (weighted / weight_sum[mine]).astype(BF16)
        write(o_buf.at[j], o_hbm.at[j])
    for copy in writes:
        copy.wait()


def attend(*handed):
    c_cache, kr_turned, scores = handed[:3]
    in_hbm, in_vmem = pl.BlockSpec(memory_space=pltpu.HBM), pl.BlockSpec(memory_space=pltpu.VMEM)
    return pl.pallas_call(
        attend_kernel,
        out_shape=[
            jax.ShapeDtypeStruct(c_cache.shape, BF16),
            jax.ShapeDtypeStruct(kr_turned.shape, BF16),
            jax.ShapeDtypeStruct((4, HEADS, LATENT), BF16),
            pltpu.VMEM(c_cache.shape, BF16),
            pltpu.VMEM(kr_turned.shape, BF16),
            pltpu.VMEM(scores.shape, F32),
        ],
        in_specs=[in_vmem] * len(handed),
        out_specs=[in_hbm] * 3 + [in_vmem] * 3,
        input_output_aliases={0: 3, 1: 4, 2: 5},
        scratch_shapes=[pltpu.VMEM((4, HEADS, LATENT), BF16), pltpu.SemaphoreType.DMA],
        compiler_params=pltpu.CompilerParams(vmem_limit_bytes=16 * 1024 * 1024),
        name="attend",
    )(*handed)[:3]


def solution(mesh):
    seq_spec = P("dp", "x", None)
    req_spec = P(("dp", "x"), None, None)

    def local_step(c_raw, k_raw, norm_gain, rope_cos, rope_sin, seq_lens, q_lat, q_rope):
        args = (c_raw.reshape(FULL[:4] + (4, 8, LATENT)), k_raw.transpose(1, 2, 0), rope_cos, rope_sin, norm_gain, seq_lens, q_lat, q_rope)
        handed = exchange(*[pltpu.with_memory_space_constraint(arg, pltpu.HBM) for arg in args])
        c_cache, kr_turned, o_lat = attend(*handed)
        c_cache = c_cache.reshape(4, POSITIONS, LATENT)
        return c_cache, kr_turned.transpose(0, 2, 1), o_lat

    return jax.shard_map(local_step, mesh=mesh, in_specs=(seq_spec, seq_spec, P(None), P("x", None), P("x", None), P("dp"), req_spec, req_spec), out_specs=(req_spec, req_spec, req_spec), check_vma=False)
```

```python
import jax
import jax.numpy as jnp
from jax import lax
from jax.experimental import pallas as pl
from jax.experimental.pallas import tpu as pltpu
from jax.sharding import PartitionSpec as P

NORM_EPS = 1e-6
ATTN_SCALE = (512 + 64) ** -0.5
ORDERS = ((0, 1, 2), (1, 2, 0), (2, 0, 1))
FULL = (4, 4, 4, 2, 8, 768)
STRIDES = (256, 64, 16)
POSITIONS, LATENT, ROPE, HEADS, LANES = 1024, 512, 64, 16, 128
ROWS = 64
KEY_COLS = 256
C_COLS, K_COLS, ALL_COLS = (0, LATENT), (LATENT, KEY_COLS), (0, LATENT + KEY_COLS)
CORE, COL = 3, 5
PARTS = range(3)
PAIR = range(2)
REQUESTS = range(4)
REQ = 512
GROUPS = 23
LOADS = 9
SIGNS = (1, -1)
OFFSETS = (0, -1, 1, 2)
NT = (((1,), (1,)), ((), ()))
F32, BF16 = jnp.float32, jnp.bfloat16


def all_parts(step, *args):
    for p in PARTS:
        step(p, *args)


def index(sel, dims=len(FULL)):
    return tuple(pl.ds(*sel[d]) if d in sel else slice(None) for d in range(dims))


def one(i):
    return (i, 1)


def place_of(me):
    return (me // 32, (me // 8) % 4, (me // 2) % 4)


def stepper(place):
    return lambda dim, delta: (place[dim] + delta + 4) % 4


def row_work(at, length, got, gain_row, q_cols, qk_cols, c_out, kr_out, score_out):
    def row_positions(a, b, c, ib, ic):
        r = lax.broadcasted_iota(jnp.int32, (ROWS, 1), 0)
        return (r // 16) * STRIDES[a] + r % 16 + ib * STRIDES[b] + ic * STRIDES[c]

    def unit_shape(a, width):
        return tuple(4 if d == a else 1 for d in range(3)) + (2, 8, width)

    def add_scores(a, wheres, rows, columns):
        part = jnp.dot(jnp.concatenate(rows, axis=0), columns, preferred_element_type=F32)
        for i, where in enumerate(wheres):
            score_out[where] += part[ROWS * i : ROWS * (i + 1)].reshape(unit_shape(a, LANES))

    def finish(j, a, wheres, raws, positions):
        gain = gain_row()
        rows = []
        for where, raw, pos in zip(wheres, raws, positions):
            square = jnp.sum(raw * raw, axis=-1, keepdims=True) * (1.0 / LATENT)
            inv_rms = jnp.where(pos < length(j), lax.rsqrt(square + NORM_EPS), 0.0)
            c_norm = raw * inv_rms * gain
            c_out[(j,) + where] = c_norm.reshape(unit_shape(a, LATENT)).astype(BF16)
            rows.append(c_norm.astype(BF16))
        add_scores(a, wheres, rows, q_cols[j])

    def units(p, off, steps):
        a, b, c = ORDERS[p]
        ib, ics = at(b, off), [at(c, step) for step in steps]
        wheres = [index({b: one(ib), c: one(ic)})[:COL] for ic in ics]
        full = [where + (slice(None),) for where in wheres]
        raws = [got[p][where + (pl.ds(*C_COLS),)].astype(F32).reshape(ROWS, LATENT) for where in wheres]
        finish(p, a, full, raws, [row_positions(a, b, c, ib, ic) for ic in ics])
        if p == 2:
            tiles = [got[2][where + (pl.ds(*K_COLS),)].astype(F32).reshape(ROWS, KEY_COLS).astype(BF16) for where in wheres]
            add_scores(a, full, tiles, qk_cols[...])

    def key_columns(z):
        row = lax.broadcasted_iota(jnp.int32, (KEY_COLS, KEY_COLS), 0)
        col = lax.broadcasted_iota(jnp.int32, (KEY_COLS, KEY_COLS), 1)
        eye = jnp.where(row == col, 1.0, 0.0).astype(BF16)
        tile = got[2][pl.ds(z, 1), :, :, :, :, pl.ds(*K_COLS)].astype(F32).reshape(KEY_COLS, KEY_COLS).astype(BF16)
        turned = lax.dot_general(eye, tile, NT, preferred_element_type=F32)
        for j in REQUESTS:
            valid = col[:ROPE] + z * KEY_COLS < length(j)
            kr_out[j, :, pl.ds(pl.multiple_of(z * KEY_COLS, KEY_COLS), KEY_COLS)] = jnp.where(valid, turned[ROPE * j : ROPE * (j + 1)], 0.0).astype(BF16)

    def last_request(steps):
        places = [(at(1, y), at(2, x)) for y, x in steps]
        wheres = [index({1: one(y), 2: one(x)})[:COL] for y, x in places]
        raws = [jnp.concatenate([got[p][where + (pl.ds(*K_COLS),)].astype(F32).reshape(ROWS, KEY_COLS) for p in PAIR], axis=1) for where in wheres]
        finish(3, 0, [where + (slice(None),) for where in wheres], raws, [row_positions(0, 1, 2, y, x) for y, x in places])

    return units, last_request, key_columns


def exchange_kernel(c_ref, k_ref, cos_ref, sin_ref, gain_ref, len_ref, qlat_ref, qrope_ref, c_out, kr_out, score_out, len_out, got, q_cols, qk_cols, gain_out, scratch):
    parts, k_laid, hop1, hop2, hop3, small, sems = scratch
    mid1, mid2 = [[parts.at[3 * stage + p] for p in PARTS] for stage in PAIR]
    got = [got.at[p] for p in PARTS]
    k_buf, cos_buf, sin_buf, gain_buf, len_buf, qlat_buf, qrope_buf = small
    load_sem, send_sem, recv_sem = sems

    me = lax.axis_index("x")
    core = me % 2
    other = me + 1 - 2 * core
    other_core = 1 - core
    cores = (core, other_core)
    place = place_of(me)
    at = stepper(place)

    def device(dim, delta, to_core=None):
        pos = list(place)
        pos[dim] = (pos[dim] + delta + 4) % 4
        last = core if to_core is None else to_core
        return ((pos[0] * 4 + pos[1]) * 4 + pos[2]) * 2 + last

    def halves(s):
        return (2 * s, 2)

    def view(ref, sel):
        return ref.at[index(sel)]

    barrier = pltpu.get_barrier_semaphore()
    for dim in PARTS:
        for delta in SIGNS:
            for k in PAIR:
                pl.semaphore_signal(barrier, inc=1, device_id={"x": device(dim, delta, k)}, device_id_type=pl.DeviceIdType.MESH)
    pl.semaphore_signal(barrier, inc=1, device_id={"x": other}, device_id_type=pl.DeviceIdType.MESH)

    def taken(sem, n, shape):
        block = parts.at[(pl.ds(0, n),) + index(shape)]
        pltpu.make_async_copy(block, block, sem).wait()

    def taken_from(p, sel, extra):
        where = index(sel, COL - 1)
        if extra:
            return c_ref.at[where + (3, slice(None), pl.ds(KEY_COLS * p, KEY_COLS))]
        return c_ref.at[where + (p, slice(None), pl.ds(*C_COLS))]

    def load(slot, a, b):
        copy = pltpu.make_async_copy(a, b, load_sem.at[slot])
        copy.start()
        return copy

    key_loads = [load(i, a, b) for i, (a, b) in enumerate(((k_ref, k_buf), (cos_ref, cos_buf), (sin_ref, sin_buf)))]
    other_loads = [load(3 + i, a, b) for i, (a, b) in enumerate(((gain_ref, gain_buf), (len_ref, len_buf), (qlat_ref, qlat_buf), (qrope_ref, qrope_buf)))]
    for p in PARTS:
        own = {ORDERS[p][0]: one(place[ORDERS[p][0]])}
        load(LOADS - 1 if p == 2 else LOADS - 2, taken_from(p, own, False), view(mid1[p], {**own, COL: C_COLS}))
        if p < 2:
            load(LOADS - 2, taken_from(p, own, True), view(mid1[p], {**own, COL: K_COLS}))

    slots = {}

    def send(group, a, b, to, sent=0):
        slot = slots.setdefault(group, len(slots))
        pltpu.make_async_remote_copy(src_ref=a, dst_ref=b, send_sem=send_sem.at[sent], recv_sem=recv_sem.at[slot], device_id={"x": to}, device_id_type=pl.DeviceIdType.MESH).start()

    def arrived(group, n, shape):
        taken(recv_sem.at[slots[group]], n, shape)

    def held(p, sel, cols):
        if cols == C_COLS:
            return taken_from(p, sel, False)
        return taken_from(p, sel, True) if p < 2 else view(k_laid, sel)

    def first_group(p, cols):
        return ("1far", cols if p == 2 else None)

    def far1(p, cols):
        a, b, _ = ORDERS[p]
        wide = {COL: cols}
        for s, sign in enumerate(SIGNS):
            send(first_group(p, cols), held(p, {a: one(at(a, 2)), b: halves(s)}, cols), view(hop1[2 * p + s], wide), device(a, sign))

    def near1(p, cols):
        a, b, _ = ORDERS[p]
        wide = {COL: cols}
        for s, sign in enumerate(SIGNS):
            send("1near", held(p, {a: one(at(a, sign))}, cols), view(mid1[p], {a: one(place[a]), **wide}), device(a, sign))

    def forward1(p, cols=ALL_COLS):
        a, b, _ = ORDERS[p]
        wide = {COL: cols}
        for s, sign in enumerate(SIGNS):
            send("1fwd", view(hop1[2 * p + s], wide), view(mid1[p], {a: one(at(a, -sign)), b: halves(s), **wide}), device(a, sign))

    def phase2(p, off):
        a, b, c = ORDERS[p]
        sa = {a: one(at(a, off))}
        hop_sa = {a: one(off % 4)}
        for s, sign in enumerate(SIGNS):
            send(("2far", off), view(mid1[p], {**sa, b: one(at(b, 2)), c: halves(s)}), view(hop2[2 * p + s], hop_sa), device(b, sign))
        for s, sign in enumerate(SIGNS):
            send("2near", view(mid1[p], {**sa, b: one(at(b, sign))}), view(mid2[p], {**sa, b: one(place[b])}), device(b, sign))

    def forward2(p, off):
        a, b, c = ORDERS[p]
        sa = {a: one(at(a, off))}
        hop_sa = {a: one(off % 4)}
        for s, sign in enumerate(SIGNS):
            send("2fwd", view(hop2[2 * p + s], hop_sa), view(mid2[p], {**sa, b: one(at(b, -sign)), c: halves(s)}), device(b, sign))

    def phase3(p, off):
        a, b, c = ORDERS[p]
        sb = {b: one(at(b, off))}
        hop_sb = {b: one(off % 4)}
        got_b = mid1[p] if off == 0 else mid2[p]
        mine = {**sb, c: one(place[c]), CORE: one(core)}
        for s, sign in enumerate(SIGNS):
            send(("3far", off), view(got_b, {**sb, c: one(at(c, 2)), CORE: one(cores[s])}), view(hop3[2 * p + s], hop_sb), device(c, sign, cores[1 - s]))
        for s, sign in enumerate(SIGNS):
            for k in PAIR:
                send(("3near", off), view(got_b, {**sb, c: one(at(c, sign)), CORE: one(cores[k])}), view(got[p], mine), device(c, sign, cores[k]))
        send(("3near", off), view(got_b, {**sb, c: one(place[c]), CORE: one(cores[1])}), view(got[p], mine), other, 1)
        got[p][index(mine)] = got_b[index(mine)]

    def forward3(p, off):
        a, b, c = ORDERS[p]
        sb = {b: one(at(b, off))}
        hop_sb = {b: one(off % 4)}
        for s, sign in enumerate(SIGNS):
            send(("3fwd", off), view(hop3[2 * p + s], hop_sb), view(got[p], {**sb, c: one(at(c, -sign)), CORE: one(cores[1 - s])}), device(c, sign, other_core))

    def length(j):
        return len_buf[4 * me + j]

    def keys():
        row = lax.broadcasted_iota(jnp.int32, (32, 32), 0)
        diag = row == lax.broadcasted_iota(jnp.int32, (32, 32), 1)
        roped = []
        for pos in range(8):
            cos = jnp.sum(jnp.where(diag, cos_buf[pos : pos + 1, :], 0.0), axis=1, keepdims=True)
            sin = jnp.sum(jnp.where(diag, sin_buf[pos : pos + 1, :], 0.0), axis=1, keepdims=True)
            lo = k_buf[pos, 0:32, :].astype(F32)
            hi = k_buf[pos, 32:64, :].astype(F32)
            roped.append(jnp.concatenate([lo * cos - hi * sin, hi * cos + lo * sin], axis=0).astype(BF16))
        out_row = lax.broadcasted_iota(jnp.int32, (256, 128), 0)
        lane = lax.broadcasted_iota(jnp.int32, (256, 128), 1)
        picks = [jnp.where((out_row % 8 == pos) & (out_row // 8 == lane // 4), 1.0, 0.0).astype(BF16) for pos in range(8)]
        pick = jnp.concatenate(picks, axis=1)
        request = lax.broadcasted_iota(jnp.int32, (64, 1024), 1) % 4
        for z in REQUESTS:
            cat = jnp.concatenate([r[:, 128 * z : 128 * (z + 1)] for r in roped], axis=1)
            masked = jnp.concatenate([jnp.where(request == j, cat, jnp.zeros_like(cat)) for j in REQUESTS], axis=0)
            laid = lax.dot_general(pick, masked, NT, preferred_element_type=F32)
            laid = laid.reshape(1, 4, 4, 2, 8, 256).astype(BF16)
            k_laid[z : z + 1] = laid
        own = {2: one(place[2])}
        mid1[2][index({**own, COL: K_COLS})] = k_laid[index(own)]

    def queries():
        for j in REQUESTS:
            rows = [qlat_buf[j].astype(F32) if i == j else jnp.zeros((HEADS, LATENT), F32) for i in REQUESTS]
            q_cols[j] = jnp.concatenate(rows + [jnp.zeros((LANES - 4 * HEADS, LATENT), F32)], axis=0).T.astype(BF16)
        zero = jnp.zeros((HEADS, ROPE), F32)
        rows = [jnp.concatenate([qrope_buf[j].astype(F32) if i == j else zero for i in REQUESTS], axis=1) for j in REQUESTS]
        qk_cols[...] = jnp.concatenate(rows + [jnp.zeros((LANES - 4 * HEADS, KEY_COLS), F32)], axis=0).T.astype(BF16)
        score_out[...] = jnp.zeros_like(score_out)
        lane = lax.broadcasted_iota(jnp.int32, (8, LANES), 1)
        lens = jnp.zeros((8, LANES), jnp.int32)
        for j in REQUESTS:
            lens = jnp.where(lane // HEADS == j, length(j), lens)
            len_out[j] = jnp.zeros((8, LANES), jnp.int32) + length(j)
        len_out[4] = lens
        gain_out[...] = jnp.broadcast_to(gain_buf[...].astype(F32).reshape(1, LATENT), gain_out.shape)

    units, last_request, key_columns = row_work(at, length, got, lambda: gain_out[0:1, :], q_cols, qk_cols, c_out, kr_out, score_out)

    def near_units(off):
        arrived(("3near", off), 5, {0: (0, 3), 1: one(0), CORE: one(0)})
        all_parts(units, off, OFFSETS[:3])

    def far_units(off):
        arrived(("3fwd", off), 3, {0: one(0), 1: one(0)})
        all_parts(units, off, OFFSETS[3:])
        key_columns(at(ORDERS[2][1], off))

    EIGHTH, SIXTEENTH = {0: one(0), 1: (0, 2)}, {0: one(0), 1: one(0)}
    pl.semaphore_wait(barrier, 13)
    for first in (far1, near1):
        all_parts(first, C_COLS)
        first(0, K_COLS)
        first(1, K_COLS)
    for copy in key_loads:
        copy.wait()
    keys()
    for copy in other_loads:
        copy.wait()
    queries()
    far1(2, K_COLS)
    near1(2, K_COLS)
    taken(load_sem.at[LOADS - 2], 2, {0: one(0)})
    taken(load_sem.at[LOADS - 1], 1, {0: one(0), COL: C_COLS})
    arrived(first_group(0, None), 2, {0: one(0)})
    forward1(0)
    forward1(1)
    arrived(first_group(2, C_COLS), 1, {0: one(0), COL: C_COLS})
    forward1(2, C_COLS)
    all_parts(phase2, 0)
    arrived(first_group(2, K_COLS), 1, {0: one(0), COL: K_COLS})
    forward1(2, K_COLS)
    arrived("1near", 3, {0: (0, 2)})
    all_parts(phase2, -1)
    all_parts(phase2, 1)
    arrived(("2far", 0), 3, SIXTEENTH)
    all_parts(forward2, 0)
    arrived("1fwd", 3, {0: one(0)})
    all_parts(phase2, 2)
    for off in (-1, 1):
        arrived(("2far", off), 3, SIXTEENTH)
        all_parts(forward2, off)
    arrived(("2far", 2), 3, SIXTEENTH)
    all_parts(forward2, 2)
    all_parts(phase3, 0)
    arrived("2near", 3, {0: (0, 2)})
    all_parts(phase3, -1)
    arrived(("3far", 0), 3, SIXTEENTH)
    all_parts(forward3, 0)
    all_parts(phase3, 1)
    near_units(0)
    arrived("2fwd", 3, {0: one(0)})
    arrived(("3far", -1), 3, SIXTEENTH)
    all_parts(forward3, -1)
    all_parts(phase3, 2)
    near_units(-1)
    far_units(0)
    arrived(("3far", 1), 3, SIXTEENTH)
    all_parts(forward3, 1)
    near_units(1)
    far_units(-1)
    last_request([(y, x) for y in OFFSETS[:2] for x in OFFSETS[:2]])
    arrived(("3far", 2), 3, SIXTEENTH)
    all_parts(forward3, 2)
    near_units(2)
    far_units(1)
    last_request([(y, x) for y in OFFSETS for x in OFFSETS[:3] if y > 0 or x > 0])
    arrived(("3fwd", 2), 3, SIXTEENTH)
    taken(send_sem.at[0], 9, {})
    taken(send_sem.at[1], 3, EIGHTH)


def exchange(c_raw, k_turned, rope_cos, rope_sin, gain, seq_lens, q_lat, q_rope):
    def shaped(sizes):
        return pltpu.VMEM(tuple(sizes.get(d, FULL[d]) for d in range(6)), BF16)

    hop1 = [shaped({o[0]: 1, o[1]: 2}) for o in ORDERS for _ in PAIR]
    hop2 = [shaped({o[1]: 1, o[2]: 2}) for o in ORDERS for _ in PAIR]
    hop3 = [shaped({o[2]: 1, 3: 1}) for o in ORDERS for _ in PAIR]
    small = [
        pltpu.VMEM((8, 64, 512), BF16),
        pltpu.VMEM((8, 32), F32),
        pltpu.VMEM((8, 32), F32),
        pltpu.VMEM((LATENT,), BF16),
        pltpu.SMEM((REQ,), jnp.int32),
        pltpu.VMEM((4, 16, 512), BF16),
        pltpu.VMEM((4, 16, 64), BF16),
    ]
    sems = [pltpu.SemaphoreType.DMA((n,)) for n in (LOADS, 2, GROUPS)]
    return pl.pallas_call(
        exchange_kernel,
        out_shape=[
            pltpu.VMEM((4, 4, 4, 4, 2, 8, 512), BF16),
            pltpu.VMEM((4, 64, 1024), BF16),
            pltpu.VMEM(FULL[:COL] + (LANES,), F32),
            pltpu.VMEM((5, 8, LANES), jnp.int32),
            pltpu.VMEM((3,) + FULL, BF16),
            pltpu.VMEM((4, LATENT, LANES), BF16),
            pltpu.VMEM((KEY_COLS, LANES), BF16),
            pltpu.VMEM((8, LATENT), F32),
        ],
        in_specs=[pl.BlockSpec(memory_space=pltpu.HBM)] * 8,
        out_specs=[pl.BlockSpec(memory_space=pltpu.VMEM)] * 8,
        scratch_shapes=[[pltpu.VMEM((9,) + FULL, BF16), shaped({COL: KEY_COLS}), hop1, hop2, hop3, small, sems]],
        compiler_params=pltpu.CompilerParams(collective_id=0, has_side_effects=True, vmem_limit_bytes=40 * 1024 * 1024),
        name="exchange",
    )(c_raw, k_turned, rope_cos, rope_sin, gain, seq_lens, q_lat, q_rope)


def attend_kernel(c_in, kr_in, score_in, len_ref, got_ref, q_cols, qk_cols, gain_ref, c_hbm, kr_hbm, o_hbm, c_buf, kr_buf, scores, o_buf, sem):
    at = stepper(place_of(lax.axis_index("x")))
    writes = []

    def write(a, b):
        writes.append(pltpu.make_async_copy(a, b, sem))
        writes[-1].start()

    def write_rows(j, sel):
        where = (j,) + index(sel)
        write(c_buf.at[where], c_hbm.at[where])

    def write_keys(z):
        where = (slice(None), slice(None), pl.ds(pl.multiple_of(z * KEY_COLS, KEY_COLS), KEY_COLS))
        write(kr_buf.at[where], kr_hbm.at[where])

    near, far = OFFSETS[:3], OFFSETS[3]
    for p, (_, b, c) in enumerate(ORDERS):
        for off in near:
            write_rows(p, {b: one(at(b, off))})
        for off in near:
            write_rows(p, {b: one(at(b, far)), c: one(at(c, off))})
    for off in near:
        write_rows(3, {2: one(at(2, off))})
        write_keys(at(ORDERS[2][1], off))

    got = [got_ref.at[p] for p in PARTS]
    units, last_request, key_columns = row_work(at, lambda j: len_ref[j, 0:1, 0:1], got, lambda: gain_ref[0:1, :], q_cols, qk_cols, c_buf, kr_buf, scores)
    all_parts(units, far, OFFSETS[3:])
    last_request([(y, far) for y in OFFSETS])
    for p, (_, b, c) in enumerate(ORDERS):
        write_rows(p, {b: one(at(b, far)), c: one(at(c, far))})
    write_rows(3, {2: one(at(2, far))})
    key_columns(at(ORDERS[2][1], far))
    write_keys(at(ORDERS[2][1], far))

    row = lax.broadcasted_iota(jnp.int32, (POSITIONS, LANES), 0)
    masked = jnp.where(row < len_ref[4, 0:1, :], scores[...].reshape(POSITIONS, LANES) * ATTN_SCALE, -1e30)
    weights = jnp.exp(masked - jnp.max(masked, axis=0, keepdims=True)).T
    weight_sum = jnp.sum(weights[: 4 * HEADS], axis=1, keepdims=True)
    rounded = weights[: 4 * HEADS].astype(BF16)
    for j in REQUESTS:
        mine = slice(HEADS * j, HEADS * (j + 1))
        weighted = jnp.dot(rounded[mine], c_buf[j].reshape(POSITIONS, LATENT), preferred_element_type=F32)
        o_buf[j] = (weighted / weight_sum[mine]).astype(BF16)
        write(o_buf.at[j], o_hbm.at[j])
    for copy in writes:
        copy.wait()


def attend(*handed):
    c_cache, kr_turned, scores = handed[:3]
    in_hbm, in_vmem = pl.BlockSpec(memory_space=pltpu.HBM), pl.BlockSpec(memory_space=pltpu.VMEM)
    return pl.pallas_call(
        attend_kernel,
        out_shape=[
            jax.ShapeDtypeStruct(c_cache.shape, BF16),
            jax.ShapeDtypeStruct(kr_turned.shape, BF16),
            jax.ShapeDtypeStruct((4, HEADS, LATENT), BF16),
            pltpu.VMEM(c_cache.shape, BF16),
            pltpu.VMEM(kr_turned.shape, BF16),
            pltpu.VMEM(scores.shape, F32),
        ],
        in_specs=[in_vmem] * len(handed),
        out_specs=[in_hbm] * 3 + [in_vmem] * 3,
        input_output_aliases={0: 3, 1: 4, 2: 5},
        scratch_shapes=[pltpu.VMEM((4, HEADS, LATENT), BF16), pltpu.SemaphoreType.DMA],
        compiler_params=pltpu.CompilerParams(vmem_limit_bytes=16 * 1024 * 1024),
        name="attend",
    )(*handed)[:3]


def solution(mesh):
    seq_spec = P("dp", "x", None)
    req_spec = P(("dp", "x"), None, None)

    def local_step(c_raw, k_raw, norm_gain, rope_cos, rope_sin, seq_lens, q_lat, q_rope):
        args = (c_raw.reshape(FULL[:4] + (4, 8, LATENT)), k_raw.transpose(1, 2, 0), rope_cos, rope_sin, norm_gain, seq_lens, q_lat, q_rope)
        handed = exchange(*[pltpu.with_memory_space_constraint(arg, pltpu.HBM) for arg in args])
        c_cache, kr_turned, o_lat = attend(*handed)
        c_cache = c_cache.reshape(4, POSITIONS, LATENT)
        return c_cache, kr_turned.transpose(0, 2, 1), o_lat

    return jax.shard_map(local_step, mesh=mesh, in_specs=(seq_spec, seq_spec, P(None), P("x", None), P("x", None), P("dp"), req_spec, req_spec), out_specs=(req_spec, req_spec, req_spec), check_vma=False)
```

```python
import jax
import jax.numpy as jnp
from jax import lax
from jax.experimental import pallas as pl
from jax.experimental.pallas import tpu as pltpu
from jax.sharding import PartitionSpec as P

NORM_EPS = 1e-6
ATTN_SCALE = (512 + 64) ** -0.5
ORDERS = ((0, 1, 2), (1, 2, 0), (2, 0, 1))
FULL = (4, 4, 4, 2, 8, 768)
STRIDES = (256, 64, 16)
POSITIONS, LATENT, ROPE, HEADS, LANES = 1024, 512, 64, 16, 128
ROWS = 64
KEY_COLS = 256
C_COLS, K_COLS, ALL_COLS = (0, LATENT), (LATENT, KEY_COLS), (0, LATENT + KEY_COLS)
CORE, COL = 3, 5
PARTS = range(3)
PAIR = range(2)
REQUESTS = range(4)
REQ = 512
GROUPS = 19
LOADS = 7
SIGNS = (1, -1)
EARLY, LATE = "1fwd and 2far", "2fwd and 3far"
OFFSETS = (0, -1, 1, 2)
NT = (((1,), (1,)), ((), ()))
F32, BF16 = jnp.float32, jnp.bfloat16


def all_parts(step, *args):
    for p in PARTS:
        step(p, *args)


def index(sel, dims=len(FULL)):
    return tuple(pl.ds(*sel[d]) if d in sel else slice(None) for d in range(dims))


def one(i):
    return (i, 1)


def place_of(me):
    return (me // 32, (me // 8) % 4, (me // 2) % 4)


def stepper(place):
    return lambda dim, delta: (place[dim] + delta + 4) % 4


def row_work(at, length, got, gain_row, q_cols, qk_cols, c_out, kr_out, score_out):
    def row_positions(a, b, c, ib, ic):
        r = lax.broadcasted_iota(jnp.int32, (ROWS, 1), 0)
        return (r // 16) * STRIDES[a] + r % 16 + ib * STRIDES[b] + ic * STRIDES[c]

    def unit_shape(a, width):
        return tuple(4 if d == a else 1 for d in range(3)) + (2, 8, width)

    def add_scores(a, wheres, rows, columns):
        part = jnp.dot(jnp.concatenate(rows, axis=0), columns, preferred_element_type=F32)
        for i, where in enumerate(wheres):
            score_out[where] += part[ROWS * i : ROWS * (i + 1)].reshape(unit_shape(a, LANES))

    def finish(j, a, wheres, raws, positions):
        gain = gain_row()
        rows = []
        for where, raw, pos in zip(wheres, raws, positions):
            square = jnp.sum(raw * raw, axis=-1, keepdims=True) * (1.0 / LATENT)
            inv_rms = jnp.where(pos < length(j), lax.rsqrt(square + NORM_EPS), 0.0)
            c_norm = raw * inv_rms * gain
            c_out[(j,) + where] = c_norm.reshape(unit_shape(a, LATENT)).astype(BF16)
            rows.append(c_norm.astype(BF16))
        add_scores(a, wheres, rows, q_cols[j])

    def units(p, off, steps):
        a, b, c = ORDERS[p]
        ib, ics = at(b, off), [at(c, step) for step in steps]
        wheres = [index({b: one(ib), c: one(ic)})[:COL] for ic in ics]
        full = [where + (slice(None),) for where in wheres]
        raws = [got[p][where + (pl.ds(*C_COLS),)].astype(F32).reshape(ROWS, LATENT) for where in wheres]
        finish(p, a, full, raws, [row_positions(a, b, c, ib, ic) for ic in ics])
        if p == 2:
            tiles = [got[2][where + (pl.ds(*K_COLS),)].astype(F32).reshape(ROWS, KEY_COLS).astype(BF16) for where in wheres]
            add_scores(a, full, tiles, qk_cols[...])

    def key_columns(z):
        row = lax.broadcasted_iota(jnp.int32, (KEY_COLS, KEY_COLS), 0)
        col = lax.broadcasted_iota(jnp.int32, (KEY_COLS, KEY_COLS), 1)
        eye = jnp.where(row == col, 1.0, 0.0).astype(BF16)
        tile = got[2][pl.ds(z, 1), :, :, :, :, pl.ds(*K_COLS)].astype(F32).reshape(KEY_COLS, KEY_COLS).astype(BF16)
        turned = lax.dot_general(eye, tile, NT, preferred_element_type=F32)
        for j in REQUESTS:
            valid = col[:ROPE] + z * KEY_COLS < length(j)
            kr_out[j, :, pl.ds(pl.multiple_of(z * KEY_COLS, KEY_COLS), KEY_COLS)] = jnp.where(valid, turned[ROPE * j : ROPE * (j + 1)], 0.0).astype(BF16)

    def last_request(steps):
        places = [(at(1, y), at(2, x)) for y, x in steps]
        wheres = [index({1: one(y), 2: one(x)})[:COL] for y, x in places]
        raws = [jnp.concatenate([got[p][where + (pl.ds(*K_COLS),)].astype(F32).reshape(ROWS, KEY_COLS) for p in PAIR], axis=1) for where in wheres]
        finish(3, 0, [where + (slice(None),) for where in wheres], raws, [row_positions(0, 1, 2, y, x) for y, x in places])

    return units, last_request, key_columns


def exchange_kernel(c_ref, k_ref, cos_ref, sin_ref, gain_ref, len_ref, qlat_ref, qrope_ref, c_out, kr_out, score_out, len_out, got, q_cols, qk_cols, gain_out, scratch):
    parts, k_laid, hop1, hop2, hop3, small, sems = scratch
    mid1, mid2 = [[parts.at[3 * stage + p] for p in PARTS] for stage in PAIR]
    got = [got.at[p] for p in PARTS]
    k_buf, angles, gain_buf, len_buf, qlat_buf, qrope_buf = small
    load_sem, send_sem, recv_sem = sems

    me = lax.axis_index("x")
    core = me % 2
    other = me + 1 - 2 * core
    other_core = 1 - core
    cores = (core, other_core)
    place = place_of(me)
    at = stepper(place)

    def device(dim, delta, to_core=None):
        pos = list(place)
        pos[dim] = (pos[dim] + delta + 4) % 4
        last = core if to_core is None else to_core
        return ((pos[0] * 4 + pos[1]) * 4 + pos[2]) * 2 + last

    def halves(s):
        return (2 * s, 2)

    def view(ref, sel):
        return ref.at[index(sel)]

    barrier = pltpu.get_barrier_semaphore()
    for dim in PARTS:
        for delta in SIGNS:
            for k in PAIR:
                pl.semaphore_signal(barrier, inc=1, device_id={"x": device(dim, delta, k)}, device_id_type=pl.DeviceIdType.MESH)
    pl.semaphore_signal(barrier, inc=1, device_id={"x": other}, device_id_type=pl.DeviceIdType.MESH)

    def taken(sem, n, shape):
        block = parts.at[(pl.ds(0, n),) + index(shape)]
        pltpu.make_async_copy(block, block, sem).wait()

    def taken_from(p, sel, extra):
        where = index(sel, COL - 1)
        if extra:
            return c_ref.at[where + (3, slice(None), pl.ds(KEY_COLS * p, KEY_COLS))]
        return c_ref.at[where + (p, slice(None), pl.ds(*C_COLS))]

    def load(slot, a, b):
        copy = pltpu.make_async_copy(a, b, load_sem.at[slot])
        copy.start()
        return copy

    load(0, cos_ref, angles.at[0])
    load(0, sin_ref, angles.at[1])
    small_loads = [load(1 + i, a, b) for i, (a, b) in enumerate(((k_ref, k_buf), (gain_ref, gain_buf), (len_ref, len_buf), (qlat_ref, qlat_buf), (qrope_ref, qrope_buf)))]
    for p in PARTS:
        own = {ORDERS[p][0]: one(place[ORDERS[p][0]])}
        load(LOADS - 1, taken_from(p, own, False), view(mid1[p], {**own, COL: C_COLS}))
        if p < 2:
            load(LOADS - 1, taken_from(p, own, True), view(mid1[p], {**own, COL: K_COLS}))

    slots = {}

    def send(group, a, b, to, sent=0):
        slot = slots.setdefault(group, len(slots))
        pltpu.make_async_remote_copy(src_ref=a, dst_ref=b, send_sem=send_sem.at[sent], recv_sem=recv_sem.at[slot], device_id={"x": to}, device_id_type=pl.DeviceIdType.MESH).start()

    def arrived(group, n, shape):
        taken(recv_sem.at[slots[group]], n, shape)

    def held(p, sel, cols):
        if cols == C_COLS:
            return taken_from(p, sel, False)
        return taken_from(p, sel, True) if p < 2 else view(k_laid, sel)

    def first_group(p, cols):
        return ("1far", p == 2 and cols == K_COLS)

    def far1(p, cols):
        a, b, _ = ORDERS[p]
        wide = {COL: cols}
        for s, sign in enumerate(SIGNS):
            send(first_group(p, cols), held(p, {a: one(at(a, 2)), b: halves(s)}, cols), view(hop1[2 * p + s], wide), device(a, sign))

    def near1(p, cols):
        a, b, _ = ORDERS[p]
        wide = {COL: cols}
        for s, sign in enumerate(SIGNS):
            send("1near", held(p, {a: one(at(a, sign))}, cols), view(mid1[p], {a: one(place[a]), **wide}), device(a, sign))

    def forward1(p, cols=ALL_COLS):
        a, b, _ = ORDERS[p]
        wide = {COL: cols}
        for s, sign in enumerate(SIGNS):
            send(EARLY, view(hop1[2 * p + s], wide), view(mid1[p], {a: one(at(a, -sign)), b: halves(s), **wide}), device(a, sign))

    def phase2(p, off):
        a, b, c = ORDERS[p]
        sa = {a: one(at(a, off))}
        hop_sa = {a: one(off % 4)}
        for s, sign in enumerate(SIGNS):
            send(EARLY if off == 0 else ("2far", abs(off)), view(mid1[p], {**sa, b: one(at(b, 2)), c: halves(s)}), view(hop2[2 * p + s], hop_sa), device(b, sign))
        for s, sign in enumerate(SIGNS):
            send("2near", view(mid1[p], {**sa, b: one(at(b, sign))}), view(mid2[p], {**sa, b: one(place[b])}), device(b, sign))

    def forward2(p, off):
        a, b, c = ORDERS[p]
        sa = {a: one(at(a, off))}
        hop_sa = {a: one(off % 4)}
        for s, sign in enumerate(SIGNS):
            send(LATE, view(hop2[2 * p + s], hop_sa), view(mid2[p], {**sa, b: one(at(b, -sign)), c: halves(s)}), device(b, sign))

    def phase3(p, off):
        a, b, c = ORDERS[p]
        sb = {b: one(at(b, off))}
        hop_sb = {b: one(off % 4)}
        got_b = mid1[p] if off == 0 else mid2[p]
        mine = {**sb, c: one(place[c]), CORE: one(core)}
        for s, sign in enumerate(SIGNS):
            send(LATE if off == -1 else ("3far", off), view(got_b, {**sb, c: one(at(c, 2)), CORE: one(cores[s])}), view(hop3[2 * p + s], hop_sb), device(c, sign, cores[1 - s]))
        for s, sign in enumerate(SIGNS):
            for k in PAIR:
                send(("3near", off), view(got_b, {**sb, c: one(at(c, sign)), CORE: one(cores[k])}), view(got[p], mine), device(c, sign, cores[k]))
        send(("3near", off), view(got_b, {**sb, c: one(place[c]), CORE: one(cores[1])}), view(got[p], mine), other, 1)
        got[p][index(mine)] = got_b[index(mine)]

    def forward3(p, off):
        a, b, c = ORDERS[p]
        sb = {b: one(at(b, off))}
        hop_sb = {b: one(off % 4)}
        for s, sign in enumerate(SIGNS):
            send(("3fwd", off), view(hop3[2 * p + s], hop_sb), view(got[p], {**sb, c: one(at(c, -sign)), CORE: one(cores[1 - s])}), device(c, sign, other_core))

    def length(j):
        return len_buf[4 * me + j]

    def keys():
        row = lax.broadcasted_iota(jnp.int32, (32, 32), 0)
        diag = row == lax.broadcasted_iota(jnp.int32, (32, 32), 1)
        roped = []
        for pos in range(8):
            cos = jnp.sum(jnp.where(diag, angles[0, pos : pos + 1, :], 0.0), axis=1, keepdims=True)
            sin = jnp.sum(jnp.where(diag, angles[1, pos : pos + 1, :], 0.0), axis=1, keepdims=True)
            lo = k_buf[pos, 0:32, :].astype(F32)
            hi = k_buf[pos, 32:64, :].astype(F32)
            roped.append(jnp.concatenate([lo * cos - hi * sin, hi * cos + lo * sin], axis=0).astype(BF16))
        out_row = lax.broadcasted_iota(jnp.int32, (256, 128), 0)
        lane = lax.broadcasted_iota(jnp.int32, (256, 128), 1)
        picks = [jnp.where((out_row % 8 == pos) & (out_row // 8 == lane // 4), 1.0, 0.0).astype(BF16) for pos in range(8)]
        pick = jnp.concatenate(picks, axis=1)
        request = lax.broadcasted_iota(jnp.int32, (64, 1024), 1) % 4
        for z in REQUESTS:
            cat = jnp.concatenate([r[:, 128 * z : 128 * (z + 1)] for r in roped], axis=1)
            masked = jnp.concatenate([jnp.where(request == j, cat, jnp.zeros_like(cat)) for j in REQUESTS], axis=0)
            laid = lax.dot_general(pick, masked, NT, preferred_element_type=F32)
            laid = laid.reshape(1, 4, 4, 2, 8, 256).astype(BF16)
            k_laid[z : z + 1] = laid
        own = {2: one(place[2])}
        mid1[2][index({**own, COL: K_COLS})] = k_laid[index(own)]

    def queries():
        for j in REQUESTS:
            rows = [qlat_buf[j].astype(F32) if i == j else jnp.zeros((HEADS, LATENT), F32) for i in REQUESTS]
            q_cols[j] = jnp.concatenate(rows + [jnp.zeros((LANES - 4 * HEADS, LATENT), F32)], axis=0).T.astype(BF16)
        zero = jnp.zeros((HEADS, ROPE), F32)
        rows = [jnp.concatenate([qrope_buf[j].astype(F32) if i == j else zero for i in REQUESTS], axis=1) for j in REQUESTS]
        qk_cols[...] = jnp.concatenate(rows + [jnp.zeros((LANES - 4 * HEADS, KEY_COLS), F32)], axis=0).T.astype(BF16)
        score_out[...] = jnp.zeros_like(score_out)
        lane = lax.broadcasted_iota(jnp.int32, (8, LANES), 1)
        lens = jnp.zeros((8, LANES), jnp.int32)
        for j in REQUESTS:
            lens = jnp.where(lane // HEADS == j, length(j), lens)
            len_out[j] = jnp.zeros((8, LANES), jnp.int32) + length(j)
        len_out[4] = lens
        gain_out[...] = jnp.broadcast_to(gain_buf[...].astype(F32).reshape(1, LATENT), gain_out.shape)

    units, last_request, key_columns = row_work(at, length, got, lambda: gain_out[0:1, :], q_cols, qk_cols, c_out, kr_out, score_out)

    def near_units(off):
        arrived(("3near", off), 5, {0: (0, 3), 1: one(0), CORE: one(0)})
        all_parts(units, off, OFFSETS[:3])

    def far_units(off):
        arrived(("3fwd", off), 3, {0: one(0), 1: one(0)})
        all_parts(units, off, OFFSETS[3:])
        key_columns(at(ORDERS[2][1], off))

    BOTH = {0: (0, 3), 2: (0, 2), CORE: one(0)}
    EIGHTH, SIXTEENTH = {0: one(0), 1: (0, 2)}, {0: one(0), 1: one(0)}
    pl.semaphore_wait(barrier, 13)
    for first in (far1, near1):
        all_parts(first, C_COLS)
        first(0, K_COLS)
        first(1, K_COLS)
    pltpu.make_async_copy(angles, angles, load_sem.at[0]).wait()
    small_loads[0].wait()
    keys()
    for copy in small_loads[1:]:
        copy.wait()
    queries()
    far1(2, K_COLS)
    near1(2, K_COLS)
    taken(load_sem.at[LOADS - 1], 4, {0: one(0), COL: C_COLS})
    arrived(first_group(2, C_COLS), 4, {0: one(0), COL: C_COLS})
    forward1(0)
    forward1(1)
    forward1(2, C_COLS)
    all_parts(phase2, 0)
    arrived(first_group(2, K_COLS), 1, {0: one(0), COL: K_COLS})
    forward1(2, K_COLS)
    arrived("1near", 3, {0: (0, 2)})
    all_parts(phase2, -1)
    all_parts(phase2, 1)
    arrived(EARLY, 5, BOTH)
    all_parts(forward2, 0)
    all_parts(phase2, 2)
    arrived(("2far", 1), 3, {0: one(0), 1: (0, 2)})
    all_parts(forward2, -1)
    all_parts(forward2, 1)
    arrived(("2far", 2), 3, SIXTEENTH)
    all_parts(forward2, 2)
    all_parts(phase3, 0)
    arrived("2near", 3, {0: (0, 2)})
    all_parts(phase3, -1)
    arrived(("3far", 0), 3, SIXTEENTH)
    all_parts(forward3, 0)
    all_parts(phase3, 1)
    near_units(0)
    arrived(LATE, 5, BOTH)
    all_parts(forward3, -1)
    all_parts(phase3, 2)
    near_units(-1)
    far_units(0)
    arrived(("3far", 1), 3, SIXTEENTH)
    all_parts(forward3, 1)
    near_units(1)
    far_units(-1)
    last_request([(y, x) for y in OFFSETS[:3] for x in OFFSETS[:2]])
    arrived(("3far", 2), 3, SIXTEENTH)
    all_parts(forward3, 2)
    near_units(2)
    far_units(1)
    last_request([(2, x) for x in OFFSETS[:2]] + [(y, 1) for y in OFFSETS])
    arrived(("3fwd", 2), 3, SIXTEENTH)
    taken(send_sem.at[0], 9, {})
    taken(send_sem.at[1], 3, EIGHTH)


def exchange(c_raw, k_turned, rope_cos, rope_sin, gain, seq_lens, q_lat, q_rope):
    def shaped(sizes):
        return pltpu.VMEM(tuple(sizes.get(d, FULL[d]) for d in range(6)), BF16)

    hop1 = [shaped({o[0]: 1, o[1]: 2}) for o in ORDERS for _ in PAIR]
    hop2 = [shaped({o[1]: 1, o[2]: 2}) for o in ORDERS for _ in PAIR]
    hop3 = [shaped({o[2]: 1, 3: 1}) for o in ORDERS for _ in PAIR]
    small = [
        pltpu.VMEM((8, 64, 512), BF16),
        pltpu.VMEM((2, 8, 32), F32),
        pltpu.VMEM((LATENT,), BF16),
        pltpu.SMEM((REQ,), jnp.int32),
        pltpu.VMEM((4, 16, 512), BF16),
        pltpu.VMEM((4, 16, 64), BF16),
    ]
    sems = [pltpu.SemaphoreType.DMA((n,)) for n in (LOADS, 2, GROUPS)]
    return pl.pallas_call(
        exchange_kernel,
        out_shape=[
            pltpu.VMEM((4, 4, 4, 4, 2, 8, 512), BF16),
            pltpu.VMEM((4, 64, 1024), BF16),
            pltpu.VMEM(FULL[:COL] + (LANES,), F32),
            pltpu.VMEM((5, 8, LANES), jnp.int32),
            pltpu.VMEM((3,) + FULL, BF16),
            pltpu.VMEM((4, LATENT, LANES), BF16),
            pltpu.VMEM((KEY_COLS, LANES), BF16),
            pltpu.VMEM((8, LATENT), F32),
        ],
        in_specs=[pl.BlockSpec(memory_space=pltpu.HBM)] * 8,
        out_specs=[pl.BlockSpec(memory_space=pltpu.VMEM)] * 8,
        scratch_shapes=[[pltpu.VMEM((9,) + FULL, BF16), shaped({COL: KEY_COLS}), hop1, hop2, hop3, small, sems]],
        compiler_params=pltpu.CompilerParams(collective_id=0, has_side_effects=True, vmem_limit_bytes=40 * 1024 * 1024),
        name="exchange",
    )(c_raw, k_turned, rope_cos, rope_sin, gain, seq_lens, q_lat, q_rope)


def attend_kernel(c_in, kr_in, score_in, len_ref, got_ref, q_cols, qk_cols, gain_ref, c_hbm, kr_hbm, o_hbm, c_buf, kr_buf, scores, o_buf, sem):
    at = stepper(place_of(lax.axis_index("x")))
    writes = []

    def write(a, b):
        writes.append(pltpu.make_async_copy(a, b, sem))
        writes[-1].start()

    def write_rows(j, sel):
        where = (j,) + index(sel)
        write(c_buf.at[where], c_hbm.at[where])

    def write_keys(z):
        where = (slice(None), slice(None), pl.ds(pl.multiple_of(z * KEY_COLS, KEY_COLS), KEY_COLS))
        write(kr_buf.at[where], kr_hbm.at[where])

    near, far = OFFSETS[:3], OFFSETS[3]
    for p, (_, b, c) in enumerate(ORDERS):
        for off in near:
            write_rows(p, {b: one(at(b, off))})
        for off in near:
            write_rows(p, {b: one(at(b, far)), c: one(at(c, off))})
    for off in near:
        write_rows(3, {2: one(at(2, off))})
        write_keys(at(ORDERS[2][1], off))

    got = [got_ref.at[p] for p in PARTS]
    units, last_request, key_columns = row_work(at, lambda j: len_ref[j, 0:1, 0:1], got, lambda: gain_ref[0:1, :], q_cols, qk_cols, c_buf, kr_buf, scores)
    all_parts(units, far, OFFSETS[3:])
    last_request([(y, far) for y in OFFSETS])
    for p, (_, b, c) in enumerate(ORDERS):
        write_rows(p, {b: one(at(b, far)), c: one(at(c, far))})
    write_rows(3, {2: one(at(2, far))})
    key_columns(at(ORDERS[2][1], far))
    write_keys(at(ORDERS[2][1], far))

    row = lax.broadcasted_iota(jnp.int32, (POSITIONS, LANES), 0)
    masked = jnp.where(row < len_ref[4, 0:1, :], scores[...].reshape(POSITIONS, LANES) * ATTN_SCALE, -1e30)
    weights = jnp.exp(masked - jnp.max(masked, axis=0, keepdims=True)).T
    weight_sum = jnp.sum(weights[: 4 * HEADS], axis=1, keepdims=True)
    rounded = weights[: 4 * HEADS].astype(BF16)
    for j in REQUESTS:
        mine = slice(HEADS * j, HEADS * (j + 1))
        weighted = jnp.dot(rounded[mine], c_buf[j].reshape(POSITIONS, LATENT), preferred_element_type=F32)
        o_buf[j] = (weighted / weight_sum[mine]).astype(BF16)
        write(o_buf.at[j], o_hbm.at[j])
    for copy in writes:
        copy.wait()


def attend(*handed):
    c_cache, kr_turned, scores = handed[:3]
    in_hbm, in_vmem = pl.BlockSpec(memory_space=pltpu.HBM), pl.BlockSpec(memory_space=pltpu.VMEM)
    return pl.pallas_call(
        attend_kernel,
        out_shape=[
            jax.ShapeDtypeStruct(c_cache.shape, BF16),
            jax.ShapeDtypeStruct(kr_turned.shape, BF16),
            jax.ShapeDtypeStruct((4, HEADS, LATENT), BF16),
            pltpu.VMEM(c_cache.shape, BF16),
            pltpu.VMEM(kr_turned.shape, BF16),
            pltpu.VMEM(scores.shape, F32),
        ],
        in_specs=[in_vmem] * len(handed),
        out_specs=[in_hbm] * 3 + [in_vmem] * 3,
        input_output_aliases={0: 3, 1: 4, 2: 5},
        scratch_shapes=[pltpu.VMEM((4, HEADS, LATENT), BF16), pltpu.SemaphoreType.DMA],
        compiler_params=pltpu.CompilerParams(vmem_limit_bytes=16 * 1024 * 1024),
        name="attend",
    )(*handed)[:3]


def solution(mesh):
    seq_spec = P("dp", "x", None)
    req_spec = P(("dp", "x"), None, None)

    def local_step(c_raw, k_raw, norm_gain, rope_cos, rope_sin, seq_lens, q_lat, q_rope):
        args = (c_raw.reshape(FULL[:4] + (4, 8, LATENT)), k_raw.transpose(1, 2, 0), rope_cos, rope_sin, norm_gain, seq_lens, q_lat, q_rope)
        handed = exchange(*[pltpu.with_memory_space_constraint(arg, pltpu.HBM) for arg in args])
        c_cache, kr_turned, o_lat = attend(*handed)
        c_cache = c_cache.reshape(4, POSITIONS, LATENT)
        return c_cache, kr_turned.transpose(0, 2, 1), o_lat

    return jax.shard_map(local_step, mesh=mesh, in_specs=(seq_spec, seq_spec, P(None), P("x", None), P("x", None), P("dp"), req_spec, req_spec), out_specs=(req_spec, req_spec, req_spec), check_vma=False)
```

```python
import jax
import jax.numpy as jnp
from jax import lax
from jax.experimental import pallas as pl
from jax.experimental.pallas import tpu as pltpu
from jax.sharding import PartitionSpec as P

NORM_EPS = 1e-6
ATTN_SCALE = (512 + 64) ** -0.5
ORDERS = ((0, 1, 2), (1, 2, 0), (2, 0, 1))
FULL = (4, 4, 4, 2, 8, 768)
STRIDES = (256, 64, 16)
POSITIONS, LATENT, ROPE, HEADS, LANES = 1024, 512, 64, 16, 128
ROWS = 64
KEY_COLS = 256
C_COLS, K_COLS, ALL_COLS = (0, LATENT), (LATENT, KEY_COLS), (0, LATENT + KEY_COLS)
CORE, COL = 3, 5
PARTS = range(3)
PAIR = range(2)
REQUESTS = range(4)
REQ = 512
GROUPS = 19
LOADS = 7
SIGNS = (1, -1)
EARLY, LATE = "1fwd and 2far", "2fwd and 3far"
OFFSETS = (0, -1, 1, 2)
NT = (((1,), (1,)), ((), ()))
F32, BF16 = jnp.float32, jnp.bfloat16


def all_parts(step, *args):
    for p in PARTS:
        step(p, *args)


def index(sel, dims=len(FULL)):
    return tuple(pl.ds(*sel[d]) if d in sel else slice(None) for d in range(dims))


def one(i):
    return (i, 1)


def place_of(me):
    return (me // 32, (me // 8) % 4, (me // 2) % 4)


def stepper(place):
    return lambda dim, delta: (place[dim] + delta + 4) % 4


def row_work(at, length, got, gain_row, q_cols, qk_cols, c_out, kr_out, score_out):
    def row_positions(a, b, c, ib, ic):
        r = lax.broadcasted_iota(jnp.int32, (ROWS, 1), 0)
        return (r // 16) * STRIDES[a] + r % 16 + ib * STRIDES[b] + ic * STRIDES[c]

    def unit_shape(a, width):
        return tuple(4 if d == a else 1 for d in range(3)) + (2, 8, width)

    def add_scores(a, wheres, rows, columns):
        part = jnp.dot(jnp.concatenate(rows, axis=0), columns, preferred_element_type=F32)
        for i, where in enumerate(wheres):
            score_out[where] += part[ROWS * i : ROWS * (i + 1)].reshape(unit_shape(a, LANES))

    def finish(j, a, wheres, raws, positions):
        gain = gain_row()
        rows = []
        for where, raw, pos in zip(wheres, raws, positions):
            square = jnp.sum(raw * raw, axis=-1, keepdims=True) * (1.0 / LATENT)
            inv_rms = jnp.where(pos < length(j), lax.rsqrt(square + NORM_EPS), 0.0)
            c_norm = raw * inv_rms * gain
            c_out[(j,) + where] = c_norm.reshape(unit_shape(a, LATENT)).astype(BF16)
            rows.append(c_norm.astype(BF16))
        add_scores(a, wheres, rows, q_cols[j])

    def units(p, off, steps):
        a, b, c = ORDERS[p]
        ib, ics = at(b, off), [at(c, step) for step in steps]
        wheres = [index({b: one(ib), c: one(ic)})[:COL] for ic in ics]
        full = [where + (slice(None),) for where in wheres]
        raws = [got[p][where + (pl.ds(*C_COLS),)].astype(F32).reshape(ROWS, LATENT) for where in wheres]
        finish(p, a, full, raws, [row_positions(a, b, c, ib, ic) for ic in ics])
        if p == 2:
            tiles = [got[2][where + (pl.ds(*K_COLS),)].astype(F32).reshape(ROWS, KEY_COLS).astype(BF16) for where in wheres]
            add_scores(a, full, tiles, qk_cols[...])

    def key_columns(z):
        row = lax.broadcasted_iota(jnp.int32, (KEY_COLS, KEY_COLS), 0)
        col = lax.broadcasted_iota(jnp.int32, (KEY_COLS, KEY_COLS), 1)
        eye = jnp.where(row == col, 1.0, 0.0).astype(BF16)
        tile = got[2][pl.ds(z, 1), :, :, :, :, pl.ds(*K_COLS)].astype(F32).reshape(KEY_COLS, KEY_COLS).astype(BF16)
        turned = lax.dot_general(eye, tile, NT, preferred_element_type=F32)
        for j in REQUESTS:
            valid = col[:ROPE] + z * KEY_COLS < length(j)
            kr_out[j, :, pl.ds(pl.multiple_of(z * KEY_COLS, KEY_COLS), KEY_COLS)] = jnp.where(valid, turned[ROPE * j : ROPE * (j + 1)], 0.0).astype(BF16)

    def last_request(steps):
        places = [(at(1, y), at(2, x)) for y, x in steps]
        wheres = [index({1: one(y), 2: one(x)})[:COL] for y, x in places]
        raws = [jnp.concatenate([got[p][where + (pl.ds(*K_COLS),)].astype(F32).reshape(ROWS, KEY_COLS) for p in PAIR], axis=1) for where in wheres]
        finish(3, 0, [where + (slice(None),) for where in wheres], raws, [row_positions(0, 1, 2, y, x) for y, x in places])

    return units, last_request, key_columns


def exchange_kernel(c_ref, k_ref, cos_ref, sin_ref, gain_ref, len_ref, qlat_ref, qrope_ref, c_out, kr_out, score_out, len_out, got, q_cols, qk_cols, gain_out, scratch):
    parts, k_laid, hop1, hop2, hop3, small, sems = scratch
    mid1, mid2 = [[parts.at[3 * stage + p] for p in PARTS] for stage in PAIR]
    got = [got.at[p] for p in PARTS]
    k_buf, angles, gain_buf, len_buf, qlat_buf, qrope_buf = small
    load_sem, send_sem, recv_sem = sems

    me = lax.axis_index("x")
    core = me % 2
    other = me + 1 - 2 * core
    other_core = 1 - core
    cores = (core, other_core)
    place = place_of(me)
    at = stepper(place)

    def device(dim, delta, to_core=None):
        pos = list(place)
        pos[dim] = (pos[dim] + delta + 4) % 4
        last = core if to_core is None else to_core
        return ((pos[0] * 4 + pos[1]) * 4 + pos[2]) * 2 + last

    def halves(s):
        return (2 * s, 2)

    def view(ref, sel):
        return ref.at[index(sel)]

    barrier = pltpu.get_barrier_semaphore()
    for dim in PARTS:
        for delta in SIGNS:
            for k in PAIR:
                pl.semaphore_signal(barrier, inc=1, device_id={"x": device(dim, delta, k)}, device_id_type=pl.DeviceIdType.MESH)
    pl.semaphore_signal(barrier, inc=1, device_id={"x": other}, device_id_type=pl.DeviceIdType.MESH)

    def taken(sem, n, shape):
        block = parts.at[(pl.ds(0, n),) + index(shape)]
        pltpu.make_async_copy(block, block, sem).wait()

    def taken_from(p, sel, extra):
        where = index(sel, COL - 1)
        if extra:
            return c_ref.at[where + (3, slice(None), pl.ds(KEY_COLS * p, KEY_COLS))]
        return c_ref.at[where + (p, slice(None), pl.ds(*C_COLS))]

    def load(slot, a, b):
        copy = pltpu.make_async_copy(a, b, load_sem.at[slot])
        copy.start()
        return copy

    load(0, cos_ref, angles.at[0])
    load(0, sin_ref, angles.at[1])
    small_loads = [load(1 + i, a, b) for i, (a, b) in enumerate(((k_ref, k_buf), (gain_ref, gain_buf), (len_ref, len_buf), (qlat_ref, qlat_buf), (qrope_ref, qrope_buf)))]
    for p in PARTS:
        own = {ORDERS[p][0]: one(place[ORDERS[p][0]])}
        load(LOADS - 1, taken_from(p, own, False), view(mid1[p], {**own, COL: C_COLS}))
        if p < 2:
            load(LOADS - 1, taken_from(p, own, True), view(mid1[p], {**own, COL: K_COLS}))

    slots = {}

    def send(group, a, b, to, sent=0):
        slot = slots.setdefault(group, len(slots))
        pltpu.make_async_remote_copy(src_ref=a, dst_ref=b, send_sem=send_sem.at[sent], recv_sem=recv_sem.at[slot], device_id={"x": to}, device_id_type=pl.DeviceIdType.MESH).start()

    def arrived(group, n, shape):
        taken(recv_sem.at[slots[group]], n, shape)

    def held(p, sel, cols):
        if cols == C_COLS:
            return taken_from(p, sel, False)
        return taken_from(p, sel, True) if p < 2 else view(k_laid, sel)

    def first_group(p, cols):
        return ("1far", p == 2 and cols == K_COLS)

    def far1(p, cols):
        a, b, _ = ORDERS[p]
        wide = {COL: cols}
        for s, sign in enumerate(SIGNS):
            send(first_group(p, cols), held(p, {a: one(at(a, 2)), b: halves(s)}, cols), view(hop1[2 * p + s], wide), device(a, sign))

    def near1(p, cols):
        a, b, _ = ORDERS[p]
        wide = {COL: cols}
        for s, sign in enumerate(SIGNS):
            send("1near", held(p, {a: one(at(a, sign))}, cols), view(mid1[p], {a: one(place[a]), **wide}), device(a, sign))

    def forward1(p, cols=ALL_COLS):
        a, b, _ = ORDERS[p]
        wide = {COL: cols}
        for s, sign in enumerate(SIGNS):
            send(EARLY, view(hop1[2 * p + s], wide), view(mid1[p], {a: one(at(a, -sign)), b: halves(s), **wide}), device(a, sign))

    def phase2(p, off):
        a, b, c = ORDERS[p]
        sa = {a: one(at(a, off))}
        hop_sa = {a: one(off % 4)}
        for s, sign in enumerate(SIGNS):
            send(EARLY if off == 0 else ("2far", abs(off)), view(mid1[p], {**sa, b: one(at(b, 2)), c: halves(s)}), view(hop2[2 * p + s], hop_sa), device(b, sign))
        for s, sign in enumerate(SIGNS):
            send("2near", view(mid1[p], {**sa, b: one(at(b, sign))}), view(mid2[p], {**sa, b: one(place[b])}), device(b, sign))

    def forward2(p, off):
        a, b, c = ORDERS[p]
        sa = {a: one(at(a, off))}
        hop_sa = {a: one(off % 4)}
        for s, sign in enumerate(SIGNS):
            send(LATE, view(hop2[2 * p + s], hop_sa), view(mid2[p], {**sa, b: one(at(b, -sign)), c: halves(s)}), device(b, sign))

    def phase3(p, off):
        a, b, c = ORDERS[p]
        sb = {b: one(at(b, off))}
        hop_sb = {b: one(off % 4)}
        got_b = mid1[p] if off == 0 else mid2[p]
        mine = {**sb, c: one(place[c]), CORE: one(core)}
        for s, sign in enumerate(SIGNS):
            send(LATE if off == -1 else ("3far", off), view(got_b, {**sb, c: one(at(c, 2)), CORE: one(cores[s])}), view(hop3[2 * p + s], hop_sb), device(c, sign, cores[1 - s]))
        for s, sign in enumerate(SIGNS):
            for k in PAIR:
                send(("3near", off), view(got_b, {**sb, c: one(at(c, sign)), CORE: one(cores[k])}), view(got[p], mine), device(c, sign, cores[k]))
        send(("3near", off), view(got_b, {**sb, c: one(place[c]), CORE: one(cores[1])}), view(got[p], mine), other, 1)
        got[p][index(mine)] = got_b[index(mine)]

    def forward3(p, off):
        a, b, c = ORDERS[p]
        sb = {b: one(at(b, off))}
        hop_sb = {b: one(off % 4)}
        for s, sign in enumerate(SIGNS):
            send(("3fwd", off), view(hop3[2 * p + s], hop_sb), view(got[p], {**sb, c: one(at(c, -sign)), CORE: one(cores[1 - s])}), device(c, sign, other_core))

    def length(j):
        return len_buf[4 * me + j]

    def keys():
        row = lax.broadcasted_iota(jnp.int32, (32, 32), 0)
        diag = row == lax.broadcasted_iota(jnp.int32, (32, 32), 1)
        roped = []
        for pos in range(8):
            cos = jnp.sum(jnp.where(diag, angles[0, pos : pos + 1, :], 0.0), axis=1, keepdims=True)
            sin = jnp.sum(jnp.where(diag, angles[1, pos : pos + 1, :], 0.0), axis=1, keepdims=True)
            lo = k_buf[pos, 0:32, :].astype(F32)
            hi = k_buf[pos, 32:64, :].astype(F32)
            roped.append(jnp.concatenate([lo * cos - hi * sin, hi * cos + lo * sin], axis=0).astype(BF16))
        out_row = lax.broadcasted_iota(jnp.int32, (256, 128), 0)
        lane = lax.broadcasted_iota(jnp.int32, (256, 128), 1)
        picks = [jnp.where((out_row % 8 == pos) & (out_row // 8 == lane // 4), 1.0, 0.0).astype(BF16) for pos in range(8)]
        pick = jnp.concatenate(picks, axis=1)
        request = lax.broadcasted_iota(jnp.int32, (64, 1024), 1) % 4
        for z in REQUESTS:
            cat = jnp.concatenate([r[:, 128 * z : 128 * (z + 1)] for r in roped], axis=1)
            masked = jnp.concatenate([jnp.where(request == j, cat, jnp.zeros_like(cat)) for j in REQUESTS], axis=0)
            laid = lax.dot_general(pick, masked, NT, preferred_element_type=F32)
            laid = laid.reshape(1, 4, 4, 2, 8, 256).astype(BF16)
            k_laid[z : z + 1] = laid
        own = {2: one(place[2])}
        mid1[2][index({**own, COL: K_COLS})] = k_laid[index(own)]

    def queries():
        for j in REQUESTS:
            rows = [qlat_buf[j].astype(F32) if i == j else jnp.zeros((HEADS, LATENT), F32) for i in REQUESTS]
            q_cols[j] = jnp.concatenate(rows + [jnp.zeros((LANES - 4 * HEADS, LATENT), F32)], axis=0).T.astype(BF16)
        zero = jnp.zeros((HEADS, ROPE), F32)
        rows = [jnp.concatenate([qrope_buf[j].astype(F32) if i == j else zero for i in REQUESTS], axis=1) for j in REQUESTS]
        qk_cols[...] = jnp.concatenate(rows + [jnp.zeros((LANES - 4 * HEADS, KEY_COLS), F32)], axis=0).T.astype(BF16)
        score_out[...] = jnp.zeros_like(score_out)
        lane = lax.broadcasted_iota(jnp.int32, (8, LANES), 1)
        lens = jnp.zeros((8, LANES), jnp.int32)
        for j in REQUESTS:
            lens = jnp.where(lane // HEADS == j, length(j), lens)
            len_out[j] = jnp.zeros((8, LANES), jnp.int32) + length(j)
        len_out[4] = lens
        gain_out[...] = jnp.broadcast_to(gain_buf[...].astype(F32).reshape(1, LATENT), gain_out.shape)

    units, last_request, key_columns = row_work(at, length, got, lambda: gain_out[0:1, :], q_cols, qk_cols, c_out, kr_out, score_out)

    def near_units(off):
        arrived(("3near", off), 5, {0: (0, 3), 1: one(0), CORE: one(0)})
        all_parts(units, off, OFFSETS[:3])

    def far_units(off):
        arrived(("3fwd", off), 3, {0: one(0), 1: one(0)})
        all_parts(units, off, OFFSETS[3:])
        key_columns(at(ORDERS[2][1], off))

    BOTH = {0: (0, 3), 2: (0, 2), CORE: one(0)}
    EIGHTH, SIXTEENTH = {0: one(0), 1: (0, 2)}, {0: one(0), 1: one(0)}
    pl.semaphore_wait(barrier, 13)
    for first in (far1, near1):
        all_parts(first, C_COLS)
        first(0, K_COLS)
        first(1, K_COLS)
    pltpu.make_async_copy(angles, angles, load_sem.at[0]).wait()
    small_loads[0].wait()
    keys()
    for copy in small_loads[1:]:
        copy.wait()
    queries()
    far1(2, K_COLS)
    near1(2, K_COLS)
    taken(load_sem.at[LOADS - 1], 4, {0: one(0), COL: C_COLS})
    arrived(first_group(2, C_COLS), 4, {0: one(0), COL: C_COLS})
    forward1(0)
    forward1(1)
    forward1(2, C_COLS)
    all_parts(phase2, 0)
    arrived(first_group(2, K_COLS), 1, {0: one(0), COL: K_COLS})
    forward1(2, K_COLS)
    arrived("1near", 3, {0: (0, 2)})
    all_parts(phase2, -1)
    all_parts(phase2, 1)
    arrived(EARLY, 5, BOTH)
    all_parts(forward2, 0)
    all_parts(phase2, 2)
    arrived(("2far", 1), 3, {0: one(0), 1: (0, 2)})
    all_parts(forward2, -1)
    all_parts(forward2, 1)
    arrived(("2far", 2), 3, SIXTEENTH)
    all_parts(forward2, 2)
    all_parts(phase3, 0)
    arrived("2near", 3, {0: (0, 2)})
    all_parts(phase3, -1)
    arrived(("3far", 0), 3, SIXTEENTH)
    all_parts(forward3, 0)
    all_parts(phase3, 1)
    near_units(0)
    arrived(LATE, 5, BOTH)
    all_parts(forward3, -1)
    all_parts(phase3, 2)
    near_units(-1)
    far_units(0)
    arrived(("3far", 1), 3, SIXTEENTH)
    all_parts(forward3, 1)
    near_units(1)
    far_units(-1)
    last_request([(y, x) for y in OFFSETS[:3] for x in OFFSETS[:2]])
    arrived(("3far", 2), 3, SIXTEENTH)
    all_parts(forward3, 2)
    near_units(2)
    far_units(1)
    last_request([(2, x) for x in OFFSETS[:2]] + [(y, 1) for y in OFFSETS])
    arrived(("3fwd", 2), 3, SIXTEENTH)
    taken(send_sem.at[0], 9, {})
    taken(send_sem.at[1], 3, EIGHTH)


def exchange(c_raw, k_turned, rope_cos, rope_sin, gain, seq_lens, q_lat, q_rope):
    def shaped(sizes):
        return pltpu.VMEM(tuple(sizes.get(d, FULL[d]) for d in range(6)), BF16)

    hop1 = [shaped({o[0]: 1, o[1]: 2}) for o in ORDERS for _ in PAIR]
    hop2 = [shaped({o[1]: 1, o[2]: 2}) for o in ORDERS for _ in PAIR]
    hop3 = [shaped({o[2]: 1, 3: 1}) for o in ORDERS for _ in PAIR]
    small = [
        pltpu.VMEM((8, 64, 512), BF16),
        pltpu.VMEM((2, 8, 32), F32),
        pltpu.VMEM((LATENT,), BF16),
        pltpu.SMEM((REQ,), jnp.int32),
        pltpu.VMEM((4, 16, 512), BF16),
        pltpu.VMEM((4, 16, 64), BF16),
    ]
    sems = [pltpu.SemaphoreType.DMA((n,)) for n in (LOADS, 2, GROUPS)]
    return pl.pallas_call(
        exchange_kernel,
        out_shape=[
            pltpu.VMEM((4, 4, 4, 4, 2, 8, 512), BF16),
            pltpu.VMEM((4, 64, 1024), BF16),
            pltpu.VMEM(FULL[:COL] + (LANES,), F32),
            pltpu.VMEM((5, 8, LANES), jnp.int32),
            pltpu.VMEM((3,) + FULL, BF16),
            pltpu.VMEM((4, LATENT, LANES), BF16),
            pltpu.VMEM((KEY_COLS, LANES), BF16),
            pltpu.VMEM((8, LATENT), F32),
        ],
        in_specs=[pl.BlockSpec(memory_space=pltpu.HBM)] * 8,
        out_specs=[pl.BlockSpec(memory_space=pltpu.VMEM)] * 8,
        scratch_shapes=[[pltpu.VMEM((9,) + FULL, BF16), shaped({COL: KEY_COLS}), hop1, hop2, hop3, small, sems]],
        compiler_params=pltpu.CompilerParams(collective_id=0, has_side_effects=True, vmem_limit_bytes=40 * 1024 * 1024),
        name="exchange",
    )(c_raw, k_turned, rope_cos, rope_sin, gain, seq_lens, q_lat, q_rope)


def attend_kernel(c_in, kr_in, score_in, len_ref, got_ref, q_cols, qk_cols, gain_ref, c_hbm, kr_hbm, o_hbm, c_buf, kr_buf, scores, o_buf, sem):
    at = stepper(place_of(lax.axis_index("x")))
    writes = []

    def write(a, b):
        writes.append(pltpu.make_async_copy(a, b, sem))
        writes[-1].start(priority=len(writes) % 2)

    def write_rows(j, sel):
        where = (j,) + index(sel)
        write(c_buf.at[where], c_hbm.at[where])

    def write_keys(z):
        where = (slice(None), slice(None), pl.ds(pl.multiple_of(z * KEY_COLS, KEY_COLS), KEY_COLS))
        write(kr_buf.at[where], kr_hbm.at[where])

    near, far = OFFSETS[:3], OFFSETS[3]
    for p, (_, b, c) in enumerate(ORDERS):
        for off in near:
            write_rows(p, {b: one(at(b, off))})
        for off in near:
            write_rows(p, {b: one(at(b, far)), c: one(at(c, off))})
    for off in near:
        write_rows(3, {2: one(at(2, off))})
        write_keys(at(ORDERS[2][1], off))

    got = [got_ref.at[p] for p in PARTS]
    units, last_request, key_columns = row_work(at, lambda j: len_ref[j, 0:1, 0:1], got, lambda: gain_ref[0:1, :], q_cols, qk_cols, c_buf, kr_buf, scores)
    all_parts(units, far, OFFSETS[3:])
    last_request([(y, far) for y in OFFSETS])
    for p, (_, b, c) in enumerate(ORDERS):
        write_rows(p, {b: one(at(b, far)), c: one(at(c, far))})
    write_rows(3, {2: one(at(2, far))})
    key_columns(at(ORDERS[2][1], far))
    write_keys(at(ORDERS[2][1], far))

    row = lax.broadcasted_iota(jnp.int32, (POSITIONS, LANES), 0)
    masked = jnp.where(row < len_ref[4, 0:1, :], scores[...].reshape(POSITIONS, LANES) * ATTN_SCALE, -1e30)
    weights = jnp.exp(masked - jnp.max(masked, axis=0, keepdims=True)).T
    weight_sum = jnp.sum(weights[: 4 * HEADS], axis=1, keepdims=True)
    rounded = weights[: 4 * HEADS].astype(BF16)
    for j in REQUESTS:
        mine = slice(HEADS * j, HEADS * (j + 1))
        weighted = jnp.dot(rounded[mine], c_buf[j].reshape(POSITIONS, LATENT), preferred_element_type=F32)
        o_buf[j] = (weighted / weight_sum[mine]).astype(BF16)
        write(o_buf.at[j], o_hbm.at[j])
    for copy in writes:
        copy.wait()


def attend(*handed):
    c_cache, kr_turned, scores = handed[:3]
    in_hbm, in_vmem = pl.BlockSpec(memory_space=pltpu.HBM), pl.BlockSpec(memory_space=pltpu.VMEM)
    return pl.pallas_call(
        attend_kernel,
        out_shape=[
            jax.ShapeDtypeStruct(c_cache.shape, BF16),
            jax.ShapeDtypeStruct(kr_turned.shape, BF16),
            jax.ShapeDtypeStruct((4, HEADS, LATENT), BF16),
            pltpu.VMEM(c_cache.shape, BF16),
            pltpu.VMEM(kr_turned.shape, BF16),
            pltpu.VMEM(scores.shape, F32),
        ],
        in_specs=[in_vmem] * len(handed),
        out_specs=[in_hbm] * 3 + [in_vmem] * 3,
        input_output_aliases={0: 3, 1: 4, 2: 5},
        scratch_shapes=[pltpu.VMEM((4, HEADS, LATENT), BF16), pltpu.SemaphoreType.DMA],
        compiler_params=pltpu.CompilerParams(vmem_limit_bytes=16 * 1024 * 1024),
        name="attend",
    )(*handed)[:3]


def solution(mesh):
    seq_spec = P("dp", "x", None)
    req_spec = P(("dp", "x"), None, None)

    def local_step(c_raw, k_raw, norm_gain, rope_cos, rope_sin, seq_lens, q_lat, q_rope):
        args = (c_raw.reshape(FULL[:4] + (4, 8, LATENT)), k_raw.transpose(1, 2, 0), rope_cos, rope_sin, norm_gain, seq_lens, q_lat, q_rope)
        handed = exchange(*[pltpu.with_memory_space_constraint(arg, pltpu.HBM) for arg in args])
        c_cache, kr_turned, o_lat = attend(*handed)
        c_cache = c_cache.reshape(4, POSITIONS, LATENT)
        return c_cache, kr_turned.transpose(0, 2, 1), o_lat

    return jax.shard_map(local_step, mesh=mesh, in_specs=(seq_spec, seq_spec, P(None), P("x", None), P("x", None), P("dp"), req_spec, req_spec), out_specs=(req_spec, req_spec, req_spec), check_vma=False)
```

```python
import jax
import jax.numpy as jnp
from jax import lax
from jax.experimental import pallas as pl
from jax.experimental.pallas import tpu as pltpu
from jax.sharding import PartitionSpec as P

NORM_EPS = 1e-6
ATTN_SCALE = (512 + 64) ** -0.5
ORDERS = ((0, 1, 2), (1, 2, 0), (2, 0, 1))
FULL = (4, 4, 4, 2, 8, 768)
STRIDES = (256, 64, 16)
POSITIONS, LATENT, ROPE, HEADS, LANES = 1024, 512, 64, 16, 128
ROWS = 64
KEY_COLS = 256
C_COLS, K_COLS, ALL_COLS = (0, LATENT), (LATENT, KEY_COLS), (0, LATENT + KEY_COLS)
CORE, COL = 3, 5
PARTS = range(3)
PAIR = range(2)
REQUESTS = range(4)
REQ = 512
GROUPS = 19
LOADS = 7
SIGNS = (1, -1)
EARLY, LATE = "1fwd and 2far", "2fwd and 3far"
OFFSETS = (0, -1, 1, 2)
NT = (((1,), (1,)), ((), ()))
F32, BF16 = jnp.float32, jnp.bfloat16


def all_parts(step, *args):
    for p in PARTS:
        step(p, *args)


def index(sel, dims=len(FULL)):
    return tuple(pl.ds(*sel[d]) if d in sel else slice(None) for d in range(dims))


def one(i):
    return (i, 1)


def place_of(me):
    return (me // 32, (me // 8) % 4, (me // 2) % 4)


def stepper(place):
    return lambda dim, delta: (place[dim] + delta + 4) % 4


def row_work(at, length, got, gain_row, q_cols, qk_cols, c_out, kr_out, score_out):
    def row_positions(a, b, c, ib, ic):
        r = lax.broadcasted_iota(jnp.int32, (ROWS, 1), 0)
        return (r // 16) * STRIDES[a] + r % 16 + ib * STRIDES[b] + ic * STRIDES[c]

    def unit_shape(a, width):
        return tuple(4 if d == a else 1 for d in range(3)) + (2, 8, width)

    def add_scores(a, wheres, rows, columns):
        part = jnp.dot(jnp.concatenate(rows, axis=0), columns, preferred_element_type=F32)
        for i, where in enumerate(wheres):
            score_out[where] += part[ROWS * i : ROWS * (i + 1)].reshape(unit_shape(a, LANES))

    def finish(j, a, wheres, raws, positions):
        gain = gain_row()
        rows = []
        for where, raw, pos in zip(wheres, raws, positions):
            square = jnp.sum(raw * raw, axis=-1, keepdims=True) * (1.0 / LATENT)
            inv_rms = jnp.where(pos < length(j), lax.rsqrt(square + NORM_EPS), 0.0)
            c_norm = raw * inv_rms * gain
            c_out[(j,) + where] = c_norm.reshape(unit_shape(a, LATENT)).astype(BF16)
            rows.append(c_norm.astype(BF16))
        add_scores(a, wheres, rows, q_cols[j])

    def units(p, off, steps):
        a, b, c = ORDERS[p]
        ib, ics = at(b, off), [at(c, step) for step in steps]
        wheres = [index({b: one(ib), c: one(ic)})[:COL] for ic in ics]
        full = [where + (slice(None),) for where in wheres]
        raws = [got[p][where + (pl.ds(*C_COLS),)].astype(F32).reshape(ROWS, LATENT) for where in wheres]
        finish(p, a, full, raws, [row_positions(a, b, c, ib, ic) for ic in ics])
        if p == 2:
            tiles = [got[2][where + (pl.ds(*K_COLS),)].astype(F32).reshape(ROWS, KEY_COLS).astype(BF16) for where in wheres]
            add_scores(a, full, tiles, qk_cols[...])

    def key_columns(z):
        row = lax.broadcasted_iota(jnp.int32, (KEY_COLS, KEY_COLS), 0)
        col = lax.broadcasted_iota(jnp.int32, (KEY_COLS, KEY_COLS), 1)
        eye = jnp.where(row == col, 1.0, 0.0).astype(BF16)
        tile = got[2][pl.ds(z, 1), :, :, :, :, pl.ds(*K_COLS)].astype(F32).reshape(KEY_COLS, KEY_COLS).astype(BF16)
        turned = lax.dot_general(eye, tile, NT, preferred_element_type=F32)
        for j in REQUESTS:
            valid = col[:ROPE] + z * KEY_COLS < length(j)
            kr_out[j, :, pl.ds(pl.multiple_of(z * KEY_COLS, KEY_COLS), KEY_COLS)] = jnp.where(valid, turned[ROPE * j : ROPE * (j + 1)], 0.0).astype(BF16)

    def last_request(steps):
        places = [(at(1, y), at(2, x)) for y, x in steps]
        wheres = [index({1: one(y), 2: one(x)})[:COL] for y, x in places]
        raws = [jnp.concatenate([got[p][where + (pl.ds(*K_COLS),)].astype(F32).reshape(ROWS, KEY_COLS) for p in PAIR], axis=1) for where in wheres]
        finish(3, 0, [where + (slice(None),) for where in wheres], raws, [row_positions(0, 1, 2, y, x) for y, x in places])

    return units, last_request, key_columns


def exchange_kernel(c_ref, k_ref, cos_ref, sin_ref, gain_ref, len_ref, qlat_ref, qrope_ref, c_out, kr_out, score_out, len_out, got, q_cols, qk_cols, gain_out, scratch):
    parts, k_laid, hop1, hop2, hop3, small, sems = scratch
    mid1, mid2 = [[parts.at[3 * stage + p] for p in PARTS] for stage in PAIR]
    got = [got.at[p] for p in PARTS]
    k_buf, angles, gain_buf, len_buf, qlat_buf, qrope_buf = small
    load_sem, send_sem, recv_sem = sems

    me = lax.axis_index("x")
    core = me % 2
    other = me + 1 - 2 * core
    other_core = 1 - core
    cores = (core, other_core)
    place = place_of(me)
    at = stepper(place)

    def device(dim, delta, to_core=None):
        pos = list(place)
        pos[dim] = (pos[dim] + delta + 4) % 4
        last = core if to_core is None else to_core
        return ((pos[0] * 4 + pos[1]) * 4 + pos[2]) * 2 + last

    def halves(s):
        return (2 * s, 2)

    def view(ref, sel):
        return ref.at[index(sel)]

    barrier = pltpu.get_barrier_semaphore()
    for dim in PARTS:
        for delta in SIGNS:
            for k in PAIR:
                pl.semaphore_signal(barrier, inc=1, device_id={"x": device(dim, delta, k)}, device_id_type=pl.DeviceIdType.MESH)
    pl.semaphore_signal(barrier, inc=1, device_id={"x": other}, device_id_type=pl.DeviceIdType.MESH)

    def taken(sem, n, shape):
        block = parts.at[(pl.ds(0, n),) + index(shape)]
        pltpu.make_async_copy(block, block, sem).wait()

    def taken_from(p, sel, extra):
        where = index(sel, COL - 1)
        if extra:
            return c_ref.at[where + (3, slice(None), pl.ds(KEY_COLS * p, KEY_COLS))]
        return c_ref.at[where + (p, slice(None), pl.ds(*C_COLS))]

    def load(slot, a, b):
        copy = pltpu.make_async_copy(a, b, load_sem.at[slot])
        copy.start()
        return copy

    load(0, cos_ref, angles.at[0])
    load(0, sin_ref, angles.at[1])
    small_loads = [load(1 + i, a, b) for i, (a, b) in enumerate(((k_ref, k_buf), (gain_ref, gain_buf), (len_ref, len_buf), (qlat_ref, qlat_buf), (qrope_ref, qrope_buf)))]
    for p in PARTS:
        own = {ORDERS[p][0]: one(place[ORDERS[p][0]])}
        load(LOADS - 1, taken_from(p, own, False), view(mid1[p], {**own, COL: C_COLS}))
        if p < 2:
            load(LOADS - 1, taken_from(p, own, True), view(mid1[p], {**own, COL: K_COLS}))

    slots = {}

    def send(group, a, b, to, sent=0):
        slot = slots.setdefault(group, len(slots))
        pltpu.make_async_remote_copy(src_ref=a, dst_ref=b, send_sem=send_sem.at[sent], recv_sem=recv_sem.at[slot], device_id={"x": to}, device_id_type=pl.DeviceIdType.MESH).start()

    def arrived(group, n, shape):
        taken(recv_sem.at[slots[group]], n, shape)

    def held(p, sel, cols):
        if cols == C_COLS:
            return taken_from(p, sel, False)
        return taken_from(p, sel, True) if p < 2 else view(k_laid, sel)

    def first_group(p, cols):
        return ("1far", p == 2 and cols == K_COLS)

    def far1(p, cols):
        a, b, _ = ORDERS[p]
        wide = {COL: cols}
        for s, sign in enumerate(SIGNS):
            send(first_group(p, cols), held(p, {a: one(at(a, 2)), b: halves(s)}, cols), view(hop1[2 * p + s], wide), device(a, sign))

    def near1(p, cols):
        a, b, _ = ORDERS[p]
        wide = {COL: cols}
        for s, sign in enumerate(SIGNS):
            send("1near", held(p, {a: one(at(a, sign))}, cols), view(mid1[p], {a: one(place[a]), **wide}), device(a, sign))

    def forward1(p, cols=ALL_COLS):
        a, b, _ = ORDERS[p]
        wide = {COL: cols}
        for s, sign in enumerate(SIGNS):
            send(EARLY, view(hop1[2 * p + s], wide), view(mid1[p], {a: one(at(a, -sign)), b: halves(s), **wide}), device(a, sign))

    def phase2(p, off):
        a, b, c = ORDERS[p]
        sa = {a: one(at(a, off))}
        hop_sa = {a: one(off % 4)}
        for s, sign in enumerate(SIGNS):
            send(EARLY if off == 0 else ("2far", abs(off)), view(mid1[p], {**sa, b: one(at(b, 2)), c: halves(s)}), view(hop2[2 * p + s], hop_sa), device(b, sign))
        for s, sign in enumerate(SIGNS):
            send("2near", view(mid1[p], {**sa, b: one(at(b, sign))}), view(mid2[p], {**sa, b: one(place[b])}), device(b, sign))

    def forward2(p, off):
        a, b, c = ORDERS[p]
        sa = {a: one(at(a, off))}
        hop_sa = {a: one(off % 4)}
        for s, sign in enumerate(SIGNS):
            send(LATE, view(hop2[2 * p + s], hop_sa), view(mid2[p], {**sa, b: one(at(b, -sign)), c: halves(s)}), device(b, sign))

    def phase3(p, off):
        a, b, c = ORDERS[p]
        sb = {b: one(at(b, off))}
        hop_sb = {b: one(off % 4)}
        got_b = mid1[p] if off == 0 else mid2[p]
        mine = {**sb, c: one(place[c]), CORE: one(core)}
        for s, sign in enumerate(SIGNS):
            send(LATE if off == -1 else ("3far", off), view(got_b, {**sb, c: one(at(c, 2)), CORE: one(cores[s])}), view(hop3[2 * p + s], hop_sb), device(c, sign, cores[1 - s]))
        for s, sign in enumerate(SIGNS):
            for k in PAIR:
                send(("3near", off), view(got_b, {**sb, c: one(at(c, sign)), CORE: one(cores[k])}), view(got[p], mine), device(c, sign, cores[k]))
        send(("3near", off), view(got_b, {**sb, c: one(place[c]), CORE: one(cores[1])}), view(got[p], mine), other, 1)
        got[p][index(mine)] = got_b[index(mine)]

    def forward3(p, off):
        a, b, c = ORDERS[p]
        sb = {b: one(at(b, off))}
        hop_sb = {b: one(off % 4)}
        for s, sign in enumerate(SIGNS):
            send(("3fwd", off), view(hop3[2 * p + s], hop_sb), view(got[p], {**sb, c: one(at(c, -sign)), CORE: one(cores[1 - s])}), device(c, sign, other_core))

    def length(j):
        return len_buf[4 * me + j]

    def keys():
        row = lax.broadcasted_iota(jnp.int32, (32, 32), 0)
        diag = row == lax.broadcasted_iota(jnp.int32, (32, 32), 1)
        roped = []
        for pos in range(8):
            cos = jnp.sum(jnp.where(diag, angles[0, pos : pos + 1, :], 0.0), axis=1, keepdims=True)
            sin = jnp.sum(jnp.where(diag, angles[1, pos : pos + 1, :], 0.0), axis=1, keepdims=True)
            lo = k_buf[pos, 0:32, :].astype(F32)
            hi = k_buf[pos, 32:64, :].astype(F32)
            roped.append(jnp.concatenate([lo * cos - hi * sin, hi * cos + lo * sin], axis=0).astype(BF16))
        out_row = lax.broadcasted_iota(jnp.int32, (256, 128), 0)
        lane = lax.broadcasted_iota(jnp.int32, (256, 128), 1)
        picks = [jnp.where((out_row % 8 == pos) & (out_row // 8 == lane // 4), 1.0, 0.0).astype(BF16) for pos in range(8)]
        pick = jnp.concatenate(picks, axis=1)
        request = lax.broadcasted_iota(jnp.int32, (64, 1024), 1) % 4
        for z in REQUESTS:
            cat = jnp.concatenate([r[:, 128 * z : 128 * (z + 1)] for r in roped], axis=1)
            masked = jnp.concatenate([jnp.where(request == j, cat, jnp.zeros_like(cat)) for j in REQUESTS], axis=0)
            laid = lax.dot_general(pick, masked, NT, preferred_element_type=F32)
            laid = laid.reshape(1, 4, 4, 2, 8, 256).astype(BF16)
            k_laid[z : z + 1] = laid
        own = {2: one(place[2])}
        mid1[2][index({**own, COL: K_COLS})] = k_laid[index(own)]

    def queries():
        for j in REQUESTS:
            rows = [qlat_buf[j].astype(F32) if i == j else jnp.zeros((HEADS, LATENT), F32) for i in REQUESTS]
            q_cols[j] = jnp.concatenate(rows + [jnp.zeros((LANES - 4 * HEADS, LATENT), F32)], axis=0).T.astype(BF16)
        zero = jnp.zeros((HEADS, ROPE), F32)
        rows = [jnp.concatenate([qrope_buf[j].astype(F32) if i == j else zero for i in REQUESTS], axis=1) for j in REQUESTS]
        qk_cols[...] = jnp.concatenate(rows + [jnp.zeros((LANES - 4 * HEADS, KEY_COLS), F32)], axis=0).T.astype(BF16)
        score_out[...] = jnp.zeros_like(score_out)
        lane = lax.broadcasted_iota(jnp.int32, (8, LANES), 1)
        lens = jnp.zeros((8, LANES), jnp.int32)
        for j in REQUESTS:
            lens = jnp.where(lane // HEADS == j, length(j), lens)
            len_out[j] = jnp.zeros((8, LANES), jnp.int32) + length(j)
        len_out[4] = lens
        gain_out[...] = jnp.broadcast_to(gain_buf[...].astype(F32).reshape(1, LATENT), gain_out.shape)

    units, last_request, key_columns = row_work(at, length, got, lambda: gain_out[0:1, :], q_cols, qk_cols, c_out, kr_out, score_out)

    def near_units(off):
        arrived(("3near", off), 5, {0: (0, 3), 1: one(0), CORE: one(0)})
        all_parts(units, off, OFFSETS[:3])

    def far_units(off):
        arrived(("3fwd", off), 3, {0: one(0), 1: one(0)})
        all_parts(units, off, OFFSETS[3:])
        key_columns(at(ORDERS[2][1], off))

    BOTH = {0: (0, 3), 2: (0, 2), CORE: one(0)}
    EIGHTH, SIXTEENTH = {0: one(0), 1: (0, 2)}, {0: one(0), 1: one(0)}
    pl.semaphore_wait(barrier, 13)
    for first in (far1, near1):
        all_parts(first, C_COLS)
        first(0, K_COLS)
        first(1, K_COLS)
    pltpu.make_async_copy(angles, angles, load_sem.at[0]).wait()
    small_loads[0].wait()
    keys()
    for copy in small_loads[1:]:
        copy.wait()
    queries()
    far1(2, K_COLS)
    near1(2, K_COLS)
    taken(load_sem.at[LOADS - 1], 4, {0: one(0), COL: C_COLS})
    arrived(first_group(2, C_COLS), 4, {0: one(0), COL: C_COLS})
    forward1(0)
    forward1(1)
    forward1(2, C_COLS)
    all_parts(phase2, 0)
    arrived(first_group(2, K_COLS), 1, {0: one(0), COL: K_COLS})
    forward1(2, K_COLS)
    arrived("1near", 3, {0: (0, 2)})
    all_parts(phase2, -1)
    all_parts(phase2, 1)
    arrived(EARLY, 5, BOTH)
    all_parts(forward2, 0)
    all_parts(phase2, 2)
    arrived(("2far", 1), 3, {0: one(0), 1: (0, 2)})
    all_parts(forward2, -1)
    all_parts(forward2, 1)
    arrived(("2far", 2), 3, SIXTEENTH)
    all_parts(forward2, 2)
    all_parts(phase3, 0)
    arrived("2near", 3, {0: (0, 2)})
    all_parts(phase3, -1)
    arrived(("3far", 0), 3, SIXTEENTH)
    all_parts(forward3, 0)
    all_parts(phase3, 1)
    near_units(0)
    arrived(LATE, 5, BOTH)
    all_parts(forward3, -1)
    all_parts(phase3, 2)
    near_units(-1)
    far_units(0)
    arrived(("3far", 1), 3, SIXTEENTH)
    all_parts(forward3, 1)
    near_units(1)
    far_units(-1)
    last_request([(y, x) for y in OFFSETS[:3] for x in OFFSETS[:2]])
    arrived(("3far", 2), 3, SIXTEENTH)
    all_parts(forward3, 2)
    near_units(2)
    far_units(1)
    last_request([(2, x) for x in OFFSETS[:2]] + [(y, 1) for y in OFFSETS])
    arrived(("3fwd", 2), 3, SIXTEENTH)
    taken(send_sem.at[0], 9, {})
    taken(send_sem.at[1], 3, EIGHTH)


def exchange(c_raw, k_turned, rope_cos, rope_sin, gain, seq_lens, q_lat, q_rope):
    def shaped(sizes):
        return pltpu.VMEM(tuple(sizes.get(d, FULL[d]) for d in range(6)), BF16)

    hop1 = [shaped({o[0]: 1, o[1]: 2}) for o in ORDERS for _ in PAIR]
    hop2 = [shaped({o[1]: 1, o[2]: 2}) for o in ORDERS for _ in PAIR]
    hop3 = [shaped({o[2]: 1, 3: 1}) for o in ORDERS for _ in PAIR]
    small = [
        pltpu.VMEM((8, 64, 512), BF16),
        pltpu.VMEM((2, 8, 32), F32),
        pltpu.VMEM((LATENT,), BF16),
        pltpu.SMEM((REQ,), jnp.int32),
        pltpu.VMEM((4, 16, 512), BF16),
        pltpu.VMEM((4, 16, 64), BF16),
    ]
    sems = [pltpu.SemaphoreType.DMA((n,)) for n in (LOADS, 2, GROUPS)]
    return pl.pallas_call(
        exchange_kernel,
        out_shape=[
            pltpu.VMEM((4, 4, 4, 4, 2, 8, 512), BF16),
            pltpu.VMEM((4, 64, 1024), BF16),
            pltpu.VMEM(FULL[:COL] + (LANES,), F32),
            pltpu.VMEM((5, 8, LANES), jnp.int32),
            pltpu.VMEM((3,) + FULL, BF16),
            pltpu.VMEM((4, LATENT, LANES), BF16),
            pltpu.VMEM((KEY_COLS, LANES), BF16),
            pltpu.VMEM((8, LATENT), F32),
        ],
        in_specs=[pl.BlockSpec(memory_space=pltpu.HBM)] * 8,
        out_specs=[pl.BlockSpec(memory_space=pltpu.VMEM)] * 8,
        scratch_shapes=[[pltpu.VMEM((9,) + FULL, BF16), shaped({COL: KEY_COLS}), hop1, hop2, hop3, small, sems]],
        compiler_params=pltpu.CompilerParams(collective_id=0, has_side_effects=True, vmem_limit_bytes=40 * 1024 * 1024),
        name="exchange",
    )(c_raw, k_turned, rope_cos, rope_sin, gain, seq_lens, q_lat, q_rope)


def attend_kernel(c_in, kr_in, score_in, len_ref, got_ref, q_cols, qk_cols, gain_ref, c_hbm, kr_hbm, o_hbm, c_buf, kr_buf, scores, o_buf, sem):
    at = stepper(place_of(lax.axis_index("x")))
    writes = []

    def write(a, b):
        writes.append(pltpu.make_async_copy(a, b, sem))
        writes[-1].start(priority=len(writes) % 2)

    def write_rows(j, sel):
        where = (j,) + index(sel)
        write(c_buf.at[where], c_hbm.at[where])

    def write_keys(z):
        where = (slice(None), slice(None), pl.ds(pl.multiple_of(z * KEY_COLS, KEY_COLS), KEY_COLS))
        write(kr_buf.at[where], kr_hbm.at[where])

    near, far = OFFSETS[:3], OFFSETS[3]
    for p, (_, b, c) in enumerate(ORDERS):
        for off in near:
            write_rows(p, {b: one(at(b, off))})
        for off in near:
            write_rows(p, {b: one(at(b, far)), c: one(at(c, off))})
    for off in near:
        write_rows(3, {2: one(at(2, off))})
        write_keys(at(ORDERS[2][1], off))

    got = [got_ref.at[p] for p in PARTS]
    units, last_request, key_columns = row_work(at, lambda j: len_ref[j, 0:1, 0:1], got, lambda: gain_ref[0:1, :], q_cols, qk_cols, c_buf, kr_buf, scores)
    all_parts(units, far, OFFSETS[3:])
    last_request([(y, far) for y in OFFSETS])
    for p, (_, b, c) in enumerate(ORDERS):
        write_rows(p, {b: one(at(b, far)), c: one(at(c, far))})
    write_rows(3, {2: one(at(2, far))})

    row = lax.broadcasted_iota(jnp.int32, (POSITIONS, LANES), 0)
    masked = jnp.where(row < len_ref[4, 0:1, :], scores[...].reshape(POSITIONS, LANES) * ATTN_SCALE, -1e30)
    weights = jnp.exp(masked - jnp.max(masked, axis=0, keepdims=True)).T
    weight_sum = jnp.sum(weights[: 4 * HEADS], axis=1, keepdims=True)
    rounded = weights[: 4 * HEADS].astype(BF16)
    for j in REQUESTS:
        mine = slice(HEADS * j, HEADS * (j + 1))
        weighted = jnp.dot(rounded[mine], c_buf[j].reshape(POSITIONS, LATENT), preferred_element_type=F32)
        o_buf[j] = (weighted / weight_sum[mine]).astype(BF16)
        write(o_buf.at[j], o_hbm.at[j])
        if j == 2:
            key_columns(at(ORDERS[2][1], far))
            write_keys(at(ORDERS[2][1], far))
    for copy in writes:
        copy.wait()


def attend(*handed):
    c_cache, kr_turned, scores = handed[:3]
    in_hbm, in_vmem = pl.BlockSpec(memory_space=pltpu.HBM), pl.BlockSpec(memory_space=pltpu.VMEM)
    return pl.pallas_call(
        attend_kernel,
        out_shape=[
            jax.ShapeDtypeStruct(c_cache.shape, BF16),
            jax.ShapeDtypeStruct(kr_turned.shape, BF16),
            jax.ShapeDtypeStruct((4, HEADS, LATENT), BF16),
            pltpu.VMEM(c_cache.shape, BF16),
            pltpu.VMEM(kr_turned.shape, BF16),
            pltpu.VMEM(scores.shape, F32),
        ],
        in_specs=[in_vmem] * len(handed),
        out_specs=[in_hbm] * 3 + [in_vmem] * 3,
        input_output_aliases={0: 3, 1: 4, 2: 5},
        scratch_shapes=[pltpu.VMEM((4, HEADS, LATENT), BF16), pltpu.SemaphoreType.DMA],
        compiler_params=pltpu.CompilerParams(vmem_limit_bytes=16 * 1024 * 1024),
        name="attend",
    )(*handed)[:3]


def solution(mesh):
    seq_spec = P("dp", "x", None)
    req_spec = P(("dp", "x"), None, None)

    def local_step(c_raw, k_raw, norm_gain, rope_cos, rope_sin, seq_lens, q_lat, q_rope):
        args = (c_raw.reshape(FULL[:4] + (4, 8, LATENT)), k_raw.transpose(1, 2, 0), rope_cos, rope_sin, norm_gain, seq_lens, q_lat, q_rope)
        handed = exchange(*[pltpu.with_memory_space_constraint(arg, pltpu.HBM) for arg in args])
        c_cache, kr_turned, o_lat = attend(*handed)
        c_cache = c_cache.reshape(4, POSITIONS, LATENT)
        return c_cache, kr_turned.transpose(0, 2, 1), o_lat

    return jax.shard_map(local_step, mesh=mesh, in_specs=(seq_spec, seq_spec, P(None), P("x", None), P("x", None), P("dp"), req_spec, req_spec), out_specs=(req_spec, req_spec, req_spec), check_vma=False)
```

```python
import jax
import jax.numpy as jnp
from jax import lax
from jax.experimental import pallas as pl
from jax.experimental.pallas import tpu as pltpu
from jax.sharding import PartitionSpec as P

NORM_EPS = 1e-6
ATTN_SCALE = (512 + 64) ** -0.5
ORDERS = ((0, 1, 2), (1, 2, 0), (2, 0, 1))
FULL = (4, 4, 4, 2, 8, 768)
STRIDES = (256, 64, 16)
POSITIONS, LATENT, ROPE, HEADS, LANES = 1024, 512, 64, 16, 128
ROWS = 64
KEY_COLS = 256
C_COLS, K_COLS, ALL_COLS = (0, LATENT), (LATENT, KEY_COLS), (0, LATENT + KEY_COLS)
CORE, COL = 3, 5
PARTS = range(3)
PAIR = range(2)
REQUESTS = range(4)
REQ = 512
GROUPS = 19
LOADS = 7
SIGNS = (1, -1)
EARLY, LATE = "1fwd and 2far", "2fwd and 3far"
OFFSETS = (0, -1, 1, 2)
NT = (((1,), (1,)), ((), ()))
F32, BF16 = jnp.float32, jnp.bfloat16


def all_parts(step, *args):
    for p in PARTS:
        step(p, *args)


def index(sel, dims=len(FULL)):
    return tuple(pl.ds(*sel[d]) if d in sel else slice(None) for d in range(dims))


def one(i):
    return (i, 1)


def place_of(me):
    return (me // 32, (me // 8) % 4, (me // 2) % 4)


def stepper(place):
    return lambda dim, delta: (place[dim] + delta + 4) % 4


def row_work(at, length, got, gain_row, q_cols, qk_cols, c_out, kr_out, score_out):
    def row_positions(a, b, c, ib, ic):
        r = lax.broadcasted_iota(jnp.int32, (ROWS, 1), 0)
        return (r // 16) * STRIDES[a] + r % 16 + ib * STRIDES[b] + ic * STRIDES[c]

    def unit_shape(a, width):
        return tuple(4 if d == a else 1 for d in range(3)) + (2, 8, width)

    def add_scores(a, wheres, rows, columns):
        part = jnp.dot(jnp.concatenate(rows, axis=0), columns, preferred_element_type=F32)
        for i, where in enumerate(wheres):
            score_out[where] += part[ROWS * i : ROWS * (i + 1)].reshape(unit_shape(a, LANES))

    def finish(j, a, wheres, raws, positions):
        gain = gain_row()
        rows = []
        for where, raw, pos in zip(wheres, raws, positions):
            square = jnp.sum(raw * raw, axis=-1, keepdims=True) * (1.0 / LATENT)
            inv_rms = jnp.where(pos < length(j), lax.rsqrt(square + NORM_EPS), 0.0)
            c_norm = raw * inv_rms * gain
            c_out[(j,) + where] = c_norm.reshape(unit_shape(a, LATENT)).astype(BF16)
            rows.append(c_norm.astype(BF16))
        add_scores(a, wheres, rows, q_cols[j])

    def units(p, off, steps):
        a, b, c = ORDERS[p]
        ib, ics = at(b, off), [at(c, step) for step in steps]
        wheres = [index({b: one(ib), c: one(ic)})[:COL] for ic in ics]
        full = [where + (slice(None),) for where in wheres]
        raws = [got[p][where + (pl.ds(*C_COLS),)].astype(F32).reshape(ROWS, LATENT) for where in wheres]
        finish(p, a, full, raws, [row_positions(a, b, c, ib, ic) for ic in ics])
        if p == 2:
            tiles = [got[2][where + (pl.ds(*K_COLS),)].astype(F32).reshape(ROWS, KEY_COLS).astype(BF16) for where in wheres]
            add_scores(a, full, tiles, qk_cols[...])

    def key_columns(z):
        row = lax.broadcasted_iota(jnp.int32, (KEY_COLS, KEY_COLS), 0)
        col = lax.broadcasted_iota(jnp.int32, (KEY_COLS, KEY_COLS), 1)
        eye = jnp.where(row == col, 1.0, 0.0).astype(BF16)
        tile = got[2][pl.ds(z, 1), :, :, :, :, pl.ds(*K_COLS)].astype(F32).reshape(KEY_COLS, KEY_COLS).astype(BF16)
        turned = lax.dot_general(eye, tile, NT, preferred_element_type=F32)
        for j in REQUESTS:
            valid = col[:ROPE] + z * KEY_COLS < length(j)
            kr_out[j, :, pl.ds(pl.multiple_of(z * KEY_COLS, KEY_COLS), KEY_COLS)] = jnp.where(valid, turned[ROPE * j : ROPE * (j + 1)], 0.0).astype(BF16)

    def last_request(steps):
        places = [(at(1, y), at(2, x)) for y, x in steps]
        wheres = [index({1: one(y), 2: one(x)})[:COL] for y, x in places]
        raws = [jnp.concatenate([got[p][where + (pl.ds(*K_COLS),)].astype(F32).reshape(ROWS, KEY_COLS) for p in PAIR], axis=1) for where in wheres]
        finish(3, 0, [where + (slice(None),) for where in wheres], raws, [row_positions(0, 1, 2, y, x) for y, x in places])

    return units, last_request, key_columns


def exchange_kernel(c_ref, k_ref, cos_ref, sin_ref, gain_ref, len_ref, qlat_ref, qrope_ref, c_out, kr_out, score_out, len_out, got, q_cols, qk_cols, gain_out, scratch):
    parts, k_laid, hop1, hop2, hop3, small, sems = scratch
    mid1, mid2 = [[parts.at[3 * stage + p] for p in PARTS] for stage in PAIR]
    got = [got.at[p] for p in PARTS]
    k_buf, angles, gain_buf, len_buf, qlat_buf, qrope_buf = small
    load_sem, send_sem, recv_sem = sems

    me = lax.axis_index("x")
    core = me % 2
    other = me + 1 - 2 * core
    other_core = 1 - core
    cores = (core, other_core)
    place = place_of(me)
    at = stepper(place)

    def device(dim, delta, to_core=None):
        pos = list(place)
        pos[dim] = (pos[dim] + delta + 4) % 4
        last = core if to_core is None else to_core
        return ((pos[0] * 4 + pos[1]) * 4 + pos[2]) * 2 + last

    def halves(s):
        return (2 * s, 2)

    def view(ref, sel):
        return ref.at[index(sel)]

    barrier = pltpu.get_barrier_semaphore()
    for dim in PARTS:
        for delta in SIGNS:
            for k in PAIR:
                pl.semaphore_signal(barrier, inc=1, device_id={"x": device(dim, delta, k)}, device_id_type=pl.DeviceIdType.MESH)
    pl.semaphore_signal(barrier, inc=1, device_id={"x": other}, device_id_type=pl.DeviceIdType.MESH)

    def taken(sem, n, shape):
        block = parts.at[(pl.ds(0, n),) + index(shape)]
        pltpu.make_async_copy(block, block, sem).wait()

    def taken_from(p, sel, extra):
        where = index(sel, COL - 1)
        if extra:
            return c_ref.at[where + (3, slice(None), pl.ds(KEY_COLS * p, KEY_COLS))]
        return c_ref.at[where + (p, slice(None), pl.ds(*C_COLS))]

    def load(slot, a, b):
        copy = pltpu.make_async_copy(a, b, load_sem.at[slot])
        copy.start()
        return copy

    load(0, cos_ref, angles.at[0])
    load(0, sin_ref, angles.at[1])
    small_loads = [load(1 + i, a, b) for i, (a, b) in enumerate(((k_ref, k_buf), (gain_ref, gain_buf), (len_ref, len_buf), (qlat_ref, qlat_buf), (qrope_ref, qrope_buf)))]
    for p in PARTS:
        own = {ORDERS[p][0]: one(place[ORDERS[p][0]])}
        load(LOADS - 1, taken_from(p, own, False), view(mid1[p], {**own, COL: C_COLS}))
        if p < 2:
            load(LOADS - 1, taken_from(p, own, True), view(mid1[p], {**own, COL: K_COLS}))

    slots = {}

    def send(group, a, b, to, sent=0):
        slot = slots.setdefault(group, len(slots))
        pltpu.make_async_remote_copy(src_ref=a, dst_ref=b, send_sem=send_sem.at[sent], recv_sem=recv_sem.at[slot], device_id={"x": to}, device_id_type=pl.DeviceIdType.MESH).start()

    def arrived(group, n, shape):
        taken(recv_sem.at[slots[group]], n, shape)

    def held(p, sel, cols):
        if cols == C_COLS:
            return taken_from(p, sel, False)
        return taken_from(p, sel, True) if p < 2 else view(k_laid, sel)

    def first_group(p, cols):
        return ("1far", p == 2 and cols == K_COLS)

    def far1(p, cols):
        a, b, _ = ORDERS[p]
        wide = {COL: cols}
        for s, sign in enumerate(SIGNS):
            send(first_group(p, cols), held(p, {a: one(at(a, 2)), b: halves(s)}, cols), view(hop1[2 * p + s], wide), device(a, sign))

    def near1(p, cols):
        a, b, _ = ORDERS[p]
        wide = {COL: cols}
        for s, sign in enumerate(SIGNS):
            send("1near", held(p, {a: one(at(a, sign))}, cols), view(mid1[p], {a: one(place[a]), **wide}), device(a, sign))

    def forward1(p, cols=ALL_COLS):
        a, b, _ = ORDERS[p]
        wide = {COL: cols}
        for s, sign in enumerate(SIGNS):
            send(EARLY, view(hop1[2 * p + s], wide), view(mid1[p], {a: one(at(a, -sign)), b: halves(s), **wide}), device(a, sign))

    def phase2(p, off):
        a, b, c = ORDERS[p]
        sa = {a: one(at(a, off))}
        hop_sa = {a: one(off % 4)}
        for s, sign in enumerate(SIGNS):
            send(EARLY if off == 0 else ("2far", abs(off)), view(mid1[p], {**sa, b: one(at(b, 2)), c: halves(s)}), view(hop2[2 * p + s], hop_sa), device(b, sign))
        for s, sign in enumerate(SIGNS):
            send("2near", view(mid1[p], {**sa, b: one(at(b, sign))}), view(mid2[p], {**sa, b: one(place[b])}), device(b, sign))

    def forward2(p, off):
        a, b, c = ORDERS[p]
        sa = {a: one(at(a, off))}
        hop_sa = {a: one(off % 4)}
        for s, sign in enumerate(SIGNS):
            send(LATE, view(hop2[2 * p + s], hop_sa), view(mid2[p], {**sa, b: one(at(b, -sign)), c: halves(s)}), device(b, sign))

    def phase3(p, off):
        a, b, c = ORDERS[p]
        sb = {b: one(at(b, off))}
        hop_sb = {b: one(off % 4)}
        got_b = mid1[p] if off == 0 else mid2[p]
        mine = {**sb, c: one(place[c]), CORE: one(core)}
        for s, sign in enumerate(SIGNS):
            send(LATE if off == -1 else ("3far", off), view(got_b, {**sb, c: one(at(c, 2)), CORE: one(cores[s])}), view(hop3[2 * p + s], hop_sb), device(c, sign, cores[1 - s]))
        for s, sign in enumerate(SIGNS):
            for k in PAIR:
                send(("3near", off), view(got_b, {**sb, c: one(at(c, sign)), CORE: one(cores[k])}), view(got[p], mine), device(c, sign, cores[k]))
        send(("3near", off), view(got_b, {**sb, c: one(place[c]), CORE: one(cores[1])}), view(got[p], mine), other, 1)
        got[p][index(mine)] = got_b[index(mine)]

    def forward3(p, off):
        a, b, c = ORDERS[p]
        sb = {b: one(at(b, off))}
        hop_sb = {b: one(off % 4)}
        for s, sign in enumerate(SIGNS):
            send(("3fwd", off), view(hop3[2 * p + s], hop_sb), view(got[p], {**sb, c: one(at(c, -sign)), CORE: one(cores[1 - s])}), device(c, sign, other_core))

    def length(j):
        return len_buf[4 * me + j]

    def keys():
        row = lax.broadcasted_iota(jnp.int32, (32, 32), 0)
        diag = row == lax.broadcasted_iota(jnp.int32, (32, 32), 1)
        roped = []
        for pos in range(8):
            cos = jnp.sum(jnp.where(diag, angles[0, pos : pos + 1, :], 0.0), axis=1, keepdims=True)
            sin = jnp.sum(jnp.where(diag, angles[1, pos : pos + 1, :], 0.0), axis=1, keepdims=True)
            lo = k_buf[pos, 0:32, :].astype(F32)
            hi = k_buf[pos, 32:64, :].astype(F32)
            roped.append(jnp.concatenate([lo * cos - hi * sin, hi * cos + lo * sin], axis=0).astype(BF16))
        out_row = lax.broadcasted_iota(jnp.int32, (256, 128), 0)
        lane = lax.broadcasted_iota(jnp.int32, (256, 128), 1)
        picks = [jnp.where((out_row % 8 == pos) & (out_row // 8 == lane // 4), 1.0, 0.0).astype(BF16) for pos in range(8)]
        pick = jnp.concatenate(picks, axis=1)
        request = lax.broadcasted_iota(jnp.int32, (64, 1024), 1) % 4
        for z in REQUESTS:
            cat = jnp.concatenate([r[:, 128 * z : 128 * (z + 1)] for r in roped], axis=1)
            masked = jnp.concatenate([jnp.where(request == j, cat, jnp.zeros_like(cat)) for j in REQUESTS], axis=0)
            laid = lax.dot_general(pick, masked, NT, preferred_element_type=F32)
            laid = laid.reshape(1, 4, 4, 2, 8, 256).astype(BF16)
            k_laid[z : z + 1] = laid
        own = {2: one(place[2])}
        mid1[2][index({**own, COL: K_COLS})] = k_laid[index(own)]

    def queries():
        for j in REQUESTS:
            rows = [qlat_buf[j].astype(F32) if i == j else jnp.zeros((HEADS, LATENT), F32) for i in REQUESTS]
            q_cols[j] = jnp.concatenate(rows + [jnp.zeros((LANES - 4 * HEADS, LATENT), F32)], axis=0).T.astype(BF16)
        zero = jnp.zeros((HEADS, ROPE), F32)
        rows = [jnp.concatenate([qrope_buf[j].astype(F32) if i == j else zero for i in REQUESTS], axis=1) for j in REQUESTS]
        qk_cols[...] = jnp.concatenate(rows + [jnp.zeros((LANES - 4 * HEADS, KEY_COLS), F32)], axis=0).T.astype(BF16)
        score_out[...] = jnp.zeros_like(score_out)
        lane = lax.broadcasted_iota(jnp.int32, (8, LANES), 1)
        lens = jnp.zeros((8, LANES), jnp.int32)
        for j in REQUESTS:
            lens = jnp.where(lane // HEADS == j, length(j), lens)
            len_out[j] = jnp.zeros((8, LANES), jnp.int32) + length(j)
        len_out[4] = lens
        gain_out[...] = jnp.broadcast_to(gain_buf[...].astype(F32).reshape(1, LATENT), gain_out.shape)

    units, last_request, key_columns = row_work(at, length, got, lambda: gain_out[0:1, :], q_cols, qk_cols, c_out, kr_out, score_out)

    def near_units(off):
        arrived(("3near", off), 5, {0: (0, 3), 1: one(0), CORE: one(0)})
        all_parts(units, off, OFFSETS[:3])

    def far_units(off):
        arrived(("3fwd", off), 3, {0: one(0), 1: one(0)})
        all_parts(units, off, OFFSETS[3:])
        key_columns(at(ORDERS[2][1], off))

    BOTH = {0: (0, 3), 2: (0, 2), CORE: one(0)}
    EIGHTH, SIXTEENTH = {0: one(0), 1: (0, 2)}, {0: one(0), 1: one(0)}
    pl.semaphore_wait(barrier, 13)
    for first in (far1, near1):
        all_parts(first, C_COLS)
        first(0, K_COLS)
        first(1, K_COLS)
    pltpu.make_async_copy(angles, angles, load_sem.at[0]).wait()
    small_loads[0].wait()
    keys()
    for copy in small_loads[1:]:
        copy.wait()
    queries()
    far1(2, K_COLS)
    near1(2, K_COLS)
    taken(load_sem.at[LOADS - 1], 4, {0: one(0), COL: C_COLS})
    arrived(first_group(2, C_COLS), 4, {0: one(0), COL: C_COLS})
    forward1(0)
    forward1(1)
    forward1(2, C_COLS)
    all_parts(phase2, 0)
    arrived(first_group(2, K_COLS), 1, {0: one(0), COL: K_COLS})
    forward1(2, K_COLS)
    arrived("1near", 3, {0: (0, 2)})
    all_parts(phase2, -1)
    all_parts(phase2, 1)
    arrived(EARLY, 5, BOTH)
    all_parts(forward2, 0)
    all_parts(phase2, 2)
    arrived(("2far", 1), 3, {0: one(0), 1: (0, 2)})
    all_parts(forward2, -1)
    all_parts(forward2, 1)
    arrived(("2far", 2), 3, SIXTEENTH)
    all_parts(forward2, 2)
    all_parts(phase3, 0)
    arrived("2near", 3, {0: (0, 2)})
    all_parts(phase3, -1)
    arrived(("3far", 0), 3, SIXTEENTH)
    all_parts(forward3, 0)
    all_parts(phase3, 1)
    near_units(0)
    arrived(LATE, 5, BOTH)
    all_parts(forward3, -1)
    all_parts(phase3, 2)
    near_units(-1)
    far_units(0)
    arrived(("3far", 1), 3, SIXTEENTH)
    all_parts(forward3, 1)
    near_units(1)
    far_units(-1)
    last_request([(y, x) for y in OFFSETS[:3] for x in OFFSETS[:2]])
    arrived(("3far", 2), 3, SIXTEENTH)
    all_parts(forward3, 2)
    near_units(2)
    far_units(1)
    last_request([(2, x) for x in OFFSETS[:2]] + [(y, 1) for y in OFFSETS])
    arrived(("3fwd", 2), 3, SIXTEENTH)
    taken(send_sem.at[0], 9, {})
    taken(send_sem.at[1], 3, EIGHTH)


def exchange(c_raw, k_turned, rope_cos, rope_sin, gain, seq_lens, q_lat, q_rope):
    def shaped(sizes):
        return pltpu.VMEM(tuple(sizes.get(d, FULL[d]) for d in range(6)), BF16)

    hop1 = [shaped({o[0]: 1, o[1]: 2}) for o in ORDERS for _ in PAIR]
    hop2 = [shaped({o[1]: 1, o[2]: 2}) for o in ORDERS for _ in PAIR]
    hop3 = [shaped({o[2]: 1, 3: 1}) for o in ORDERS for _ in PAIR]
    small = [
        pltpu.VMEM((8, 64, 512), BF16),
        pltpu.VMEM((2, 8, 32), F32),
        pltpu.VMEM((LATENT,), BF16),
        pltpu.SMEM((REQ,), jnp.int32),
        pltpu.VMEM((4, 16, 512), BF16),
        pltpu.VMEM((4, 16, 64), BF16),
    ]
    sems = [pltpu.SemaphoreType.DMA((n,)) for n in (LOADS, 2, GROUPS)]
    return pl.pallas_call(
        exchange_kernel,
        out_shape=[
            pltpu.VMEM((4, 4, 4, 4, 2, 8, 512), BF16),
            pltpu.VMEM((4, 64, 1024), BF16),
            pltpu.VMEM(FULL[:COL] + (LANES,), F32),
            pltpu.VMEM((5, 8, LANES), jnp.int32),
            pltpu.VMEM((3,) + FULL, BF16),
            pltpu.VMEM((4, LATENT, LANES), BF16),
            pltpu.VMEM((KEY_COLS, LANES), BF16),
            pltpu.VMEM((8, LATENT), F32),
        ],
        in_specs=[pl.BlockSpec(memory_space=pltpu.HBM)] * 8,
        out_specs=[pl.BlockSpec(memory_space=pltpu.VMEM)] * 8,
        scratch_shapes=[[pltpu.VMEM((9,) + FULL, BF16), shaped({COL: KEY_COLS}), hop1, hop2, hop3, small, sems]],
        compiler_params=pltpu.CompilerParams(collective_id=0, has_side_effects=True, vmem_limit_bytes=40 * 1024 * 1024),
        name="exchange",
    )(c_raw, k_turned, rope_cos, rope_sin, gain, seq_lens, q_lat, q_rope)


def attend_kernel(c_in, kr_in, score_in, len_ref, got_ref, q_cols, qk_cols, gain_ref, c_hbm, kr_hbm, o_hbm, c_buf, kr_buf, scores, o_buf, sem):
    at = stepper(place_of(lax.axis_index("x")))
    writes = []

    def write(a, b):
        writes.append(pltpu.make_async_copy(a, b, sem))
        writes[-1].start(priority=len(writes) % 2)

    def write_rows(j, sel):
        where = (j,) + index(sel)
        write(c_buf.at[where], c_hbm.at[where])

    def write_keys(z):
        where = (slice(None), slice(None), pl.ds(pl.multiple_of(z * KEY_COLS, KEY_COLS), KEY_COLS))
        write(kr_buf.at[where], kr_hbm.at[where])

    near, far = OFFSETS[:3], OFFSETS[3]
    for p, (_, b, c) in enumerate(ORDERS):
        for off in near:
            write_rows(p, {b: one(at(b, off))})
        for off in near:
            write_rows(p, {b: one(at(b, far)), c: one(at(c, off))})
    for off in near:
        write_rows(3, {2: one(at(2, off))})
        write_keys(at(ORDERS[2][1], off))

    got = [got_ref.at[p] for p in PARTS]
    units, last_request, key_columns = row_work(at, lambda j: len_ref[j, 0:1, 0:1], got, lambda: gain_ref[0:1, :], q_cols, qk_cols, c_buf, kr_buf, scores)
    key_columns(at(ORDERS[2][1], far))
    write_keys(at(ORDERS[2][1], far))
    all_parts(units, far, OFFSETS[3:])
    last_request([(y, far) for y in OFFSETS])
    for p, (_, b, c) in enumerate(ORDERS):
        write_rows(p, {b: one(at(b, far)), c: one(at(c, far))})
    write_rows(3, {2: one(at(2, far))})

    row = lax.broadcasted_iota(jnp.int32, (POSITIONS, LANES), 0)
    masked = jnp.where(row < len_ref[4, 0:1, :], scores[...].reshape(POSITIONS, LANES) * ATTN_SCALE, -1e30)
    weights = jnp.exp(masked - jnp.max(masked, axis=0, keepdims=True)).T
    weight_sum = jnp.sum(weights[: 4 * HEADS], axis=1, keepdims=True)
    rounded = weights[: 4 * HEADS].astype(BF16)
    for j in REQUESTS:
        mine = slice(HEADS * j, HEADS * (j + 1))
        weighted = jnp.dot(rounded[mine], c_buf[j].reshape(POSITIONS, LATENT), preferred_element_type=F32)
        o_buf[j] = (weighted / weight_sum[mine]).astype(BF16)
        write(o_buf.at[j], o_hbm.at[j])
    for copy in writes:
        copy.wait()


def attend(*handed):
    c_cache, kr_turned, scores = handed[:3]
    in_hbm, in_vmem = pl.BlockSpec(memory_space=pltpu.HBM), pl.BlockSpec(memory_space=pltpu.VMEM)
    return pl.pallas_call(
        attend_kernel,
        out_shape=[
            jax.ShapeDtypeStruct(c_cache.shape, BF16),
            jax.ShapeDtypeStruct(kr_turned.shape, BF16),
            jax.ShapeDtypeStruct((4, HEADS, LATENT), BF16),
            pltpu.VMEM(c_cache.shape, BF16),
            pltpu.VMEM(kr_turned.shape, BF16),
            pltpu.VMEM(scores.shape, F32),
        ],
        in_specs=[in_vmem] * len(handed),
        out_specs=[in_hbm] * 3 + [in_vmem] * 3,
        input_output_aliases={0: 3, 1: 4, 2: 5},
        scratch_shapes=[pltpu.VMEM((4, HEADS, LATENT), BF16), pltpu.SemaphoreType.DMA],
        compiler_params=pltpu.CompilerParams(vmem_limit_bytes=16 * 1024 * 1024),
        name="attend",
    )(*handed)[:3]


def solution(mesh):
    seq_spec = P("dp", "x", None)
    req_spec = P(("dp", "x"), None, None)

    def local_step(c_raw, k_raw, norm_gain, rope_cos, rope_sin, seq_lens, q_lat, q_rope):
        args = (c_raw.reshape(FULL[:4] + (4, 8, LATENT)), k_raw.transpose(1, 2, 0), rope_cos, rope_sin, norm_gain, seq_lens, q_lat, q_rope)
        handed = exchange(*[pltpu.with_memory_space_constraint(arg, pltpu.HBM) for arg in args])
        c_cache, kr_turned, o_lat = attend(*handed)
        c_cache = c_cache.reshape(4, POSITIONS, LATENT)
        return c_cache, kr_turned.transpose(0, 2, 1), o_lat

    return jax.shard_map(local_step, mesh=mesh, in_specs=(seq_spec, seq_spec, P(None), P("x", None), P("x", None), P("dp"), req_spec, req_spec), out_specs=(req_spec, req_spec, req_spec), check_vma=False)
```

```python
import jax
import jax.numpy as jnp
from jax import lax
from jax.experimental import pallas as pl
from jax.experimental.pallas import tpu as pltpu
from jax.sharding import PartitionSpec as P

NORM_EPS = 1e-6
ATTN_SCALE = (512 + 64) ** -0.5
ORDERS = ((0, 1, 2), (1, 2, 0), (2, 0, 1))
FULL = (4, 4, 4, 2, 8, 768)
STRIDES = (256, 64, 16)
POSITIONS, LATENT, ROPE, HEADS, LANES = 1024, 512, 64, 16, 128
ROWS = 64
KEY_COLS = 256
C_COLS, K_COLS, ALL_COLS = (0, LATENT), (LATENT, KEY_COLS), (0, LATENT + KEY_COLS)
CORE, COL = 3, 5
PARTS = range(3)
PAIR = range(2)
REQUESTS = range(4)
REQ = 512
GROUPS = 19
LOADS = 7
SIGNS = (1, -1)
EARLY, LATE = "1fwd and 2far", "2fwd and 3far"
OFFSETS = (0, -1, 1, 2)
NT = (((1,), (1,)), ((), ()))
F32, BF16 = jnp.float32, jnp.bfloat16


def all_parts(step, *args):
    for p in PARTS:
        step(p, *args)


def index(sel, dims=len(FULL)):
    return tuple(pl.ds(*sel[d]) if d in sel else slice(None) for d in range(dims))


def one(i):
    return (i, 1)


def place_of(me):
    return (me // 32, (me // 8) % 4, (me // 2) % 4)


def stepper(place):
    return lambda dim, delta: (place[dim] + delta + 4) % 4


def row_work(at, length, got, gain_row, q_cols, qk_cols, c_out, kr_out, score_out):
    def row_positions(a, b, c, ib, ic):
        r = lax.broadcasted_iota(jnp.int32, (ROWS, 1), 0)
        return (r // 16) * STRIDES[a] + r % 16 + ib * STRIDES[b] + ic * STRIDES[c]

    def unit_shape(a, width):
        return tuple(4 if d == a else 1 for d in range(3)) + (2, 8, width)

    def add_scores(a, wheres, rows, columns):
        part = jnp.dot(jnp.concatenate(rows, axis=0), columns, preferred_element_type=F32)
        for i, where in enumerate(wheres):
            score_out[where] += part[ROWS * i : ROWS * (i + 1)].reshape(unit_shape(a, LANES))

    def finish(j, a, wheres, raws, positions):
        gain = gain_row()
        rows = []
        for where, raw, pos in zip(wheres, raws, positions):
            square = jnp.sum(raw * raw, axis=-1, keepdims=True) * (1.0 / LATENT)
            inv_rms = jnp.where(pos < length(j), lax.rsqrt(square + NORM_EPS), 0.0)
            c_norm = raw * inv_rms * gain
            c_out[(j,) + where] = c_norm.reshape(unit_shape(a, LATENT)).astype(BF16)
            rows.append(c_norm.astype(BF16))
        add_scores(a, wheres, rows, q_cols[j])

    def units(p, off, steps):
        a, b, c = ORDERS[p]
        ib, ics = at(b, off), [at(c, step) for step in steps]
        wheres = [index({b: one(ib), c: one(ic)})[:COL] for ic in ics]
        full = [where + (slice(None),) for where in wheres]
        raws = [got[p][where + (pl.ds(*C_COLS),)].astype(F32).reshape(ROWS, LATENT) for where in wheres]
        finish(p, a, full, raws, [row_positions(a, b, c, ib, ic) for ic in ics])
        if p == 2:
            tiles = [got[2][where + (pl.ds(*K_COLS),)].astype(F32).reshape(ROWS, KEY_COLS).astype(BF16) for where in wheres]
            add_scores(a, full, tiles, qk_cols[...])

    def key_columns(z):
        row = lax.broadcasted_iota(jnp.int32, (KEY_COLS, KEY_COLS), 0)
        col = lax.broadcasted_iota(jnp.int32, (KEY_COLS, KEY_COLS), 1)
        eye = jnp.where(row == col, 1.0, 0.0).astype(BF16)
        tile = got[2][pl.ds(z, 1), :, :, :, :, pl.ds(*K_COLS)].astype(F32).reshape(KEY_COLS, KEY_COLS).astype(BF16)
        turned = lax.dot_general(eye, tile, NT, preferred_element_type=F32)
        for j in REQUESTS:
            valid = col[:ROPE] + z * KEY_COLS < length(j)
            kr_out[j, :, pl.ds(pl.multiple_of(z * KEY_COLS, KEY_COLS), KEY_COLS)] = jnp.where(valid, turned[ROPE * j : ROPE * (j + 1)], 0.0).astype(BF16)

    def last_request(steps):
        places = [(at(1, y), at(2, x)) for y, x in steps]
        wheres = [index({1: one(y), 2: one(x)})[:COL] for y, x in places]
        raws = [jnp.concatenate([got[p][where + (pl.ds(*K_COLS),)].astype(F32).reshape(ROWS, KEY_COLS) for p in PAIR], axis=1) for where in wheres]
        finish(3, 0, [where + (slice(None),) for where in wheres], raws, [row_positions(0, 1, 2, y, x) for y, x in places])

    return units, last_request, key_columns


def exchange_kernel(c_ref, k_ref, cos_ref, sin_ref, gain_ref, len_ref, qlat_ref, qrope_ref, c_out, kr_out, score_out, len_out, got, q_cols, qk_cols, gain_out, scratch):
    parts, k_laid, hop1, hop2, hop3, small, sems = scratch
    mid1, mid2 = [[parts.at[3 * stage + p] for p in PARTS] for stage in PAIR]
    got = [got.at[p] for p in PARTS]
    k_buf, angles, gain_buf, len_buf, qlat_buf, qrope_buf = small
    load_sem, send_sem, recv_sem = sems

    me = lax.axis_index("x")
    core = me % 2
    other = me + 1 - 2 * core
    other_core = 1 - core
    cores = (core, other_core)
    place = place_of(me)
    at = stepper(place)

    def device(dim, delta, to_core=None):
        pos = list(place)
        pos[dim] = (pos[dim] + delta + 4) % 4
        last = core if to_core is None else to_core
        return ((pos[0] * 4 + pos[1]) * 4 + pos[2]) * 2 + last

    def halves(s):
        return (2 * s, 2)

    def view(ref, sel):
        return ref.at[index(sel)]

    barrier = pltpu.get_barrier_semaphore()
    for dim in PARTS:
        for delta in SIGNS:
            for k in PAIR:
                pl.semaphore_signal(barrier, inc=1, device_id={"x": device(dim, delta, k)}, device_id_type=pl.DeviceIdType.MESH)
    pl.semaphore_signal(barrier, inc=1, device_id={"x": other}, device_id_type=pl.DeviceIdType.MESH)

    def taken(sem, n, shape):
        block = parts.at[(pl.ds(0, n),) + index(shape)]
        pltpu.make_async_copy(block, block, sem).wait()

    def taken_from(p, sel, extra):
        where = index(sel, COL - 1)
        if extra:
            return c_ref.at[where + (3, slice(None), pl.ds(KEY_COLS * p, KEY_COLS))]
        return c_ref.at[where + (p, slice(None), pl.ds(*C_COLS))]

    def load(slot, a, b):
        copy = pltpu.make_async_copy(a, b, load_sem.at[slot])
        copy.start()
        return copy

    load(0, cos_ref, angles.at[0])
    load(0, sin_ref, angles.at[1])
    small_loads = [load(1 + i, a, b) for i, (a, b) in enumerate(((k_ref, k_buf), (gain_ref, gain_buf), (len_ref, len_buf), (qlat_ref, qlat_buf), (qrope_ref, qrope_buf)))]
    for p in PARTS:
        own = {ORDERS[p][0]: one(place[ORDERS[p][0]])}
        load(LOADS - 1, taken_from(p, own, False), view(mid1[p], {**own, COL: C_COLS}))
        if p < 2:
            load(LOADS - 1, taken_from(p, own, True), view(mid1[p], {**own, COL: K_COLS}))

    slots = {}

    def send(group, a, b, to, sent=0):
        slot = slots.setdefault(group, len(slots))
        pltpu.make_async_remote_copy(src_ref=a, dst_ref=b, send_sem=send_sem.at[sent], recv_sem=recv_sem.at[slot], device_id={"x": to}, device_id_type=pl.DeviceIdType.MESH).start()

    def arrived(group, n, shape):
        taken(recv_sem.at[slots[group]], n, shape)

    def held(p, sel, cols):
        if cols == C_COLS:
            return taken_from(p, sel, False)
        return taken_from(p, sel, True) if p < 2 else view(k_laid, sel)

    def first_group(p, cols):
        return ("1far", p == 2 and cols == K_COLS)

    def far1(p, cols):
        a, b, _ = ORDERS[p]
        wide = {COL: cols}
        for s, sign in enumerate(SIGNS):
            send(first_group(p, cols), held(p, {a: one(at(a, 2)), b: halves(s)}, cols), view(hop1[2 * p + s], wide), device(a, sign))

    def near1(p, cols):
        a, b, _ = ORDERS[p]
        wide = {COL: cols}
        for s, sign in enumerate(SIGNS):
            send("1near", held(p, {a: one(at(a, sign))}, cols), view(mid1[p], {a: one(place[a]), **wide}), device(a, sign))

    def forward1(p, cols=ALL_COLS):
        a, b, _ = ORDERS[p]
        wide = {COL: cols}
        for s, sign in enumerate(SIGNS):
            send(EARLY, view(hop1[2 * p + s], wide), view(mid1[p], {a: one(at(a, -sign)), b: halves(s), **wide}), device(a, sign))

    def phase2(p, off):
        a, b, c = ORDERS[p]
        sa = {a: one(at(a, off))}
        hop_sa = {a: one(off % 4)}
        for s, sign in enumerate(SIGNS):
            send(EARLY if off == 0 else ("2far", abs(off)), view(mid1[p], {**sa, b: one(at(b, 2)), c: halves(s)}), view(hop2[2 * p + s], hop_sa), device(b, sign))
        for s, sign in enumerate(SIGNS):
            send("2near", view(mid1[p], {**sa, b: one(at(b, sign))}), view(mid2[p], {**sa, b: one(place[b])}), device(b, sign))

    def forward2(p, off):
        a, b, c = ORDERS[p]
        sa = {a: one(at(a, off))}
        hop_sa = {a: one(off % 4)}
        for s, sign in enumerate(SIGNS):
            send(LATE, view(hop2[2 * p + s], hop_sa), view(mid2[p], {**sa, b: one(at(b, -sign)), c: halves(s)}), device(b, sign))

    def phase3(p, off):
        a, b, c = ORDERS[p]
        sb = {b: one(at(b, off))}
        hop_sb = {b: one(off % 4)}
        got_b = mid1[p] if off == 0 else mid2[p]
        mine = {**sb, c: one(place[c]), CORE: one(core)}
        for s, sign in enumerate(SIGNS):
            send(LATE if off == -1 else ("3far", off), view(got_b, {**sb, c: one(at(c, 2)), CORE: one(cores[s])}), view(hop3[2 * p + s], hop_sb), device(c, sign, cores[1 - s]))
        for s, sign in enumerate(SIGNS):
            for k in PAIR:
                send(("3near", off), view(got_b, {**sb, c: one(at(c, sign)), CORE: one(cores[k])}), view(got[p], mine), device(c, sign, cores[k]))
        send(("3near", off), view(got_b, {**sb, c: one(place[c]), CORE: one(cores[1])}), view(got[p], mine), other, 1)
        got[p][index(mine)] = got_b[index(mine)]

    def forward3(p, off):
        a, b, c = ORDERS[p]
        sb = {b: one(at(b, off))}
        hop_sb = {b: one(off % 4)}
        for s, sign in enumerate(SIGNS):
            send(("3fwd", off), view(hop3[2 * p + s], hop_sb), view(got[p], {**sb, c: one(at(c, -sign)), CORE: one(cores[1 - s])}), device(c, sign, other_core))

    def length(j):
        return len_buf[4 * me + j]

    def keys():
        row = lax.broadcasted_iota(jnp.int32, (32, 32), 0)
        diag = row == lax.broadcasted_iota(jnp.int32, (32, 32), 1)
        roped = []
        for pos in range(8):
            cos = jnp.sum(jnp.where(diag, angles[0, pos : pos + 1, :], 0.0), axis=1, keepdims=True)
            sin = jnp.sum(jnp.where(diag, angles[1, pos : pos + 1, :], 0.0), axis=1, keepdims=True)
            lo = k_buf[pos, 0:32, :].astype(F32)
            hi = k_buf[pos, 32:64, :].astype(F32)
            roped.append(jnp.concatenate([lo * cos - hi * sin, hi * cos + lo * sin], axis=0).astype(BF16))
        out_row = lax.broadcasted_iota(jnp.int32, (256, 128), 0)
        lane = lax.broadcasted_iota(jnp.int32, (256, 128), 1)
        picks = [jnp.where((out_row % 8 == pos) & (out_row // 8 == lane // 4), 1.0, 0.0).astype(BF16) for pos in range(8)]
        pick = jnp.concatenate(picks, axis=1)
        request = lax.broadcasted_iota(jnp.int32, (64, 1024), 1) % 4
        for z in REQUESTS:
            cat = jnp.concatenate([r[:, 128 * z : 128 * (z + 1)] for r in roped], axis=1)
            masked = jnp.concatenate([jnp.where(request == j, cat, jnp.zeros_like(cat)) for j in REQUESTS], axis=0)
            laid = lax.dot_general(pick, masked, NT, preferred_element_type=F32)
            laid = laid.reshape(1, 4, 4, 2, 8, 256).astype(BF16)
            k_laid[z : z + 1] = laid
        own = {2: one(place[2])}
        mid1[2][index({**own, COL: K_COLS})] = k_laid[index(own)]

    def queries():
        for j in REQUESTS:
            rows = [qlat_buf[j].astype(F32) if i == j else jnp.zeros((HEADS, LATENT), F32) for i in REQUESTS]
            q_cols[j] = jnp.concatenate(rows + [jnp.zeros((LANES - 4 * HEADS, LATENT), F32)], axis=0).T.astype(BF16)
        zero = jnp.zeros((HEADS, ROPE), F32)
        rows = [jnp.concatenate([qrope_buf[j].astype(F32) if i == j else zero for i in REQUESTS], axis=1) for j in REQUESTS]
        qk_cols[...] = jnp.concatenate(rows + [jnp.zeros((LANES - 4 * HEADS, KEY_COLS), F32)], axis=0).T.astype(BF16)
        score_out[...] = jnp.zeros_like(score_out)
        lane = lax.broadcasted_iota(jnp.int32, (8, LANES), 1)
        lens = jnp.zeros((8, LANES), jnp.int32)
        for j in REQUESTS:
            lens = jnp.where(lane // HEADS == j, length(j), lens)
            len_out[j] = jnp.zeros((8, LANES), jnp.int32) + length(j)
        len_out[4] = lens
        gain_out[...] = jnp.broadcast_to(gain_buf[...].astype(F32).reshape(1, LATENT), gain_out.shape)

    units, last_request, key_columns = row_work(at, length, got, lambda: gain_out[0:1, :], q_cols, qk_cols, c_out, kr_out, score_out)

    def near_units(off):
        arrived(("3near", off), 5, {0: (0, 3), 1: one(0), CORE: one(0)})
        all_parts(units, off, OFFSETS[:3])

    def far_units(off):
        arrived(("3fwd", off), 3, {0: one(0), 1: one(0)})
        all_parts(units, off, OFFSETS[3:])
        key_columns(at(ORDERS[2][1], off))

    BOTH = {0: (0, 3), 2: (0, 2), CORE: one(0)}
    EIGHTH, SIXTEENTH = {0: one(0), 1: (0, 2)}, {0: one(0), 1: one(0)}
    pl.semaphore_wait(barrier, 13)
    for first in (far1, near1):
        all_parts(first, C_COLS)
        first(0, K_COLS)
        first(1, K_COLS)
    pltpu.make_async_copy(angles, angles, load_sem.at[0]).wait()
    small_loads[0].wait()
    keys()
    for copy in small_loads[1:]:
        copy.wait()
    queries()
    far1(2, K_COLS)
    near1(2, K_COLS)
    taken(load_sem.at[LOADS - 1], 4, {0: one(0), COL: C_COLS})
    arrived(first_group(2, C_COLS), 4, {0: one(0), COL: C_COLS})
    forward1(0)
    forward1(1)
    forward1(2, C_COLS)
    all_parts(phase2, 0)
    arrived(first_group(2, K_COLS), 1, {0: one(0), COL: K_COLS})
    forward1(2, K_COLS)
    arrived("1near", 3, {0: (0, 2)})
    all_parts(phase2, -1)
    all_parts(phase2, 1)
    arrived(EARLY, 5, BOTH)
    all_parts(forward2, 0)
    all_parts(phase2, 2)
    arrived(("2far", 1), 3, {0: one(0), 1: (0, 2)})
    all_parts(forward2, -1)
    all_parts(forward2, 1)
    arrived(("2far", 2), 3, SIXTEENTH)
    all_parts(forward2, 2)
    all_parts(phase3, 0)
    arrived("2near", 3, {0: (0, 2)})
    all_parts(phase3, -1)
    arrived(("3far", 0), 3, SIXTEENTH)
    all_parts(forward3, 0)
    all_parts(phase3, 1)
    near_units(0)
    arrived(LATE, 5, BOTH)
    all_parts(forward3, -1)
    all_parts(phase3, 2)
    near_units(-1)
    far_units(0)
    arrived(("3far", 1), 3, SIXTEENTH)
    all_parts(forward3, 1)
    near_units(1)
    far_units(-1)
    last_request([(y, x) for y in OFFSETS[:3] for x in OFFSETS[:2]])
    arrived(("3far", 2), 3, SIXTEENTH)
    all_parts(forward3, 2)
    near_units(2)
    far_units(1)
    last_request([(2, x) for x in OFFSETS[:2]] + [(y, 1) for y in OFFSETS])
    arrived(("3fwd", 2), 3, SIXTEENTH)
    taken(send_sem.at[0], 9, {})
    taken(send_sem.at[1], 3, EIGHTH)


def exchange(c_raw, k_turned, rope_cos, rope_sin, gain, seq_lens, q_lat, q_rope):
    def shaped(sizes):
        return pltpu.VMEM(tuple(sizes.get(d, FULL[d]) for d in range(6)), BF16)

    hop1 = [shaped({o[0]: 1, o[1]: 2}) for o in ORDERS for _ in PAIR]
    hop2 = [shaped({o[1]: 1, o[2]: 2}) for o in ORDERS for _ in PAIR]
    hop3 = [shaped({o[2]: 1, 3: 1}) for o in ORDERS for _ in PAIR]
    small = [
        pltpu.VMEM((8, 64, 512), BF16),
        pltpu.VMEM((2, 8, 32), F32),
        pltpu.VMEM((LATENT,), BF16),
        pltpu.SMEM((REQ,), jnp.int32),
        pltpu.VMEM((4, 16, 512), BF16),
        pltpu.VMEM((4, 16, 64), BF16),
    ]
    sems = [pltpu.SemaphoreType.DMA((n,)) for n in (LOADS, 2, GROUPS)]
    return pl.pallas_call(
        exchange_kernel,
        out_shape=[
            pltpu.VMEM((4, 4, 4, 4, 2, 8, 512), BF16),
            pltpu.VMEM((4, 64, 1024), BF16),
            pltpu.VMEM(FULL[:COL] + (LANES,), F32),
            pltpu.VMEM((5, 8, LANES), jnp.int32),
            pltpu.VMEM((3,) + FULL, BF16),
            pltpu.VMEM((4, LATENT, LANES), BF16),
            pltpu.VMEM((KEY_COLS, LANES), BF16),
            pltpu.VMEM((8, LATENT), F32),
        ],
        in_specs=[pl.BlockSpec(memory_space=pltpu.HBM)] * 8,
        out_specs=[pl.BlockSpec(memory_space=pltpu.VMEM)] * 8,
        scratch_shapes=[[pltpu.VMEM((9,) + FULL, BF16), shaped({COL: KEY_COLS}), hop1, hop2, hop3, small, sems]],
        compiler_params=pltpu.CompilerParams(collective_id=0, has_side_effects=True, vmem_limit_bytes=40 * 1024 * 1024),
        name="exchange",
    )(c_raw, k_turned, rope_cos, rope_sin, gain, seq_lens, q_lat, q_rope)


def attend_kernel(c_in, kr_in, score_in, len_ref, got_ref, q_cols, qk_cols, gain_ref, c_hbm, kr_hbm, o_hbm, c_buf, kr_buf, scores, o_buf, sem):
    at = stepper(place_of(lax.axis_index("x")))
    writes = []

    def write(a, b):
        writes.append(pltpu.make_async_copy(a, b, sem))
        writes[-1].start()

    def write_rows(j, sel):
        where = (j,) + index(sel)
        write(c_buf.at[where], c_hbm.at[where])

    def write_keys(z):
        where = (slice(None), slice(None), pl.ds(pl.multiple_of(z * KEY_COLS, KEY_COLS), KEY_COLS))
        write(kr_buf.at[where], kr_hbm.at[where])

    near, far = OFFSETS[:3], OFFSETS[3]
    for p, (_, b, c) in enumerate(ORDERS):
        for off in near:
            write_rows(p, {b: one(at(b, off))})
        for off in near:
            write_rows(p, {b: one(at(b, far)), c: one(at(c, off))})

    got = [got_ref.at[p] for p in PARTS]
    units, last_request, key_columns = row_work(at, lambda j: len_ref[j, 0:1, 0:1], got, lambda: gain_ref[0:1, :], q_cols, qk_cols, c_buf, kr_buf, scores)
    all_parts(units, far, OFFSETS[3:])
    for off in near:
        write_rows(3, {2: one(at(2, off))})
        write_keys(at(ORDERS[2][1], off))
    last_request([(y, far) for y in OFFSETS])
    for p, (_, b, c) in enumerate(ORDERS):
        write_rows(p, {b: one(at(b, far)), c: one(at(c, far))})
    write_rows(3, {2: one(at(2, far))})
    key_columns(at(ORDERS[2][1], far))
    write_keys(at(ORDERS[2][1], far))

    row = lax.broadcasted_iota(jnp.int32, (POSITIONS, LANES), 0)
    masked = jnp.where(row < len_ref[4, 0:1, :], scores[...].reshape(POSITIONS, LANES) * ATTN_SCALE, -1e30)
    weights = jnp.exp(masked - jnp.max(masked, axis=0, keepdims=True)).T
    weight_sum = jnp.sum(weights[: 4 * HEADS], axis=1, keepdims=True)
    rounded = weights[: 4 * HEADS].astype(BF16)
    for j in REQUESTS:
        mine = slice(HEADS * j, HEADS * (j + 1))
        weighted = jnp.dot(rounded[mine], c_buf[j].reshape(POSITIONS, LATENT), preferred_element_type=F32)
        o_buf[j] = (weighted / weight_sum[mine]).astype(BF16)
        write(o_buf.at[j], o_hbm.at[j])
    for copy in writes:
        copy.wait()


def attend(*handed):
    c_cache, kr_turned, scores = handed[:3]
    in_hbm, in_vmem = pl.BlockSpec(memory_space=pltpu.HBM), pl.BlockSpec(memory_space=pltpu.VMEM)
    return pl.pallas_call(
        attend_kernel,
        out_shape=[
            jax.ShapeDtypeStruct(c_cache.shape, BF16),
            jax.ShapeDtypeStruct(kr_turned.shape, BF16),
            jax.ShapeDtypeStruct((4, HEADS, LATENT), BF16),
            pltpu.VMEM(c_cache.shape, BF16),
            pltpu.VMEM(kr_turned.shape, BF16),
            pltpu.VMEM(scores.shape, F32),
        ],
        in_specs=[in_vmem] * len(handed),
        out_specs=[in_hbm] * 3 + [in_vmem] * 3,
        input_output_aliases={0: 3, 1: 4, 2: 5},
        scratch_shapes=[pltpu.VMEM((4, HEADS, LATENT), BF16), pltpu.SemaphoreType.DMA],
        compiler_params=pltpu.CompilerParams(vmem_limit_bytes=16 * 1024 * 1024),
        name="attend",
    )(*handed)[:3]


def solution(mesh):
    seq_spec = P("dp", "x", None)
    req_spec = P(("dp", "x"), None, None)

    def local_step(c_raw, k_raw, norm_gain, rope_cos, rope_sin, seq_lens, q_lat, q_rope):
        args = (c_raw.reshape(FULL[:4] + (4, 8, LATENT)), k_raw.transpose(1, 2, 0), rope_cos, rope_sin, norm_gain, seq_lens, q_lat, q_rope)
        handed = exchange(*[pltpu.with_memory_space_constraint(arg, pltpu.HBM) for arg in args])
        c_cache, kr_turned, o_lat = attend(*handed)
        c_cache = c_cache.reshape(4, POSITIONS, LATENT)
        return c_cache, kr_turned.transpose(0, 2, 1), o_lat

    return jax.shard_map(local_step, mesh=mesh, in_specs=(seq_spec, seq_spec, P(None), P("x", None), P("x", None), P("dp"), req_spec, req_spec), out_specs=(req_spec, req_spec, req_spec), check_vma=False)
```
